32 devices in a mesh: shard: 8 (over y, x, core), width: 4 (over z).
Axes of the slice: x: 2, y: 2, z: 4, core: 2. Of those that a mesh axis runs over, the one named last changes fastest.
Arguments:
- w_query: bfloat16 [5120, 5120], P('shard', 'width'), may hold values from -0.125 to 0.125
- low_query: bfloat16 [5120, 32], P('shard'), may hold values from -0.078125 to 0.078125
- high_query: bfloat16 [32, 5120], P(None, 'width'), may hold values from -1 to 1
- w_key: bfloat16 [5120, 5120], P('shard', 'width'), may hold values from -0.125 to 0.125
- low_key: bfloat16 [5120, 32], P('shard'), may hold values from -0.078125 to 0.078125
- high_key: bfloat16 [32, 5120], P(None, 'width'), may hold values from -1 to 1
- w_value: bfloat16 [5120, 5120], P('shard', 'width'), may hold values from -0.125 to 0.125
- low_value: bfloat16 [5120, 32], P('shard'), may hold values from -0.078125 to 0.078125
- high_value: bfloat16 [32, 5120], P(None, 'width'), may hold values from -1 to 1
- norm_train: float32 [5120], P(('shard', 'width')), may hold values from 0.25 to 1.75
- norm_step: float32 [5120], P(('shard', 'width')), may hold values from -0.3 to 0.3
Outputs:
- ready_query: bfloat16 [5120, 5120], P(None, 'width')
- ready_key: bfloat16 [5120, 5120], P(None, 'width')
- ready_value: bfloat16 [5120, 5120], P(None, 'width')
- factor_query: float32 [5120], P('width')
- factor_key: float32 [5120], P('width')
- factor_value: float32 [5120], P('width')
- serve_norm: bfloat16 [5120], replicated
The draws below stay inside these ranges and needn't reach their ends.
All inputs are finite; a program needn't handle non-finite values. Where the reference program divides by a largest or mean magnitude, that divisor is 1e-20 or more.
Results may differ from the reference program's by a relative error of at most 0.001.
Values may be sent and summed in bfloat16 or wider, within the bound.
A program may use at most 128 MiB of HBM per device.

```python
import jax
import jax.numpy as jnp

D_MODEL = 5120
Q_DIM = 5120
KV_DIM = 5120
RANK = 32


def with_spikes(result, own_key, source, target, parts, factor):
    def block_of(dim):
        return (jnp.arange(result.shape[dim]) // (result.shape[dim] // parts)).reshape((-1,) + (1,) * (result.ndim - 1 - dim))

    one_side = jax.random.permutation(own_key, parts)[block_of(target)]
    other_side = (block_of(target) + parts // 2) % parts
    return jnp.where((block_of(source) == one_side) | (block_of(source) == other_side), factor * result, result)


def steps_of(stream_key, extent, split, least, high):
    def one(position, shards_of):
        steps = jax.random.uniform(jax.random.fold_in(jax.random.fold_in(stream_key, 6), position), (shards_of,), jnp.float32, least / len(split), high / len(split))
        return jnp.repeat(jnp.exp(steps), extent[position] // shards_of).reshape((-1,) + (1,) * (len(extent) - position - 1))

    factor_of = one(*split[0])
    for cut in split[1:]:
        factor_of = factor_of * one(*cut)
    return factor_of


def scatter_about(key, extent, spread, reach, shards=(), kind=jnp.bfloat16):
    entries = jax.random.normal(key, extent, jnp.float32) * spread
    if len(shards) > 0:
        entries = steps_of(key, extent, shards, -0.22, 0.18) * entries
    return jnp.clip(entries, min=-reach, max=reach).astype(kind)


def noise_with(key, extent, spread, most, cuts, heavy, kind=jnp.bfloat16):
    result = spread * jax.random.normal(key, extent, jnp.float32)
    if cuts:
        result = result * steps_of(key, extent, cuts, -0.22, 0.18)
    return jnp.clip(with_spikes(result, jax.random.fold_in(key, 3), *heavy), -most, most).astype(kind)


def setup_inputs(seed: int = 0) -> dict:
    splits = jax.random.split(jax.random.key(seed), 12)
    w_query = noise_with(splits[0], (D_MODEL, Q_DIM), D_MODEL ** -0.5, 0.125, ((0, 8), (1, 4)), (0, 1, 8, 2.0))
    low_query = scatter_about(splits[1], (D_MODEL, RANK), D_MODEL ** -0.5, 0.078125, ((0, 8),))
    high_query = scatter_about(splits[2], (RANK, Q_DIM), RANK ** -0.5, 1.0, ((1, 4),))
    w_key = noise_with(splits[3], (D_MODEL, KV_DIM), D_MODEL ** -0.5, 0.125, ((0, 8), (1, 4)), (0, 1, 8, 2.0))
    low_key = scatter_about(splits[4], (D_MODEL, RANK), D_MODEL ** -0.5, 0.078125, ((0, 8),))
    high_key = scatter_about(splits[5], (RANK, KV_DIM), RANK ** -0.5, 1.0, ((1, 4),))
    w_value = noise_with(splits[6], (D_MODEL, KV_DIM), D_MODEL ** -0.5, 0.125, ((0, 8), (1, 4)), (0, 1, 8, 2.0))
    low_value = scatter_about(splits[7], (D_MODEL, RANK), D_MODEL ** -0.5, 0.078125, ((0, 8),))
    high_value = scatter_about(splits[8], (RANK, KV_DIM), RANK ** -0.5, 1.0, ((1, 4),))
    norm_train = jnp.clip(1.0 + 0.15 * jax.random.normal(splits[9], (D_MODEL,), jnp.float32), 0.25, 1.75)
    norm_step = jnp.clip(jax.random.uniform(splits[10], (D_MODEL,), jnp.float32, -0.3, 0.3) * steps_of(splits[10], (D_MODEL,), ((0, 32),), -0.4, 0.0), -0.3, 0.3)
    return dict(w_query=w_query, low_query=low_query, high_query=high_query, w_key=w_key, low_key=low_key, high_key=high_key, w_value=w_value, low_value=low_value, high_value=high_value, norm_train=norm_train, norm_step=norm_step)


mix_rate = 0.5


def reference(w_query, low_query, high_query, w_key, low_key, high_key, w_value, low_value, high_value, norm_train, norm_step):
    latest_query = w_query.astype(jnp.float32) + mix_rate * jnp.dot(low_query, high_query, preferred_element_type=jnp.float32)
    latest_key = w_key.astype(jnp.float32) + mix_rate * jnp.dot(low_key, high_key, preferred_element_type=jnp.float32)
    latest_value = w_value.astype(jnp.float32) + mix_rate * jnp.dot(low_value, high_value, preferred_element_type=jnp.float32)
    factor_query = jnp.max(jnp.abs(latest_query), axis=0)
    ready_query = (latest_query / factor_query).astype(jnp.bfloat16)
    factor_key = jnp.max(jnp.abs(latest_key), axis=0)
    ready_key = (latest_key / factor_key).astype(jnp.bfloat16)
    factor_value = jnp.max(jnp.abs(latest_value), axis=0)
    ready_value = (latest_value / factor_value).astype(jnp.bfloat16)
    serve_norm = (norm_train + norm_step).astype(jnp.bfloat16)
    return ready_query, ready_key, ready_value, factor_query, factor_key, factor_value, serve_norm
```

```python
import functools

import jax
import jax.numpy as jnp
from jax import lax
from jax.experimental import pallas as pl
from jax.experimental.pallas import tpu as pltpu
from jax.sharding import PartitionSpec as P

mix_rate = 0.5
MESH = pl.DeviceIdType.MESH
ANY = pl.BlockSpec(memory_space=pl.ANY)


def chunks_of(rows):
    for count in (5, 4, 2):
        if rows % (2 * count * 16) == 0:
            return count
    return 1


def raw_steps(rows):
    return min(2, chunks_of(rows))


def gather_kernel(n, width, *refs):
    weights, lows, highs, norms = refs[0:3], refs[3:6], refs[6:9], refs[9:11]
    ready, small_outs = refs[11], refs[12:16]
    w_mem, low_mem, high_mem, norm_mem, latest, scale, largest_of = refs[16:23]
    load_sem, ring_send, pair_send, max_send, max_recv, norm_send, norm_recv = refs[23:30]
    ring_sem, pair_sem, low_turned, held, gains, out_sem = refs[30:36]
    low_raw, low_far, raw_send, low_send, low_recv, max_in, line_send, line_recv = refs[36:44]
    outs = [ready.at[m] for m in range(3)]

    rows = w_mem.shape[1]
    chips = n // 2
    half = chips // 2
    count = chunks_of(rows)
    piece = rows // (2 * count)
    steps = 3 * count
    raw = raw_steps(rows)
    raw_rows = 2 * piece * raw
    reach = low_raw.shape[2]
    rounds = n.bit_length() - 1
    assert n == 1 << rounds

    me = lax.axis_index("shard")
    line = lax.axis_index("width")
    chip, core = me // 2, lax.rem(me, 2)
    sibling = me + 1 - 2 * core

    def turned(c):
        return jnp.where(c < half, c, chips + half - 1 - c)

    place = turned(chip)

    def shard_at(offset):
        return turned(lax.rem(place + offset + 2 * chips, chips)) * 2 + core

    def group(r):
        return lax.div(me, 1 << r)

    def partner(r):
        return me + (1 << r) * (1 - 2 * lax.rem(group(r), 2))

    def load(source, target, m, slot):
        return pltpu.make_async_copy(source, target, load_sem.at[m, slot])

    first = load(weights[0].at[pl.ds(0, raw_rows)], w_mem.at[0, pl.ds(0, raw_rows)], 3, 2)
    loads = []
    for m in range(3):
        parts = [load(lows[m], low_turned.at[m], m, 0), load(highs[m], high_mem.at[m], m, 1)]
        if m > 0:
            parts.append(load(weights[m], w_mem.at[m], m, 2))
        elif raw_rows < rows:
            rest = pl.ds(raw_rows, rows - raw_rows)
            parts.append(load(weights[0].at[rest], w_mem.at[0, rest], m, 2))
        loads.append(parts)
    norm_loads = [load(norms[i], norm_mem.at[i], 3, i) for i in range(2)]
    first.start()

    barrier = pltpu.get_barrier_semaphore()

    def greet(axis, index):
        pl.semaphore_signal(barrier, inc=1, device_id={axis: index}, device_id_type=MESH)

    greet("shard", shard_at(1))
    greet("shard", shard_at(-1))
    for r in range(rounds):
        greet("shard", partner(r))

    @pl.when(line > 0)
    def _():
        greet("width", line - 1)

    @pl.when(line < width - 1)
    def _():
        greet("width", line + 1)

    for parts in loads:
        for copy in parts:
            copy.start()
    for copy in norm_loads:
        copy.start()

    tile = piece

    def merge(m):
        for copy in loads[m]:
            copy.wait()
        low_mem[m] = low_turned[m].T

        def body(t, largest):
            at = pl.ds(pl.multiple_of(t * tile, tile), tile)
            value = w_mem[m, at, :].astype(jnp.float32) + mix_rate * jnp.dot(
                low_mem[m, at, :], high_mem[m], preferred_element_type=jnp.float32
            )
            latest[m, at, :] = value
            sizes = jnp.abs(value).reshape(tile // 8, 8, value.shape[1])
            return jnp.maximum(largest, jnp.max(sizes, axis=0))

        largest = lax.fori_loop(0, rows // tile, body, jnp.zeros((8, w_mem.shape[2]), jnp.float32))
        largest_of[m, 0] = jnp.max(largest, axis=0, keepdims=True)
        max_copy(m, 0).start()

    def max_copy(m, r):
        return pltpu.make_async_remote_copy(
            src_ref=largest_of.at[m, r],
            dst_ref=max_in.at[m, r],
            send_sem=max_send.at[m, r],
            recv_sem=max_recv.at[m, r],
            device_id={"shard": partner(r)},
            device_id_type=MESH,
        )

    met = [0, 0, 0]

    def advance(m):
        r = met[m]
        if r == rounds:
            return
        max_copy(m, r).wait_recv()
        largest_of[m, r + 1] = jnp.maximum(largest_of[m, r], max_in[m, r])
        met[m] = r + 1
        if r + 1 < rounds:
            max_copy(m, r + 1).start()

    def settle(m):
        while met[m] < rounds:
            advance(m)
        factor = largest_of[m, rounds]
        held[m] = factor
        scale[m] = 1.0 / factor

    def gain_copy(r):
        return pltpu.make_async_remote_copy(
            src_ref=gains.at[line, pl.ds(group(r) * (1 << r), 1 << r)],
            dst_ref=gains.at[line, pl.ds(group(r) * (1 << r), 1 << r)],
            send_sem=norm_send.at[r],
            recv_sem=norm_recv.at[r],
            device_id={"shard": partner(r)},
            device_id_type=MESH,
        )

    def gain_arrival(r):
        theirs = gains.at[line, pl.ds(lax.div(partner(r), 1 << r) * (1 << r), 1 << r)]
        pltpu.make_async_copy(theirs, theirs, norm_recv.at[r]).wait()

    def line_copy(way, s):
        sign = 1 - 2 * way
        block = gains.at[line - sign * s]
        return pltpu.make_async_remote_copy(
            src_ref=block,
            dst_ref=block,
            send_sem=line_send.at[way, s],
            recv_sem=line_recv.at[way, s],
            device_id={"width": line + sign},
            device_id_type=MESH,
        )

    def inside(value):
        return (value >= 0) & (value < width)

    def line_start(way, s):
        sign = 1 - 2 * way

        @pl.when(inside(line - sign * s) & inside(line + sign))
        def _():
            line_copy(way, s).start()

    def line_finish(way, s):
        sign = 1 - 2 * way

        @pl.when(inside(line - sign * (s + 1)))
        def _():
            block = gains.at[line - sign * (s + 1)]
            pltpu.make_async_copy(block, block, line_recv.at[way, s]).wait()

        @pl.when(inside(line - sign * s) & inside(line + sign))
        def _():
            line_copy(way, s).wait_send()

    def gain_first():
        for copy in norm_loads:
            copy.wait()
        gains[line, me] = norm_mem[0] + norm_mem[1]
        gain_copy(0).start()

    def gain_round(r):
        gain_arrival(r)
        if r + 1 < rounds:
            gain_copy(r + 1).start()
        elif width > 1:
            for way in range(2):
                line_start(way, 0)

    def gain_line(s):
        for way in range(2):
            line_finish(way, s)
        if s + 1 < width - 1:
            for way in range(2):
                line_start(way, s + 1)

    errands = [gain_first]
    errands += [functools.partial(gain_round, r) for r in range(rounds)]
    errands += [functools.partial(gain_line, s) for s in range(width - 1)]

    def rows_of(letter, k):
        return (2 * (k % count) + letter) * piece

    def finish(k):
        m = k // count
        at = pl.ds(rows_of(0, k), 2 * piece)
        ready[m, me, at, :] = (latest[m, at, :] * scale[m]).astype(jnp.bfloat16)

    def view(k, letter, owner):
        return outs[k // count].at[owner, pl.ds(rows_of(letter, k), piece)]

    def ring_copy(k, side, letter, hop):
        sign = 1 - 2 * side
        owner = shard_at(-sign * hop)
        where = view(k, letter, owner)
        source = where
        if k < raw and hop == 0:
            source = w_mem.at[0, pl.ds(rows_of(letter, k), piece)]
        return pltpu.make_async_remote_copy(
            src_ref=source,
            dst_ref=where,
            send_sem=raw_send.at[k, side, letter, hop] if k < raw else ring_send.at[k // count],
            recv_sem=ring_sem.at[k, side, letter, hop],
            device_id={"shard": shard_at(sign)},
            device_id_type=MESH,
        )

    def low_copy(side, hop):
        sign = 1 - 2 * side
        where = low_raw.at[shard_at(-sign * hop)]
        return pltpu.make_async_remote_copy(
            src_ref=low_turned.at[0, :, pl.ds(0, reach)] if hop == 0 else where,
            dst_ref=where,
            send_sem=low_send.at[side, hop],
            recv_sem=low_recv.at[side, hop],
            device_id={"shard": shard_at(sign)},
            device_id_type=MESH,
        )

    def ring_start(k, side, letter, hop):
        ring_copy(k, side, letter, hop).start()

    def low_arrival(side, hop):
        sign = 1 - 2 * side
        owner = shard_at(-sign * (hop + 1))
        where = low_raw.at[owner]
        pltpu.make_async_copy(where, where, low_recv.at[side, hop]).wait()
        if hop + 1 < hops(side, 0):
            low_copy(side, hop + 1).start()
        low_far[owner] = low_raw[owner].T

    def ring_arrival(k, side, letter, hop):
        sign = 1 - 2 * side
        owner = shard_at(-sign * (hop + 1))
        where = view(k, letter, owner)
        pltpu.make_async_copy(where, where, ring_sem.at[k, side, letter, hop]).wait()
        return owner

    def pair_copy(k, letter, owner):
        where = view(k, letter, owner)
        pltpu.make_async_remote_copy(
            src_ref=where,
            dst_ref=where,
            send_sem=pair_send.at[k // count],
            recv_sem=pair_sem.at[k // count],
            device_id={"shard": sibling},
            device_id_type=MESH,
        ).start()

    def hops(side, letter):
        return half if side == letter else half - 1

    pending = []

    def landed(k, side, letter, hop, owner):
        if k < raw:
            pending.append((k, side, letter, hop, owner))
        else:
            pair_copy(k, letter, owner)

    low_seen = set()

    def absorb():
        for k, side, letter, hop, owner in pending:
            if hop + 1 < hops(side, letter):
                ring_copy(k, side, letter, hop + 1).wait_send()
            from_side, from_hop = (side, hop) if hop < hops(side, 0) else (0, half - 1)
            for h in range(from_hop + 1):
                if (from_side, h) not in low_seen:
                    low_seen.add((from_side, h))
                    low_arrival(from_side, h)
            at = pl.ds(rows_of(letter, k), piece)
            value = ready[0, owner, at, :].astype(jnp.float32) + mix_rate * jnp.dot(
                low_far[owner, at, :], high_mem[0], preferred_element_type=jnp.float32
            )
            ready[0, owner, at, :] = (value * scale[0]).astype(jnp.bfloat16)
            pair_copy(k, letter, owner)
        pending.clear()

    small_writes = [
        pltpu.make_async_copy(held.at[m], small_outs[m], out_sem.at[m]) for m in range(3)
    ] + [pltpu.make_async_copy(gains, small_outs[3], out_sem.at[3])]
    first.wait()
    pl.semaphore_wait(
        barrier,
        2 + rounds + (line > 0).astype(jnp.int32) + (line < width - 1).astype(jnp.int32),
    )

    for j in range(steps + half + 1):
        if j < steps:
            for side in range(2):
                if hops(side, side) > 0:
                    ring_start(j, side, side, 0)
        if j == 1:
            merge(1)
            advance(0)
        for hop in range(half):
            k = j - 1 - hop
            if 0 <= k < steps and hop + 1 < half:
                for side in range(2):
                    owner = ring_arrival(k, side, side, hop)
                    ring_start(k, side, side, hop + 1)
                    landed(k, side, side, hop, owner)
        if j < steps:
            for side in range(2):
                if hops(side, 1 - side) > 0:
                    ring_start(j, side, 1 - side, 0)
        for hop in range(half - 1):
            k = j - 1 - hop
            if 0 <= k < steps and hop + 1 < half - 1:
                for side in range(2):
                    owner = ring_arrival(k, side, 1 - side, hop)
                    ring_start(k, side, 1 - side, hop + 1)
                    landed(k, side, 1 - side, hop, owner)
        if raw <= j < steps:
            for letter in range(2):
                pair_copy(j, letter, me)
        if j == 0:
            merge(0)
            for side in range(2):
                if hops(side, 0) > 0:
                    low_copy(side, 0).start()
            advance(0)
        if j == raw:
            merge(2)
        for m in range(1, 3):
            if j > m and met[m] < rounds:
                advance(m)
        if 1 <= j < half:
            for side in range(2):
                if j - 1 < hops(side, 0):
                    low_seen.add((side, j - 1))
                    low_arrival(side, j - 1)
        if j > 0 and errands:
            errands.pop(0)()
        if j == steps - 1:
            while errands:
                errands.pop(0)()
            for copy in small_writes:
                copy.start()
        if raw <= j + 1 < steps:
            if j + 1 == raw:
                settle(0)
            if (j + 1) % count == 0:
                settle((j + 1) // count)
            finish(j + 1)
        for side in range(2):
            for letter in (side, 1 - side):
                hop = hops(side, letter) - 1
                k = j - 2 - hop
                if hop >= 0 and 0 <= k < steps:
                    owner = ring_arrival(k, side, letter, hop)
                    landed(k, side, letter, hop, owner)
        if j == raw:
            for k in range(raw):
                finish(k)
                for letter in range(2):
                    pair_copy(k, letter, me)
        if j >= raw:
            absorb()

    for m in range(3):
        theirs = outs[m].at[pl.ds(0, chips)]
        pltpu.make_async_copy(theirs, theirs, pair_sem.at[m]).wait()
        pltpu.make_async_copy(theirs, theirs, pair_send.at[m]).wait()
        kept = raw_rows if m == 0 else 0
        if kept < rows:
            sent = outs[m].at[pl.ds(0, chips - 1), pl.ds(kept, rows - kept)]
            pltpu.make_async_copy(sent, sent, ring_send.at[m]).wait()
        for r in range(rounds):
            max_copy(m, r).wait_send()
    for side in range(2):
        for k in range(raw):
            for letter in range(2):
                if hops(side, letter) > 0:
                    ring_copy(k, side, letter, 0).wait_send()
        for hop in range(hops(side, 0)):
            low_copy(side, hop).wait_send()
    for r in range(rounds):
        gain_copy(r).wait_send()
    for copy in small_writes:
        copy.wait()


def place_kernel(*refs):
    source, small = refs[0], refs[1:5]
    targets, finals, sem = refs[5:8], refs[8:12], refs[12]
    factors, gains, small_sem = refs[13:16], refs[16], refs[17]
    scales, serve = refs[18:21], refs[21]
    writes = [
        pltpu.make_async_copy(refs[18 + i], finals[i], small_sem.at[4 + i]) for i in range(4)
    ]
    loads = [
        pltpu.make_async_copy(small[i], refs[13 + i], small_sem.at[i]) for i in range(4)
    ]
    for copy in loads:
        copy.start()
    copies = []
    for m in range(3):
        for i in range(source.shape[1]):
            copies.append(
                pltpu.make_async_copy(source.at[m, i], targets[m].at[i], sem.at[m, i])
            )
    for copy in copies:
        copy.start()
    for copy in loads:
        copy.wait()
    for m in range(3):
        scales[m][...] = factors[m][...].reshape(scales[m].shape)
    blocks = [gains[k, i] for i in range(gains.shape[1]) for k in range(gains.shape[0])]
    line = jnp.concatenate(blocks, axis=1)
    serve[...] = line.reshape(serve.shape).astype(jnp.bfloat16)
    copies[0].wait()
    for copy in writes:
        copy.start()
    for copy in copies[1:] + writes:
        copy.wait()


def body(n, width, w_query, low_query, high_query, w_key, low_key, high_key, w_value, low_value, high_value, norm_train, norm_step):
    rows, columns = w_query.shape
    rank = low_query.shape[1]
    length = norm_train.shape[0]
    half = n // 4
    steps = 3 * chunks_of(rows)
    raw = raw_steps(rows)
    rounds = n.bit_length() - 1
    reach = min(rows, -(-(rows // chunks_of(rows)) * raw // 128) * 128)
    results = pl.pallas_call(
        functools.partial(gather_kernel, n, width),
        name="merge_gather",
        out_shape=[pltpu.VMEM((3, n, rows, columns), jnp.bfloat16)]
        + [jax.ShapeDtypeStruct((1, columns), jnp.float32)] * 3
        + [jax.ShapeDtypeStruct((width, n, 1, length), jnp.float32)],
        in_specs=[ANY] * 11,
        out_specs=[pl.BlockSpec(memory_space=pltpu.VMEM)]
        + [pl.BlockSpec(memory_space=pltpu.HBM)] * 4,
        scratch_shapes=[
            pltpu.VMEM((3, rows, columns), jnp.bfloat16),
            pltpu.VMEM((3, rows, rank), jnp.bfloat16),
            pltpu.VMEM((3, rank, columns), jnp.bfloat16),
            pltpu.VMEM((2, 1, length), jnp.float32),
            pltpu.VMEM((3, rows, columns), jnp.float32),
            pltpu.VMEM((3, 1, columns), jnp.float32),
            pltpu.VMEM((3, rounds + 1, 1, columns), jnp.float32),
            pltpu.SemaphoreType.DMA((4, 3)),
            pltpu.SemaphoreType.DMA((3,)),
            pltpu.SemaphoreType.DMA((3,)),
            pltpu.SemaphoreType.DMA((3, rounds)),
            pltpu.SemaphoreType.DMA((3, rounds)),
            pltpu.SemaphoreType.DMA((rounds,)),
            pltpu.SemaphoreType.DMA((rounds,)),
            pltpu.SemaphoreType.DMA((steps, 2, 2, half)),
            pltpu.SemaphoreType.DMA((3,)),
            pltpu.VMEM((3, rank, rows), jnp.bfloat16),
            pltpu.VMEM((3, 1, columns), jnp.float32),
            pltpu.VMEM((width, n, 1, length), jnp.float32),
            pltpu.SemaphoreType.DMA((4,)),
            pltpu.VMEM((n, rank, reach), jnp.bfloat16),
            pltpu.VMEM((n, reach, rank), jnp.bfloat16),
            pltpu.SemaphoreType.DMA((raw, 2, 2, half)),
            pltpu.SemaphoreType.DMA((2, half)),
            pltpu.SemaphoreType.DMA((2, half)),
            pltpu.VMEM((3, rounds, 1, columns), jnp.float32),
            pltpu.SemaphoreType.DMA((2, max(width - 1, 1))),
            pltpu.SemaphoreType.DMA((2, max(width - 1, 1))),
        ],
        compiler_params=pltpu.CompilerParams(
            collective_id=0, has_side_effects=True, vmem_limit_bytes=20 * 2**20
        ),
    )(
        w_query, w_key, w_value,
        low_query.T, low_key.T, low_value.T,
        high_query, high_key, high_value,
        norm_train.reshape(1, length), norm_step.reshape(1, length),
    )
    placed = pl.pallas_call(
        place_kernel,
        name="place",
        out_shape=[jax.ShapeDtypeStruct((n, rows, columns), jnp.bfloat16)] * 3
        + [jax.ShapeDtypeStruct((columns,), jnp.float32)] * 3
        + [jax.ShapeDtypeStruct((n * width * length,), jnp.bfloat16)],
        in_specs=[ANY] + [pl.BlockSpec(memory_space=pltpu.HBM)] * 4,
        out_specs=[ANY] * 3 + [pl.BlockSpec(memory_space=pltpu.HBM)] * 4,
        scratch_shapes=[
            pltpu.SemaphoreType.DMA((3, n)),
            *[pltpu.VMEM((1, columns), jnp.float32)] * 3,
            pltpu.VMEM((width, n, 1, length), jnp.float32),
            pltpu.SemaphoreType.DMA((8,)),
            *[pltpu.VMEM((columns,), jnp.float32)] * 3,
            pltpu.VMEM((n * width * length,), jnp.bfloat16),
        ],
        compiler_params=pltpu.CompilerParams(vmem_limit_bytes=2**20),
    )(pltpu.with_memory_space_constraint(results[0], pltpu.VMEM), *(pltpu.with_memory_space_constraint(small, pltpu.HBM) for small in results[1:]))
    return (
        *(ready.reshape(n * rows, columns) for ready in placed[0:3]),
        *placed[3:],
    )


def solution(mesh):
    n, width = mesh.shape["shard"], mesh.shape["width"]
    return jax.shard_map(
        functools.partial(body, n, width),
        mesh=mesh,
        in_specs=(
            P("shard", "width"),
            P("shard", None),
            P(None, "width"),
            P("shard", "width"),
            P("shard", None),
            P(None, "width"),
            P("shard", "width"),
            P("shard", None),
            P(None, "width"),
            P(("shard", "width")),
            P(("shard", "width")),
        ),
        out_specs=(
            P(None, "width"),
            P(None, "width"),
            P(None, "width"),
            P("width"),
            P("width"),
            P("width"),
            P(),
        ),
        check_vma=False,
    )
```

```python
import functools

import jax
import jax.numpy as jnp
from jax import lax
from jax.experimental import pallas as pl
from jax.experimental.pallas import tpu as pltpu
from jax.sharding import PartitionSpec as P

mix_rate = 0.5
LEAD = 1
MESH = pl.DeviceIdType.MESH
ANY = pl.BlockSpec(memory_space=pl.ANY)
HBM = pl.BlockSpec(memory_space=pltpu.HBM)


def chunks_of(rows):
    for count in (5, 4, 2):
        if rows % (2 * count * 16) == 0:
            return count
    return 1


def raw_steps(rows):
    return min(2, chunks_of(rows))


def extra_steps(rows):
    return 3 * chunks_of(rows) // 5


def ring_slots(half):
    return [
        (side, letter, hop)
        for side in range(2)
        for letter in range(2)
        for hop in range(half if side == letter else half - 1)
    ]


def gather_kernel(n, width, *refs):
    weights, lows, highs, norms = refs[0:3], refs[3:6], refs[6:9], refs[9:11]
    ready, early, small_outs = refs[11], refs[12], refs[13:15]
    w_mem, low_mem, high_mem, norm_mem, latest, scale, largest_of = refs[15:22]
    load_sem, ring_send, pair_send, max_send, max_recv, norm_send, norm_recv = refs[22:29]
    ring_sem, pair_sem, low_turned, held, gains, out_sem = refs[29:35]
    low_raw, low_far, raw_send, low_send, low_recv, max_in, line_send, line_recv = refs[35:43]
    outs = [ready.at[0], ready.at[1], early]

    rows = w_mem.shape[1]
    chips = n // 2
    half = chips // 2
    count = chunks_of(rows)
    piece = rows // (2 * count)
    shared = 2 * count
    extra = extra_steps(rows)
    raw = raw_steps(rows)
    raw_rows = 2 * piece * raw
    reach = low_raw.shape[2]
    rounds = n.bit_length() - 1
    assert n == 1 << rounds

    me = lax.axis_index("shard")
    line = lax.axis_index("width")
    chip, core = me // 2, lax.rem(me, 2)
    sibling = me + 1 - 2 * core
    slots = ring_slots(half)

    def turned(c):
        return jnp.where(c < half, c, chips + half - 1 - c)

    place = turned(chip)

    def shard_at(offset):
        return turned(lax.rem(place + offset + 2 * chips, chips)) * 2 + core

    def group(r):
        return lax.div(me, 1 << r)

    def partner(r):
        return me + (1 << r) * (1 - 2 * lax.rem(group(r), 2))

    def load(source, target, m, slot):
        return pltpu.make_async_copy(source, target, load_sem.at[m, slot])

    first = load(weights[0].at[pl.ds(0, raw_rows)], w_mem.at[0, pl.ds(0, raw_rows)], 3, 2)
    loads = []
    for m in range(3):
        parts = [load(lows[m], low_turned.at[m], m, 0), load(highs[m], high_mem.at[m], m, 1)]
        if m > 0:
            parts.append(load(weights[m], w_mem.at[m], m, 2))
        elif raw_rows < rows:
            rest = pl.ds(raw_rows, rows - raw_rows)
            parts.append(load(weights[0].at[rest], w_mem.at[0, rest], m, 2))
        loads.append(parts)
    norm_loads = [load(norms[i], norm_mem.at[i], 3, i) for i in range(2)]
    first.start()

    barrier = pltpu.get_barrier_semaphore()

    def greet(axis, index):
        pl.semaphore_signal(barrier, inc=1, device_id={axis: index}, device_id_type=MESH)

    greet("shard", shard_at(1))
    greet("shard", shard_at(-1))
    for r in range(rounds):
        greet("shard", partner(r))

    @pl.when(line > 0)
    def _():
        greet("width", line - 1)

    @pl.when(line < width - 1)
    def _():
        greet("width", line + 1)

    for parts in loads:
        for copy in parts:
            copy.start()
    for copy in norm_loads:
        copy.start()

    tile = piece

    def merge(m):
        for copy in loads[m]:
            copy.wait()
        low_mem[m] = low_turned[m].T

        def body(t, largest):
            at = pl.ds(pl.multiple_of(t * tile, tile), tile)
            value = w_mem[m, at, :].astype(jnp.float32) + mix_rate * jnp.dot(
                low_mem[m, at, :], high_mem[m], preferred_element_type=jnp.float32
            )
            latest[m, at, :] = value
            sizes = jnp.abs(value).reshape(tile // 8, 8, value.shape[1])
            return jnp.maximum(largest, jnp.max(sizes, axis=0))

        largest = lax.fori_loop(0, rows // tile, body, jnp.zeros((8, w_mem.shape[2]), jnp.float32))
        largest_of[m, 0] = jnp.max(largest, axis=0, keepdims=True)
        max_copy(m, 0).start()

    def max_copy(m, r):
        return pltpu.make_async_remote_copy(
            src_ref=largest_of.at[m, r],
            dst_ref=max_in.at[m, r],
            send_sem=max_send.at[0],
            recv_sem=max_recv.at[m, r],
            device_id={"shard": partner(r)},
            device_id_type=MESH,
        )

    met = [0, 0, 0]

    def advance(m):
        r = met[m]
        if r == rounds:
            return
        max_copy(m, r).wait_recv()
        largest_of[m, r + 1] = jnp.maximum(largest_of[m, r], max_in[m, r])
        met[m] = r + 1
        if r + 1 < rounds:
            max_copy(m, r + 1).start()

    def settle(m):
        while met[m] < rounds:
            advance(m)
        factor = largest_of[m, rounds]
        held[m] = factor
        scale[m] = 1.0 / factor

    def gain_copy(r):
        return pltpu.make_async_remote_copy(
            src_ref=gains.at[line, pl.ds(group(r) * (1 << r), 1 << r)],
            dst_ref=gains.at[line, pl.ds(group(r) * (1 << r), 1 << r)],
            send_sem=norm_send.at[0],
            recv_sem=norm_recv.at[r],
            device_id={"shard": partner(r)},
            device_id_type=MESH,
        )

    def gain_arrival(r):
        theirs = gains.at[line, pl.ds(lax.div(partner(r), 1 << r) * (1 << r), 1 << r)]
        pltpu.make_async_copy(theirs, theirs, norm_recv.at[r]).wait()

    def line_copy(way, s):
        sign = 1 - 2 * way
        block = gains.at[line - sign * s]
        return pltpu.make_async_remote_copy(
            src_ref=block,
            dst_ref=block,
            send_sem=line_send.at[way],
            recv_sem=line_recv.at[way, s],
            device_id={"width": line + sign},
            device_id_type=MESH,
        )

    def inside(value):
        return (value >= 0) & (value < width)

    def line_start(way, s):
        sign = 1 - 2 * way

        @pl.when(inside(line - sign * s) & inside(line + sign))
        def _():
            line_copy(way, s).start()

    def line_finish(way, s):
        sign = 1 - 2 * way

        @pl.when(inside(line - sign * (s + 1)))
        def _():
            block = gains.at[line - sign * (s + 1)]
            pltpu.make_async_copy(block, block, line_recv.at[way, s]).wait()

        @pl.when(inside(line - sign * s) & inside(line + sign))
        def _():
            line_copy(way, s).wait_send()

    def gain_first():
        for copy in norm_loads:
            copy.wait()
        gains[line, me] = norm_mem[0] + norm_mem[1]
        gain_copy(0).start()

    def gain_round(r):
        gain_arrival(r)
        if r + 1 < rounds:
            gain_copy(r + 1).start()
        elif width > 1:
            for way in range(2):
                line_start(way, 0)

    def gain_line(s):
        for way in range(2):
            line_finish(way, s)
        if s + 1 < width - 1:
            for way in range(2):
                line_start(way, s + 1)

    errands = [gain_first]
    errands += [functools.partial(gain_round, r) for r in range(rounds)]
    errands += [functools.partial(gain_line, s) for s in range(width - 1)]

    def rows_of(letter, k):
        return (2 * (k % count) + letter) * piece

    def finish(k):
        m = k // count
        at = pl.ds(rows_of(0, k), 2 * piece)
        outs[m][me, at, :] = (latest[m, at, :] * scale[m]).astype(jnp.bfloat16)

    def view(k, letter, owner):
        return outs[k // count].at[owner, pl.ds(rows_of(letter, k), piece)]

    def landing(k, side, letter, hop):
        return ring_sem.at[k % ring_sem.shape[0], slots.index((side, letter, hop))]

    def ring_copy(k, side, letter, hop):
        sign = 1 - 2 * side
        owner = shard_at(-sign * hop)
        where = view(k, letter, owner)
        source = where
        if k < raw and hop == 0:
            source = w_mem.at[0, pl.ds(rows_of(letter, k), piece)]
        sent = ring_send.at[k // count]
        if k < raw:
            sent = ring_send.at[3]
            if hop > 0:
                sent = raw_send.at[k, slots.index((side, letter, hop))]
        return pltpu.make_async_remote_copy(
            src_ref=source,
            dst_ref=where,
            send_sem=sent,
            recv_sem=landing(k, side, letter, hop),
            device_id={"shard": shard_at(sign)},
            device_id_type=MESH,
        )

    def low_copy(side, hop):
        sign = 1 - 2 * side
        where = low_raw.at[shard_at(-sign * hop)]
        return pltpu.make_async_remote_copy(
            src_ref=low_turned.at[0, :, pl.ds(0, reach)] if hop == 0 else where,
            dst_ref=where,
            send_sem=low_send.at[0],
            recv_sem=low_recv.at[side * half + hop],
            device_id={"shard": shard_at(sign)},
            device_id_type=MESH,
        )

    def ring_start(k, side, letter, hop):
        ring_copy(k, side, letter, hop).start()

    def low_arrival(side, hop):
        sign = 1 - 2 * side
        owner = shard_at(-sign * (hop + 1))
        where = low_raw.at[owner]
        pltpu.make_async_copy(where, where, low_recv.at[side * half + hop]).wait()
        if hop + 1 < hops(side, 0):
            low_copy(side, hop + 1).start()
        low_far[owner] = low_raw[owner].T

    def ring_arrival(k, side, letter, hop):
        sign = 1 - 2 * side
        owner = shard_at(-sign * (hop + 1))
        where = view(k, letter, owner)
        pltpu.make_async_copy(where, where, landing(k, side, letter, hop)).wait()
        return owner

    def pair_copy(k, letter, owner):
        where = view(k, letter, owner)
        pltpu.make_async_remote_copy(
            src_ref=where,
            dst_ref=where,
            send_sem=pair_send.at[0],
            recv_sem=pair_sem.at[0],
            device_id={"shard": sibling},
            device_id_type=MESH,
        ).start()

    def pair_own():
        for k in range(shared, shared + count):
            finish(k)
        return pltpu.make_async_remote_copy(
            src_ref=early.at[me],
            dst_ref=early.at[me],
            send_sem=pair_send.at[1],
            recv_sem=pair_sem.at[1],
            device_id={"shard": sibling},
            device_id_type=MESH,
        )

    def by_role(k):
        if k < shared:
            return lambda act: act()
        return pl.when(core != LEAD)

    def hops(side, letter):
        return half if side == letter else half - 1

    pending = []

    def landed(k, side, letter, hop, owner):
        if k < raw:
            pending.append((k, side, letter, hop, owner))
        elif k < shared:
            pair_copy(k, letter, owner)

    low_seen = set()

    def absorb():
        for k, side, letter, hop, owner in pending:
            if hop + 1 < hops(side, letter):
                ring_copy(k, side, letter, hop + 1).wait_send()
            from_side, from_hop = (side, hop) if hop < hops(side, 0) else (0, half - 1)
            for h in range(from_hop + 1):
                if (from_side, h) not in low_seen:
                    low_seen.add((from_side, h))
                    low_arrival(from_side, h)
            at = pl.ds(rows_of(letter, k), piece)
            value = ready[0, owner, at, :].astype(jnp.float32) + mix_rate * jnp.dot(
                low_far[owner, at, :], high_mem[0], preferred_element_type=jnp.float32
            )
            ready[0, owner, at, :] = (value * scale[0]).astype(jnp.bfloat16)
            pair_copy(k, letter, owner)
        pending.clear()

    small_writes = [
        pltpu.make_async_copy(held, small_outs[0], out_sem.at[0]),
        pltpu.make_async_copy(gains, small_outs[1], out_sem.at[1]),
    ]
    first.wait()
    pl.semaphore_wait(
        barrier,
        2 + rounds + (line > 0).astype(jnp.int32) + (line < width - 1).astype(jnp.int32),
    )

    own_value = []

    for j in range(shared + extra + half + 1):
        if j < shared + extra:

            @by_role(j)
            def _():
                for side in range(2):
                    if hops(side, side) > 0:
                        ring_start(j, side, side, 0)

        if j == 1:
            merge(1)
            advance(0)
        for hop in range(half - 1):
            k = j - 1 - hop
            if 0 <= k < shared + extra:

                @by_role(k)
                def _():
                    for side in range(2):
                        owner = ring_arrival(k, side, side, hop)
                        ring_start(k, side, side, hop + 1)
                        landed(k, side, side, hop, owner)

        if j < shared + extra:

            @by_role(j)
            def _():
                for side in range(2):
                    if hops(side, 1 - side) > 0:
                        ring_start(j, side, 1 - side, 0)

        for hop in range(half - 2):
            k = j - 1 - hop
            if 0 <= k < shared + extra:

                @by_role(k)
                def _():
                    for side in range(2):
                        owner = ring_arrival(k, side, 1 - side, hop)
                        ring_start(k, side, 1 - side, hop + 1)
                        landed(k, side, 1 - side, hop, owner)

        if raw <= j < shared:
            for letter in range(2):
                pair_copy(j, letter, me)
        if j == 0:
            merge(0)
            for side in range(2):
                if hops(side, 0) > 0:
                    low_copy(side, 0).start()
            advance(0)
        if j == raw:
            merge(2)
        for m in range(1, 3):
            if j > m and met[m] < rounds:
                advance(m)
        if 1 <= j < half:
            for side in range(2):
                if j - 1 < hops(side, 0):
                    low_seen.add((side, j - 1))
                    low_arrival(side, j - 1)
        if j > 0 and errands:
            errands.pop(0)()
        if j == min(raw + rounds + 2, shared - 1):
            settle(2)
            own_value.append(pair_own())
            own_value[0].start()
        if j == shared - 1:
            while errands:
                errands.pop(0)()
            for copy in small_writes:
                copy.start()
        if raw <= j + 1 < shared:
            if j + 1 == raw:
                settle(0)
            if (j + 1) % count == 0:
                settle((j + 1) // count)
            finish(j + 1)
        for side in range(2):
            for letter in (side, 1 - side):
                hop = hops(side, letter) - 1
                k = j - 2 - hop
                if hop >= 0 and 0 <= k < shared + extra:

                    @by_role(k)
                    def _():
                        owner = ring_arrival(k, side, letter, hop)
                        landed(k, side, letter, hop, owner)

        if j == raw:
            for k in range(raw):
                finish(k)
                for letter in range(2):
                    pair_copy(k, letter, me)
        if j >= raw:
            absorb()

    theirs = ready.at[:, pl.ds(0, chips)]
    pltpu.make_async_copy(theirs, theirs, pair_sem.at[0]).wait()
    pltpu.make_async_copy(theirs, theirs, pair_send.at[0]).wait()
    pltpu.make_async_copy(early.at[sibling], early.at[sibling], pair_sem.at[1]).wait()
    own_value[0].wait_send()
    for m in range(2):
        kept = raw_rows if m == 0 else 0
        if kept < rows:
            sent = outs[m].at[pl.ds(0, chips - 1), pl.ds(kept, rows - kept)]
            pltpu.make_async_copy(sent, sent, ring_send.at[m]).wait()
    sent = ready.at[0, pl.ds(0, len([s for s in slots if s[2] == 0]) // 2), pl.ds(0, raw_rows)]
    pltpu.make_async_copy(sent, sent, ring_send.at[3]).wait()
    if extra > 0:

        @pl.when(core != LEAD)
        def _():
            sent = early.at[pl.ds(0, chips - 1), pl.ds(0, 2 * piece * extra)]
            pltpu.make_async_copy(sent, sent, ring_send.at[2]).wait()

    pltpu.make_async_copy(max_in, max_in, max_send.at[0]).wait()
    sent = low_raw.at[pl.ds(0, chips - 1)]
    pltpu.make_async_copy(sent, sent, low_send.at[0]).wait()
    sent = gains.at[line, pl.ds(0, n - 1)]
    pltpu.make_async_copy(sent, sent, norm_send.at[0]).wait()
    for copy in small_writes:
        copy.wait()


def late_kernel(n, *refs):
    early, late = refs[0], refs[2]
    ring_send, pair_send, pair_sem, ring_sem, joined = refs[3:8]
    rows = early.shape[1]
    chips = n // 2
    half = chips // 2
    count = chunks_of(rows)
    piece = rows // (2 * count)
    extra = extra_steps(rows)
    early_rows = 2 * piece * extra
    slots = ring_slots(half)

    me = lax.axis_index("shard")
    chip, core = me // 2, lax.rem(me, 2)
    sibling = me + 1 - 2 * core

    def turned(c):
        return jnp.where(c < half, c, chips + half - 1 - c)

    place = turned(chip)

    def shard_at(offset):
        return turned(lax.rem(place + offset + 2 * chips, chips)) * 2 + core

    def hops(side, letter):
        return half if side == letter else half - 1

    def view(ref, k, letter, owner):
        return ref.at[owner, pl.ds((2 * k + letter) * piece, piece)]

    def ring_copy(k, side, letter, hop):
        sign = 1 - 2 * side
        owner = shard_at(-sign * hop)
        return pltpu.make_async_remote_copy(
            src_ref=view(early if hop == 0 else late, k, letter, owner),
            dst_ref=view(late, k, letter, owner),
            send_sem=ring_send.at[0],
            recv_sem=ring_sem.at[k, slots.index((side, letter, hop))],
            device_id={"shard": shard_at(sign)},
            device_id_type=MESH,
        )

    def ring_arrival(k, side, letter, hop):
        sign = 1 - 2 * side
        owner = shard_at(-sign * (hop + 1))
        where = view(late, k, letter, owner)
        landed = ring_sem.at[k, slots.index((side, letter, hop))]
        pltpu.make_async_copy(where, where, landed).wait()
        return owner

    def to_sibling(source, target):
        pltpu.make_async_remote_copy(
            src_ref=source,
            dst_ref=target,
            send_sem=pair_send.at[0],
            recv_sem=pair_sem.at[0],
            device_id={"shard": sibling},
            device_id_type=MESH,
        ).start()

    barrier = pltpu.get_barrier_semaphore()
    for offset in (1, -1):
        pl.semaphore_signal(
            barrier, inc=1, device_id={"shard": shard_at(offset)}, device_id_type=MESH
        )

    def run(first, join):
        waiting = []

        def landed(k, letter, owner):
            where = view(late, k, letter, owner)
            if join is not None and not joined_at:
                waiting.append(where)
            else:
                to_sibling(where, where)

        joined_at = []
        for j in range(first, count + half + 1):
            if j < count:
                for side in range(2):
                    if hops(side, side) > 0:
                        ring_copy(j, side, side, 0).start()
            for hop in range(half - 1):
                k = j - 1 - hop
                if first <= k < count:
                    for side in range(2):
                        owner = ring_arrival(k, side, side, hop)
                        ring_copy(k, side, side, hop + 1).start()
                        landed(k, side, owner)
            if j < count:
                for side in range(2):
                    if hops(side, 1 - side) > 0:
                        ring_copy(j, side, 1 - side, 0).start()
            for hop in range(half - 2):
                k = j - 1 - hop
                if first <= k < count:
                    for side in range(2):
                        owner = ring_arrival(k, side, 1 - side, hop)
                        ring_copy(k, side, 1 - side, hop + 1).start()
                        landed(k, 1 - side, owner)
            if j == join:
                pl.semaphore_wait(joined, 1)
                joined_at.append(j)
                for where in waiting:
                    to_sibling(where, where)
            for side in range(2):
                for letter in (side, 1 - side):
                    hop = hops(side, letter) - 1
                    k = j - 2 - hop
                    if hop >= 0 and first <= k < count:
                        landed(k, letter, ring_arrival(k, side, letter, hop))
        sent = late.at[pl.ds(0, chips - 1), pl.ds(0, 2 * piece * (count - first))]
        pltpu.make_async_copy(sent, sent, ring_send.at[0]).wait()

    @pl.when(core == LEAD)
    def _():
        pl.semaphore_signal(barrier, inc=1, device_id={"shard": sibling}, device_id_type=MESH)
        pl.semaphore_wait(barrier, 2)
        run(0, min(extra + 1, count - 1))

    @pl.when(core != LEAD)
    def _():
        pl.semaphore_wait(barrier, 3)
        pl.semaphore_signal(joined, inc=1, device_id={"shard": sibling}, device_id_type=MESH)
        if extra > 0:
            for offset in range(1, chips):
                owner = shard_at(offset)
                at = pl.ds(0, early_rows)
                to_sibling(early.at[owner, at], late.at[owner, at])
        run(extra, None)

    theirs = late.at[pl.ds(0, chips - 1)]
    pltpu.make_async_copy(theirs, theirs, pair_sem.at[0]).wait()
    pltpu.make_async_copy(theirs, theirs, pair_send.at[0]).wait()


def place_first(*refs):
    source, small = refs[0], refs[1:3]
    targets, finals, sem = refs[3:5], refs[5:9], refs[9]
    factors, gains, small_sem = refs[10], refs[11], refs[12]
    scales, serve = refs[13:16], refs[16]
    writes = [
        pltpu.make_async_copy(refs[13 + i], finals[i], small_sem.at[2 + i]) for i in range(4)
    ]
    loads = [
        pltpu.make_async_copy(small[i], refs[10 + i], small_sem.at[i]) for i in range(2)
    ]
    copies = [
        pltpu.make_async_copy(source.at[m, i], targets[m].at[i], sem.at[2 if m else min(i, 1)])
        for m in range(2)
        for i in range(source.shape[1])
    ]
    for copy in loads + copies:
        copy.start()
    for copy in loads:
        copy.wait()
    for m in range(3):
        scales[m][...] = factors[m].reshape(scales[m].shape)
    blocks = [gains[k, i] for i in range(gains.shape[1]) for k in range(gains.shape[0])]
    line = jnp.concatenate(blocks, axis=1)
    serve[...] = line.reshape(serve.shape).astype(jnp.bfloat16)
    copies[0].wait()
    for copy in writes:
        copy.start()
    rest = source.at[0, pl.ds(1, source.shape[1] - 1)]
    both = source.at[1]
    pltpu.make_async_copy(rest, rest, sem.at[1]).wait()
    pltpu.make_async_copy(both, both, sem.at[2]).wait()
    for copy in writes:
        copy.wait()


def place_last(*refs):
    early, late, target, sem = refs
    n, rows = early.shape[0], early.shape[1]
    chips = n // 2
    early_rows = 2 * (rows // (2 * chunks_of(rows))) * extra_steps(rows)
    me = lax.axis_index("shard")
    chip, core = me // 2, lax.rem(me, 2)

    def put(source, owner, *at):
        where = (owner, *at)
        pltpu.make_async_copy(source.at[where], target.at[where], sem.at[0]).start()

    put(early, me)
    put(early, me + 1 - 2 * core)
    for offset in range(1, chips):
        other = lax.rem(chip + offset, chips) * 2
        put(late, other + 1 - core)

        @pl.when(core == LEAD)
        def _():
            put(late, other + core)

        @pl.when(core != LEAD)
        def _():
            if early_rows > 0:
                put(early, other + core, pl.ds(0, early_rows))
            put(late, other + core, pl.ds(early_rows, rows - early_rows))

    pltpu.make_async_copy(late, late, sem.at[0]).wait()


def body(n, width, w_query, low_query, high_query, w_key, low_key, high_key, w_value, low_value, high_value, norm_train, norm_step):
    rows, columns = w_query.shape
    rank = low_query.shape[1]
    length = norm_train.shape[0]
    half = n // 4
    count = chunks_of(rows)
    raw = raw_steps(rows)
    rounds = n.bit_length() - 1
    reach = min(rows, -(-(rows // count) * raw // 128) * 128)
    slots = len(ring_slots(half))
    block = jax.ShapeDtypeStruct((n, rows, columns), jnp.bfloat16)

    def near(value):
        return pltpu.with_memory_space_constraint(value, pltpu.VMEM)

    def far(value):
        return pltpu.with_memory_space_constraint(value, pltpu.HBM)

    ready, early, factors, gains = pl.pallas_call(
        functools.partial(gather_kernel, n, width),
        name="merge_gather",
        out_shape=[
            pltpu.VMEM((2, n, rows, columns), jnp.bfloat16),
            pltpu.VMEM((n, rows, columns), jnp.bfloat16),
            jax.ShapeDtypeStruct((3, 1, columns), jnp.float32),
            jax.ShapeDtypeStruct((width, n, 1, length), jnp.float32),
        ],
        in_specs=[ANY] * 11,
        out_specs=[pl.BlockSpec(memory_space=pltpu.VMEM)] * 2 + [HBM] * 2,
        scratch_shapes=[
            pltpu.VMEM((3, rows, columns), jnp.bfloat16),
            pltpu.VMEM((3, rows, rank), jnp.bfloat16),
            pltpu.VMEM((3, rank, columns), jnp.bfloat16),
            pltpu.VMEM((2, 1, length), jnp.float32),
            pltpu.VMEM((3, rows, columns), jnp.float32),
            pltpu.VMEM((3, 1, columns), jnp.float32),
            pltpu.VMEM((3, rounds + 1, 1, columns), jnp.float32),
            pltpu.SemaphoreType.DMA((4, 3)),
            pltpu.SemaphoreType.DMA((4,)),
            pltpu.SemaphoreType.DMA((2,)),
            pltpu.SemaphoreType.DMA((1,)),
            pltpu.SemaphoreType.DMA((3, rounds)),
            pltpu.SemaphoreType.DMA((1,)),
            pltpu.SemaphoreType.DMA((rounds,)),
            pltpu.SemaphoreType.DMA((5, slots)),
            pltpu.SemaphoreType.DMA((2,)),
            pltpu.VMEM((3, rank, rows), jnp.bfloat16),
            pltpu.VMEM((3, 1, columns), jnp.float32),
            pltpu.VMEM((width, n, 1, length), jnp.float32),
            pltpu.SemaphoreType.DMA((2,)),
            pltpu.VMEM((n, rank, reach), jnp.bfloat16),
            pltpu.VMEM((n, reach, rank), jnp.bfloat16),
            pltpu.SemaphoreType.DMA((raw, slots)),
            pltpu.SemaphoreType.DMA((1,)),
            pltpu.SemaphoreType.DMA((2 * half,)),
            pltpu.VMEM((3, rounds, 1, columns), jnp.float32),
            pltpu.SemaphoreType.DMA((2,)),
            pltpu.SemaphoreType.DMA((2, max(width - 1, 1))),
        ],
        compiler_params=pltpu.CompilerParams(
            collective_id=0, has_side_effects=True, vmem_limit_bytes=20 * 2**20
        ),
    )(
        w_query, w_key, w_value,
        low_query.T, low_key.T, low_value.T,
        high_query, high_key, high_value,
        norm_train.reshape(1, length), norm_step.reshape(1, length),
    )
    query, key, *small = pl.pallas_call(
        place_first,
        name="place_first",
        out_shape=[block] * 2
        + [jax.ShapeDtypeStruct((columns,), jnp.float32)] * 3
        + [jax.ShapeDtypeStruct((n * width * length,), jnp.bfloat16)],
        in_specs=[ANY] + [HBM] * 2,
        out_specs=[HBM] * 6,
        scratch_shapes=[
            pltpu.SemaphoreType.DMA((3,)),
            pltpu.VMEM((3, 1, columns), jnp.float32),
            pltpu.VMEM((width, n, 1, length), jnp.float32),
            pltpu.SemaphoreType.DMA((6,)),
            *[pltpu.VMEM((columns,), jnp.float32)] * 3,
            pltpu.VMEM((n * width * length,), jnp.bfloat16),
        ],
        compiler_params=pltpu.CompilerParams(vmem_limit_bytes=2**20),
    )(near(ready), far(factors), far(gains))
    late = pl.pallas_call(
        functools.partial(late_kernel, n),
        name="gather_late",
        out_shape=pltpu.VMEM((n, rows, columns), jnp.bfloat16),
        in_specs=[ANY, HBM],
        out_specs=pl.BlockSpec(memory_space=pltpu.VMEM),
        scratch_shapes=[
            pltpu.SemaphoreType.DMA((1,)),
            pltpu.SemaphoreType.DMA((1,)),
            pltpu.SemaphoreType.DMA((1,)),
            pltpu.SemaphoreType.DMA((count, slots)),
            pltpu.SemaphoreType.REGULAR,
        ],
        compiler_params=pltpu.CompilerParams(
            collective_id=1, has_side_effects=True, vmem_limit_bytes=2**20
        ),
    )(near(early), far(small[0]))
    value = pl.pallas_call(
        place_last,
        name="place_last",
        out_shape=block,
        in_specs=[ANY] * 2,
        out_specs=HBM,
        scratch_shapes=[pltpu.SemaphoreType.DMA((1,))],
        compiler_params=pltpu.CompilerParams(vmem_limit_bytes=2**20),
    )(near(early), near(late))
    return (
        *(ready.reshape(n * rows, columns) for ready in (query, key, value)),
        *small,
    )


def solution(mesh):
    n, width = mesh.shape["shard"], mesh.shape["width"]
    return jax.shard_map(
        functools.partial(body, n, width),
        mesh=mesh,
        in_specs=(
            P("shard", "width"),
            P("shard", None),
            P(None, "width"),
            P("shard", "width"),
            P("shard", None),
            P(None, "width"),
            P("shard", "width"),
            P("shard", None),
            P(None, "width"),
            P(("shard", "width")),
            P(("shard", "width")),
        ),
        out_specs=(
            P(None, "width"),
            P(None, "width"),
            P(None, "width"),
            P("width"),
            P("width"),
            P("width"),
            P(),
        ),
        check_vma=False,
    )
```

```python
import functools

import jax
import jax.numpy as jnp
from jax import lax
from jax.experimental import pallas as pl
from jax.experimental.pallas import tpu as pltpu
from jax.sharding import PartitionSpec as P

mix_rate = 0.5
LEAD = 1
BOTH = 1
MESH = pl.DeviceIdType.MESH
ANY = pl.BlockSpec(memory_space=pl.ANY)
HBM = pl.BlockSpec(memory_space=pltpu.HBM)


def chunks_of(rows):
    for count in (5, 4, 2):
        if rows % (2 * count * 16) == 0:
            return count
    return 1


def raw_steps(rows):
    return min(2, chunks_of(rows))


def value_split(rows):
    count = chunks_of(rows)
    extra = 3 * count // 5
    return min(count // 5 * BOTH, count - extra), extra


def ring_slots(half):
    return [
        (side, letter, hop)
        for side in range(2)
        for letter in range(2)
        for hop in range(half if side == letter else half - 1)
    ]


def gather_kernel(n, width, *refs):
    weights, lows, highs, norms = refs[0:3], refs[3:6], refs[6:9], refs[9:11]
    ready, early, small_outs = refs[11], refs[12], refs[13:15]
    w_mem, low_mem, high_mem, norm_mem, latest, scale, largest_of = refs[15:22]
    load_sem, ring_send, pair_send, max_send, max_recv, norm_send, norm_recv = refs[22:29]
    ring_sem, pair_sem, low_turned, held, gains, out_sem = refs[29:35]
    low_raw, low_far, raw_send, low_send, low_recv, max_in, line_send, line_recv = refs[35:43]
    outs = [ready.at[0], ready.at[1], early]

    rows = w_mem.shape[1]
    chips = n // 2
    half = chips // 2
    count = chunks_of(rows)
    piece = rows // (2 * count)
    both, extra = value_split(rows)
    shared = 2 * count + both
    both_rows = 2 * piece * both
    raw = raw_steps(rows)
    raw_rows = 2 * piece * raw
    reach = low_raw.shape[2]
    rounds = n.bit_length() - 1
    assert n == 1 << rounds

    me = lax.axis_index("shard")
    line = lax.axis_index("width")
    chip, core = me // 2, lax.rem(me, 2)
    sibling = me + 1 - 2 * core
    slots = ring_slots(half)

    def turned(c):
        return jnp.where(c < half, c, chips + half - 1 - c)

    place = turned(chip)

    def shard_at(offset):
        return turned(lax.rem(place + offset + 2 * chips, chips)) * 2 + core

    def group(r):
        return lax.div(me, 1 << r)

    def partner(r):
        return me + (1 << r) * (1 - 2 * lax.rem(group(r), 2))

    def load(source, target, m, slot):
        return pltpu.make_async_copy(source, target, load_sem.at[m, slot])

    first = load(weights[0].at[pl.ds(0, raw_rows)], w_mem.at[0, pl.ds(0, raw_rows)], 3, 2)
    loads = []
    for m in range(3):
        parts = [load(lows[m], low_turned.at[m], m, 0), load(highs[m], high_mem.at[m], m, 1)]
        if m > 0:
            parts.append(load(weights[m], w_mem.at[m], m, 2))
        elif raw_rows < rows:
            rest = pl.ds(raw_rows, rows - raw_rows)
            parts.append(load(weights[0].at[rest], w_mem.at[0, rest], m, 2))
        loads.append(parts)
    norm_loads = [load(norms[i], norm_mem.at[i], 3, i) for i in range(2)]
    first.start()

    barrier = pltpu.get_barrier_semaphore()

    def greet(axis, index):
        pl.semaphore_signal(barrier, inc=1, device_id={axis: index}, device_id_type=MESH)

    greet("shard", shard_at(1))
    greet("shard", shard_at(-1))
    for r in range(rounds):
        greet("shard", partner(r))

    @pl.when(line > 0)
    def _():
        greet("width", line - 1)

    @pl.when(line < width - 1)
    def _():
        greet("width", line + 1)

    for parts in loads:
        for copy in parts:
            copy.start()
    for copy in norm_loads:
        copy.start()

    tile = piece

    def merge(m):
        for copy in loads[m]:
            copy.wait()
        low_mem[m] = low_turned[m].T

        def body(t, largest):
            at = pl.ds(pl.multiple_of(t * tile, tile), tile)
            value = w_mem[m, at, :].astype(jnp.float32) + mix_rate * jnp.dot(
                low_mem[m, at, :], high_mem[m], preferred_element_type=jnp.float32
            )
            latest[m, at, :] = value
            sizes = jnp.abs(value).reshape(tile // 8, 8, value.shape[1])
            return jnp.maximum(largest, jnp.max(sizes, axis=0))

        largest = lax.fori_loop(0, rows // tile, body, jnp.zeros((8, w_mem.shape[2]), jnp.float32))
        largest_of[m, 0] = jnp.max(largest, axis=0, keepdims=True)
        max_copy(m, 0).start()

    def max_copy(m, r):
        return pltpu.make_async_remote_copy(
            src_ref=largest_of.at[m, r],
            dst_ref=max_in.at[m, r],
            send_sem=max_send.at[0],
            recv_sem=max_recv.at[m, r],
            device_id={"shard": partner(r)},
            device_id_type=MESH,
        )

    met = [0, 0, 0]

    def advance(m):
        r = met[m]
        if r == rounds:
            return
        max_copy(m, r).wait_recv()
        largest_of[m, r + 1] = jnp.maximum(largest_of[m, r], max_in[m, r])
        met[m] = r + 1
        if r + 1 < rounds:
            max_copy(m, r + 1).start()

    def settle(m):
        while met[m] < rounds:
            advance(m)
        factor = largest_of[m, rounds]
        held[m] = factor
        scale[m] = 1.0 / factor

    def gain_copy(r):
        return pltpu.make_async_remote_copy(
            src_ref=gains.at[line, pl.ds(group(r) * (1 << r), 1 << r)],
            dst_ref=gains.at[line, pl.ds(group(r) * (1 << r), 1 << r)],
            send_sem=norm_send.at[0],
            recv_sem=norm_recv.at[r],
            device_id={"shard": partner(r)},
            device_id_type=MESH,
        )

    def gain_arrival(r):
        theirs = gains.at[line, pl.ds(lax.div(partner(r), 1 << r) * (1 << r), 1 << r)]
        pltpu.make_async_copy(theirs, theirs, norm_recv.at[r]).wait()

    def line_copy(way, s):
        sign = 1 - 2 * way
        block = gains.at[line - sign * s]
        return pltpu.make_async_remote_copy(
            src_ref=block,
            dst_ref=block,
            send_sem=line_send.at[way],
            recv_sem=line_recv.at[way, s],
            device_id={"width": line + sign},
            device_id_type=MESH,
        )

    def inside(value):
        return (value >= 0) & (value < width)

    def line_start(way, s):
        sign = 1 - 2 * way

        @pl.when(inside(line - sign * s) & inside(line + sign))
        def _():
            line_copy(way, s).start()

    def line_finish(way, s):
        sign = 1 - 2 * way

        @pl.when(inside(line - sign * (s + 1)))
        def _():
            block = gains.at[line - sign * (s + 1)]
            pltpu.make_async_copy(block, block, line_recv.at[way, s]).wait()

        @pl.when(inside(line - sign * s) & inside(line + sign))
        def _():
            line_copy(way, s).wait_send()

    def gain_first():
        for copy in norm_loads:
            copy.wait()
        gains[line, me] = norm_mem[0] + norm_mem[1]
        gain_copy(0).start()

    def gain_round(r):
        gain_arrival(r)
        if r + 1 < rounds:
            gain_copy(r + 1).start()
        elif width > 1:
            for way in range(2):
                line_start(way, 0)

    def gain_line(s):
        for way in range(2):
            line_finish(way, s)
        if s + 1 < width - 1:
            for way in range(2):
                line_start(way, s + 1)

    errands = [gain_first]
    errands += [functools.partial(gain_round, r) for r in range(rounds)]
    errands += [functools.partial(gain_line, s) for s in range(width - 1)]

    def rows_of(letter, k):
        return (2 * (k % count) + letter) * piece

    def finish(k):
        m = k // count
        at = pl.ds(rows_of(0, k), 2 * piece)
        outs[m][me, at, :] = (latest[m, at, :] * scale[m]).astype(jnp.bfloat16)

    def view(k, letter, owner):
        return outs[k // count].at[owner, pl.ds(rows_of(letter, k), piece)]

    def landing(k, side, letter, hop):
        return ring_sem.at[k % ring_sem.shape[0], slots.index((side, letter, hop))]

    def ring_copy(k, side, letter, hop):
        sign = 1 - 2 * side
        owner = shard_at(-sign * hop)
        where = view(k, letter, owner)
        source = where
        if k < raw and hop == 0:
            source = w_mem.at[0, pl.ds(rows_of(letter, k), piece)]
        sent = ring_send.at[k // count]
        if k < raw:
            sent = ring_send.at[3]
            if hop > 0:
                sent = raw_send.at[k, slots.index((side, letter, hop))]
        return pltpu.make_async_remote_copy(
            src_ref=source,
            dst_ref=where,
            send_sem=sent,
            recv_sem=landing(k, side, letter, hop),
            device_id={"shard": shard_at(sign)},
            device_id_type=MESH,
        )

    def low_copy(side, hop):
        sign = 1 - 2 * side
        where = low_raw.at[shard_at(-sign * hop)]
        return pltpu.make_async_remote_copy(
            src_ref=low_turned.at[0, :, pl.ds(0, reach)] if hop == 0 else where,
            dst_ref=where,
            send_sem=low_send.at[0],
            recv_sem=low_recv.at[side * half + hop],
            device_id={"shard": shard_at(sign)},
            device_id_type=MESH,
        )

    def ring_start(k, side, letter, hop):
        ring_copy(k, side, letter, hop).start()

    def low_arrival(side, hop):
        sign = 1 - 2 * side
        owner = shard_at(-sign * (hop + 1))
        where = low_raw.at[owner]
        pltpu.make_async_copy(where, where, low_recv.at[side * half + hop]).wait()
        if hop + 1 < hops(side, 0):
            low_copy(side, hop + 1).start()
        low_far[owner] = low_raw[owner].T

    def ring_arrival(k, side, letter, hop):
        sign = 1 - 2 * side
        owner = shard_at(-sign * (hop + 1))
        where = view(k, letter, owner)
        pltpu.make_async_copy(where, where, landing(k, side, letter, hop)).wait()
        return owner

    def pair_copy(k, letter, owner):
        where = view(k, letter, owner)
        pltpu.make_async_remote_copy(
            src_ref=where,
            dst_ref=where,
            send_sem=pair_send.at[k // (2 * count) * 2],
            recv_sem=pair_sem.at[k // (2 * count) * 2],
            device_id={"shard": sibling},
            device_id_type=MESH,
        ).start()

    def pair_own():
        for k in range(2 * count, 3 * count):
            finish(k)
        return pltpu.make_async_remote_copy(
            src_ref=early.at[me],
            dst_ref=early.at[me],
            send_sem=pair_send.at[1],
            recv_sem=pair_sem.at[1],
            device_id={"shard": sibling},
            device_id_type=MESH,
        )

    def by_role(k):
        if k < shared:
            return lambda act: act()
        return pl.when(core != LEAD)

    def hops(side, letter):
        return half if side == letter else half - 1

    pending = []

    def landed(k, side, letter, hop, owner):
        if k < raw:
            pending.append((k, side, letter, hop, owner))
        elif k < shared:
            pair_copy(k, letter, owner)

    low_seen = set()

    def absorb():
        for k, side, letter, hop, owner in pending:
            if hop + 1 < hops(side, letter):
                ring_copy(k, side, letter, hop + 1).wait_send()
            from_side, from_hop = (side, hop) if hop < hops(side, 0) else (0, half - 1)
            for h in range(from_hop + 1):
                if (from_side, h) not in low_seen:
                    low_seen.add((from_side, h))
                    low_arrival(from_side, h)
            at = pl.ds(rows_of(letter, k), piece)
            value = ready[0, owner, at, :].astype(jnp.float32) + mix_rate * jnp.dot(
                low_far[owner, at, :], high_mem[0], preferred_element_type=jnp.float32
            )
            ready[0, owner, at, :] = (value * scale[0]).astype(jnp.bfloat16)
            pair_copy(k, letter, owner)
        pending.clear()

    small_writes = [
        pltpu.make_async_copy(held, small_outs[0], out_sem.at[0]),
        pltpu.make_async_copy(gains, small_outs[1], out_sem.at[1]),
    ]
    first.wait()
    pl.semaphore_wait(
        barrier,
        2 + rounds + (line > 0).astype(jnp.int32) + (line < width - 1).astype(jnp.int32),
    )

    own_value = []
    closed = set()
    last_hops = [s for side in range(2) for s in slots[::-1] if s[0] == side and s[2] == hops(*s[0:2]) - 1]

    def close(k, side, letter, hop):
        closed.add((k, side, letter))
        landed(k, side, letter, hop, ring_arrival(k, side, letter, hop))

    for j in range(shared + extra + half):
        def first_own():
            for side in range(2):
                if hops(side, side) > 0:
                    ring_start(j, side, side, 0)

        if j < shared + extra and j != shared:
            by_role(j)(first_own)
        if j == 1:
            merge(1)
            advance(0)
        for hop in range(half - 1):
            k = j - 1 - hop
            if 0 <= k < shared + extra:

                @by_role(k)
                def _():
                    for side in range(2):
                        owner = ring_arrival(k, side, side, hop)
                        ring_start(k, side, side, hop + 1)
                        landed(k, side, side, hop, owner)

        if j == shared and extra > 0:
            by_role(j)(first_own)
        if j < shared + extra:

            @by_role(j)
            def _():
                for side in range(2):
                    if hops(side, 1 - side) > 0:
                        ring_start(j, side, 1 - side, 0)

        for hop in range(half - 2):
            k = j - 1 - hop
            if 0 <= k < shared + extra:

                @by_role(k)
                def _():
                    for side in range(2):
                        owner = ring_arrival(k, side, 1 - side, hop)
                        ring_start(k, side, 1 - side, hop + 1)
                        landed(k, side, 1 - side, hop, owner)

        if raw <= j < 2 * count:
            for letter in range(2):
                pair_copy(j, letter, me)
        if j == 0:
            merge(0)
            for side in range(2):
                if hops(side, 0) > 0:
                    low_copy(side, 0).start()
            advance(0)
        if j == raw:
            merge(2)
        for m in range(1, 3):
            if j > m and met[m] < rounds:
                advance(m)
        if 1 <= j < half:
            for side in range(2):
                if j - 1 < hops(side, 0):
                    low_seen.add((side, j - 1))
                    low_arrival(side, j - 1)
        if j > 0 and errands:
            errands.pop(0)()
        if j == min(raw + rounds + 2, 2 * count - 1):
            settle(2)
            own_value.append(pair_own())
            own_value[0].start()
        if j == 2 * count - 1:
            while errands:
                errands.pop(0)()
            for copy in small_writes:
                copy.start()
        if raw <= j + 1 < 2 * count:
            if j + 1 == raw:
                settle(0)
            if (j + 1) % count == 0:
                settle((j + 1) // count)
            finish(j + 1)
        for side, letter, hop in last_hops:
            k = j - 1 - hop
            if 0 <= k < shared + extra and (k, side, letter) not in closed:
                by_role(k)(functools.partial(close, k, side, letter, hop))
        if j == shared and half == 2:
            for side in range(2):
                close(shared - 1, side, side, half - 1)
        if j == raw:
            for k in range(raw):
                finish(k)
                for letter in range(2):
                    pair_copy(k, letter, me)
        if j >= raw:
            absorb()

    theirs = ready.at[:, pl.ds(0, chips)]
    pltpu.make_async_copy(theirs, theirs, pair_sem.at[0]).wait()
    pltpu.make_async_copy(theirs, theirs, pair_send.at[0]).wait()
    pltpu.make_async_copy(early.at[sibling], early.at[sibling], pair_sem.at[1]).wait()
    own_value[0].wait_send()

    def value_part(share):
        return early.at[pl.ds(0, chips - 1), pl.ds(0, share * 2 * piece)]

    if both > 0:
        theirs = value_part(both)
        pltpu.make_async_copy(theirs, theirs, pair_sem.at[2]).wait()
        pltpu.make_async_copy(theirs, theirs, pair_send.at[2]).wait()
    for m in range(2):
        kept = raw_rows if m == 0 else 0
        if kept < rows:
            sent = outs[m].at[pl.ds(0, chips - 1), pl.ds(kept, rows - kept)]
            pltpu.make_async_copy(sent, sent, ring_send.at[m]).wait()
    sent = ready.at[0, pl.ds(0, len([s for s in slots if s[2] == 0]) // 2), pl.ds(0, raw_rows)]
    pltpu.make_async_copy(sent, sent, ring_send.at[3]).wait()
    for share, mine in ((both, core == LEAD), (both + extra, core != LEAD)):
        if share > 0:

            @pl.when(mine)
            def _():
                sent = value_part(share)
                pltpu.make_async_copy(sent, sent, ring_send.at[2]).wait()

    pltpu.make_async_copy(max_in, max_in, max_send.at[0]).wait()
    sent = low_raw.at[pl.ds(0, chips - 1)]
    pltpu.make_async_copy(sent, sent, low_send.at[0]).wait()
    sent = gains.at[line, pl.ds(0, n - 1)]
    pltpu.make_async_copy(sent, sent, norm_send.at[0]).wait()
    for copy in small_writes:
        copy.wait()


def late_kernel(n, *refs):
    early, late = refs[0], refs[2]
    ring_send, pair_send, pair_sem, ring_sem, joined = refs[3:8]
    rows = early.shape[1]
    chips = n // 2
    half = chips // 2
    count = chunks_of(rows)
    piece = rows // (2 * count)
    both, extra = value_split(rows)
    slots = ring_slots(half)

    me = lax.axis_index("shard")
    chip, core = me // 2, lax.rem(me, 2)
    sibling = me + 1 - 2 * core

    def turned(c):
        return jnp.where(c < half, c, chips + half - 1 - c)

    place = turned(chip)

    def shard_at(offset):
        return turned(lax.rem(place + offset + 2 * chips, chips)) * 2 + core

    def hops(side, letter):
        return half if side == letter else half - 1

    def view(ref, k, letter, owner):
        return ref.at[owner, pl.ds((2 * k + letter) * piece, piece)]

    def ring_copy(k, side, letter, hop):
        sign = 1 - 2 * side
        owner = shard_at(-sign * hop)
        return pltpu.make_async_remote_copy(
            src_ref=view(early if hop == 0 else late, k, letter, owner),
            dst_ref=view(late, k, letter, owner),
            send_sem=ring_send.at[0],
            recv_sem=ring_sem.at[k, slots.index((side, letter, hop))],
            device_id={"shard": shard_at(sign)},
            device_id_type=MESH,
        )

    def ring_arrival(k, side, letter, hop):
        sign = 1 - 2 * side
        owner = shard_at(-sign * (hop + 1))
        where = view(late, k, letter, owner)
        landed = ring_sem.at[k, slots.index((side, letter, hop))]
        pltpu.make_async_copy(where, where, landed).wait()
        return owner

    def to_sibling(source, target):
        pltpu.make_async_remote_copy(
            src_ref=source,
            dst_ref=target,
            send_sem=pair_send.at[0],
            recv_sem=pair_sem.at[0],
            device_id={"shard": sibling},
            device_id_type=MESH,
        ).start()

    barrier = pltpu.get_barrier_semaphore()
    for offset in (1, -1):
        pl.semaphore_signal(
            barrier, inc=1, device_id={"shard": shard_at(offset)}, device_id_type=MESH
        )

    def run(first, join):
        waiting = []

        def landed(k, letter, owner):
            where = view(late, k, letter, owner)
            if join is not None and not joined_at:
                waiting.append(where)
            else:
                to_sibling(where, where)

        joined_at = []
        for j in range(first, count + half):
            if j < count:
                for side in range(2):
                    if hops(side, side) > 0:
                        ring_copy(j, side, side, 0).start()
            for hop in range(half - 1):
                k = j - 1 - hop
                if first <= k < count:
                    for side in range(2):
                        owner = ring_arrival(k, side, side, hop)
                        ring_copy(k, side, side, hop + 1).start()
                        landed(k, side, owner)
            if j < count:
                for side in range(2):
                    if hops(side, 1 - side) > 0:
                        ring_copy(j, side, 1 - side, 0).start()
            for hop in range(half - 2):
                k = j - 1 - hop
                if first <= k < count:
                    for side in range(2):
                        owner = ring_arrival(k, side, 1 - side, hop)
                        ring_copy(k, side, 1 - side, hop + 1).start()
                        landed(k, 1 - side, owner)
            if j == join:
                pl.semaphore_wait(joined, 1)
                joined_at.append(j)
                for where in waiting:
                    to_sibling(where, where)
            for side in range(2):
                for letter in (side, 1 - side):
                    hop = hops(side, letter) - 1
                    k = j - 1 - hop
                    if hop >= 0 and first <= k < count:
                        landed(k, letter, ring_arrival(k, side, letter, hop))
        if first < count:
            sent = late.at[pl.ds(0, chips - 1), pl.ds(0, 2 * piece * (count - first))]
            pltpu.make_async_copy(sent, sent, ring_send.at[0]).wait()

    @pl.when(core == LEAD)
    def _():
        pl.semaphore_signal(barrier, inc=1, device_id={"shard": sibling}, device_id_type=MESH)
        pl.semaphore_wait(barrier, 2)
        run(both, count - 1 if both + extra < count else count)

    @pl.when(core != LEAD)
    def _():
        pl.semaphore_wait(barrier, 3)
        pl.semaphore_signal(joined, inc=1, device_id={"shard": sibling}, device_id_type=MESH)
        if extra > 0:
            for offset in range(1, chips):
                owner = shard_at(offset)
                at = pl.ds(2 * piece * both, 2 * piece * extra)
                to_sibling(early.at[owner, at], late.at[owner, at])
        run(both + extra, None)

    theirs = late.at[pl.ds(0, chips - 1), pl.ds(0, 2 * piece * (count - both))]
    pltpu.make_async_copy(theirs, theirs, pair_sem.at[0]).wait()
    pltpu.make_async_copy(theirs, theirs, pair_send.at[0]).wait()


def place_first(*refs):
    source, early, small = refs[0], refs[1], refs[2:4]
    targets, finals, sem = refs[4:7], refs[7:11], refs[11]
    factors, gains, small_sem = refs[12], refs[13], refs[14]
    scales, serve = refs[15:18], refs[18]
    writes = [
        pltpu.make_async_copy(refs[15 + i], finals[i], small_sem.at[2 + i]) for i in range(4)
    ]
    loads = [
        pltpu.make_async_copy(small[i], refs[12 + i], small_sem.at[i]) for i in range(2)
    ]
    n, rows = early.shape[0], early.shape[1]
    both_rows = rows // chunks_of(rows) * value_split(rows)[0]
    chip = lax.div(lax.axis_index("shard"), 2)
    copies = [
        pltpu.make_async_copy(source.at[m, i], targets[m].at[i], sem.at[2 if m else min(i, 1)])
        for m in range(2)
        for i in range(source.shape[1])
    ]
    for copy in loads + copies:
        copy.start()
    ours = pl.ds(2 * chip, 2)
    pltpu.make_async_copy(early.at[ours], targets[2].at[ours], sem.at[3]).start()
    if both_rows > 0:
        for offset in range(1, n // 2):
            where = pl.ds(2 * lax.rem(chip + offset, n // 2), 2), pl.ds(0, both_rows)
            pltpu.make_async_copy(early.at[where], targets[2].at[where], sem.at[4]).start()
    for copy in loads:
        copy.wait()
    for m in range(3):
        scales[m][...] = factors[m].reshape(scales[m].shape)
    blocks = [gains[k, i] for i in range(gains.shape[1]) for k in range(gains.shape[0])]
    line = jnp.concatenate(blocks, axis=1)
    serve[...] = line.reshape(serve.shape).astype(jnp.bfloat16)
    copies[0].wait()
    for copy in writes:
        copy.start()
    rest = source.at[0, pl.ds(1, source.shape[1] - 1)]
    both = source.at[1]
    pltpu.make_async_copy(rest, rest, sem.at[1]).wait()
    pltpu.make_async_copy(both, both, sem.at[2]).wait()
    pltpu.make_async_copy(early.at[ours], targets[2].at[ours], sem.at[3]).wait()
    if both_rows > 0:
        part = early.at[pl.ds(0, n - 2), pl.ds(0, both_rows)]
        pltpu.make_async_copy(part, part, sem.at[4]).wait()
    for copy in writes:
        copy.wait()


def place_last(early, late, before, target, sem):
    n, rows = early.shape[0], early.shape[1]
    chips = n // 2
    share = rows // chunks_of(rows)
    both, extra = value_split(rows)
    me = lax.axis_index("shard")
    chip, core = me // 2, lax.rem(me, 2)

    def put(source, owner, start, stop):
        if start < stop:
            where = owner, pl.ds(start * share, (stop - start) * share)
            pltpu.make_async_copy(source.at[where], target.at[where], sem.at[0]).start()

    count = rows // share
    for offset in range(1, chips):
        other = lax.rem(chip + offset, chips) * 2
        put(late, other + 1 - core, both, count)

        @pl.when(core == LEAD)
        def _():
            put(late, other + core, both, count)

        @pl.when(core != LEAD)
        def _():
            put(early, other + core, both, both + extra)
            put(late, other + core, both + extra, count)

    part = late.at[pl.ds(0, n - 2), pl.ds(both * share, rows - both * share)]
    pltpu.make_async_copy(part, part, sem.at[0]).wait()


def body(n, width, w_query, low_query, high_query, w_key, low_key, high_key, w_value, low_value, high_value, norm_train, norm_step):
    rows, columns = w_query.shape
    rank = low_query.shape[1]
    length = norm_train.shape[0]
    half = n // 4
    count = chunks_of(rows)
    raw = raw_steps(rows)
    rounds = n.bit_length() - 1
    reach = min(rows, -(-(rows // count) * raw // 128) * 128)
    slots = len(ring_slots(half))
    block = jax.ShapeDtypeStruct((n, rows, columns), jnp.bfloat16)

    def near(value):
        return pltpu.with_memory_space_constraint(value, pltpu.VMEM)

    def far(value):
        return pltpu.with_memory_space_constraint(value, pltpu.HBM)

    ready, early, factors, gains = pl.pallas_call(
        functools.partial(gather_kernel, n, width),
        name="merge_gather",
        out_shape=[
            pltpu.VMEM((2, n, rows, columns), jnp.bfloat16),
            pltpu.VMEM((n, rows, columns), jnp.bfloat16),
            jax.ShapeDtypeStruct((3, 1, columns), jnp.float32),
            jax.ShapeDtypeStruct((width, n, 1, length), jnp.float32),
        ],
        in_specs=[ANY] * 11,
        out_specs=[pl.BlockSpec(memory_space=pltpu.VMEM)] * 2 + [HBM] * 2,
        scratch_shapes=[
            pltpu.VMEM((3, rows, columns), jnp.bfloat16),
            pltpu.VMEM((3, rows, rank), jnp.bfloat16),
            pltpu.VMEM((3, rank, columns), jnp.bfloat16),
            pltpu.VMEM((2, 1, length), jnp.float32),
            pltpu.VMEM((3, rows, columns), jnp.float32),
            pltpu.VMEM((3, 1, columns), jnp.float32),
            pltpu.VMEM((3, rounds + 1, 1, columns), jnp.float32),
            pltpu.SemaphoreType.DMA((4, 3)),
            pltpu.SemaphoreType.DMA((4,)),
            pltpu.SemaphoreType.DMA((3,)),
            pltpu.SemaphoreType.DMA((1,)),
            pltpu.SemaphoreType.DMA((3, rounds)),
            pltpu.SemaphoreType.DMA((1,)),
            pltpu.SemaphoreType.DMA((rounds,)),
            pltpu.SemaphoreType.DMA((5, slots)),
            pltpu.SemaphoreType.DMA((3,)),
            pltpu.VMEM((3, rank, rows), jnp.bfloat16),
            pltpu.VMEM((3, 1, columns), jnp.float32),
            pltpu.VMEM((width, n, 1, length), jnp.float32),
            pltpu.SemaphoreType.DMA((2,)),
            pltpu.VMEM((n, rank, reach), jnp.bfloat16),
            pltpu.VMEM((n, reach, rank), jnp.bfloat16),
            pltpu.SemaphoreType.DMA((raw, slots)),
            pltpu.SemaphoreType.DMA((1,)),
            pltpu.SemaphoreType.DMA((2 * half,)),
            pltpu.VMEM((3, rounds, 1, columns), jnp.float32),
            pltpu.SemaphoreType.DMA((2,)),
            pltpu.SemaphoreType.DMA((2, max(width - 1, 1))),
        ],
        compiler_params=pltpu.CompilerParams(
            collective_id=0, has_side_effects=True, vmem_limit_bytes=20 * 2**20
        ),
    )(
        w_query, w_key, w_value,
        low_query.T, low_key.T, low_value.T,
        high_query, high_key, high_value,
        norm_train.reshape(1, length), norm_step.reshape(1, length),
    )
    query, key, value, *small = pl.pallas_call(
        place_first,
        name="place_first",
        out_shape=[block] * 3
        + [jax.ShapeDtypeStruct((columns,), jnp.float32)] * 3
        + [jax.ShapeDtypeStruct((n * width * length,), jnp.bfloat16)],
        in_specs=[ANY] * 2 + [HBM] * 2,
        out_specs=[HBM] * 7,
        scratch_shapes=[
            pltpu.SemaphoreType.DMA((5,)),
            pltpu.VMEM((3, 1, columns), jnp.float32),
            pltpu.VMEM((width, n, 1, length), jnp.float32),
            pltpu.SemaphoreType.DMA((6,)),
            *[pltpu.VMEM((columns,), jnp.float32)] * 3,
            pltpu.VMEM((n * width * length,), jnp.bfloat16),
        ],
        compiler_params=pltpu.CompilerParams(vmem_limit_bytes=2**20),
    )(near(ready), near(early), far(factors), far(gains))
    late = pl.pallas_call(
        functools.partial(late_kernel, n),
        name="gather_late",
        out_shape=pltpu.VMEM((n, rows, columns), jnp.bfloat16),
        in_specs=[ANY, HBM],
        out_specs=pl.BlockSpec(memory_space=pltpu.VMEM),
        scratch_shapes=[
            pltpu.SemaphoreType.DMA((1,)),
            pltpu.SemaphoreType.DMA((1,)),
            pltpu.SemaphoreType.DMA((1,)),
            pltpu.SemaphoreType.DMA((count, slots)),
            pltpu.SemaphoreType.REGULAR,
        ],
        compiler_params=pltpu.CompilerParams(
            collective_id=1, has_side_effects=True, vmem_limit_bytes=2**20
        ),
    )(near(early), far(small[0]))
    value = pl.pallas_call(
        place_last,
        name="place_last",
        out_shape=block,
        in_specs=[ANY] * 2 + [HBM],
        out_specs=HBM,
        scratch_shapes=[pltpu.SemaphoreType.DMA((1,))],
        input_output_aliases={2: 0},
        compiler_params=pltpu.CompilerParams(vmem_limit_bytes=2**20),
    )(near(early), near(late), far(value))
    return (
        *(ready.reshape(n * rows, columns) for ready in (query, key, value)),
        *small,
    )


def solution(mesh):
    n, width = mesh.shape["shard"], mesh.shape["width"]
    return jax.shard_map(
        functools.partial(body, n, width),
        mesh=mesh,
        in_specs=(
            P("shard", "width"),
            P("shard", None),
            P(None, "width"),
            P("shard", "width"),
            P("shard", None),
            P(None, "width"),
            P("shard", "width"),
            P("shard", None),
            P(None, "width"),
            P(("shard", "width")),
            P(("shard", "width")),
        ),
        out_specs=(
            P(None, "width"),
            P(None, "width"),
            P(None, "width"),
            P("width"),
            P("width"),
            P("width"),
            P(),
        ),
        check_vma=False,
    )
```

```python
import functools

import jax
import jax.numpy as jnp
from jax import lax
from jax.experimental import pallas as pl
from jax.experimental.pallas import tpu as pltpu
from jax.sharding import PartitionSpec as P

mix_rate = 0.5
LEAD = 1
FINER = 1
LAST = 16
JOIN = 4
BOTH = 2
EXTRA = 6
MESH = pl.DeviceIdType.MESH
ANY = pl.BlockSpec(memory_space=pl.ANY)
HBM = pl.BlockSpec(memory_space=pltpu.HBM)


def chunks_of(rows):
    for count in (5, 4, 2):
        if rows % (2 * count * 16) == 0:
            return count
    return 1


def value_split(rows):
    count = FINER * chunks_of(rows)
    if rows % (2 * count * 16) != 0:
        count = chunks_of(rows)
    extra = EXTRA * count // 10
    return count, min(count * BOTH // 10, count - extra), extra


def ring_slots(half):
    return [
        (side, letter, hop)
        for side in range(2)
        for letter in range(2)
        for hop in range(half if side == letter else half - 1)
    ]


def gather_kernel(n, width, *refs):
    weights, lows, highs, norms = refs[0:3], refs[3:6], refs[6:9], refs[9:11]
    ready, early, small_outs = refs[11], refs[12], refs[13:15]
    w_mem, low_mem, high_mem, norm_mem, latest, scale, largest_of = refs[15:22]
    load_sem, ring_send, pair_send, max_send, max_recv, norm_send, norm_recv = refs[22:29]
    ring_sem, pair_sem, low_turned, held, gains, out_sem = refs[29:35]
    low_raw, low_far, raw_send, low_send, low_recv, max_in, line_send, line_recv = refs[35:43]
    outs = [ready.at[0], ready.at[1], early]

    rows = w_mem.shape[1]
    chips = n // 2
    half = chips // 2
    count = chunks_of(rows)
    piece = rows // (2 * count)
    value_count, both, extra = value_split(rows)
    value_piece = rows // (2 * value_count)
    shared = 2 * count + both
    raw = 1
    raw_rows = 2 * piece * raw
    reach = low_raw.shape[2]
    rounds = n.bit_length() - 1
    assert n == 1 << rounds

    me = lax.axis_index("shard")
    line = lax.axis_index("width")
    chip, core = me // 2, lax.rem(me, 2)
    sibling = me + 1 - 2 * core
    slots = ring_slots(half)

    def turned(c):
        return jnp.where(c < half, c, chips + half - 1 - c)

    place = turned(chip)

    def shard_at(offset):
        return turned(lax.rem(place + offset + 2 * chips, chips)) * 2 + core

    def group(r):
        return lax.div(me, 1 << r)

    def partner(r):
        return me + (1 << r) * (1 - 2 * lax.rem(group(r), 2))

    def load(source, target, m, slot):
        return pltpu.make_async_copy(source, target, load_sem.at[m, slot])

    first = load(weights[0].at[pl.ds(0, raw_rows)], w_mem.at[0, pl.ds(0, raw_rows)], 3, 2)
    loads = []
    for m in range(3):
        parts = [load(lows[m], low_turned.at[m], m, 0), load(highs[m], high_mem.at[m], m, 1)]
        if m > 0:
            parts.append(load(weights[m], w_mem.at[m], m, 2))
        elif raw_rows < rows:
            rest = pl.ds(raw_rows, rows - raw_rows)
            parts.append(load(weights[0].at[rest], w_mem.at[0, rest], m, 2))
        loads.append(parts)
    norm_loads = [load(norms[i], norm_mem.at[i], 3, i) for i in range(2)]
    first.start()

    barrier = pltpu.get_barrier_semaphore()

    def greet(axis, index):
        pl.semaphore_signal(barrier, inc=1, device_id={axis: index}, device_id_type=MESH)

    greet("shard", shard_at(1))
    greet("shard", shard_at(-1))
    for r in range(rounds):
        greet("shard", partner(r))

    @pl.when(line > 0)
    def _():
        greet("width", line - 1)

    @pl.when(line < width - 1)
    def _():
        greet("width", line + 1)

    for parts in loads:
        for copy in parts:
            copy.start()
    for copy in norm_loads:
        copy.start()

    tile = piece

    def merge(m):
        for copy in loads[m]:
            copy.wait()
        low_mem[m] = low_turned[m].T

        def body(t, largest):
            at = pl.ds(pl.multiple_of(t * tile, tile), tile)
            value = w_mem[m, at, :].astype(jnp.float32) + mix_rate * jnp.dot(
                low_mem[m, at, :], high_mem[m], preferred_element_type=jnp.float32
            )
            latest[m, at, :] = value
            sizes = jnp.abs(value).reshape(tile // 8, 8, value.shape[1])
            return jnp.maximum(largest, jnp.max(sizes, axis=0))

        largest = lax.fori_loop(0, rows // tile, body, jnp.zeros((8, w_mem.shape[2]), jnp.float32))
        largest_of[m, 0] = jnp.max(largest, axis=0, keepdims=True)
        max_copy(m, 0).start()

    def max_copy(m, r):
        return pltpu.make_async_remote_copy(
            src_ref=largest_of.at[m, r],
            dst_ref=max_in.at[m, r],
            send_sem=max_send.at[0],
            recv_sem=max_recv.at[m, r],
            device_id={"shard": partner(r)},
            device_id_type=MESH,
        )

    met = [0, 0, 0]

    def advance(m):
        r = met[m]
        if r == rounds:
            return
        max_copy(m, r).wait_recv()
        largest_of[m, r + 1] = jnp.maximum(largest_of[m, r], max_in[m, r])
        met[m] = r + 1
        if r + 1 < rounds:
            max_copy(m, r + 1).start()

    def settle(m):
        while met[m] < rounds:
            advance(m)
        factor = largest_of[m, rounds]
        held[m] = factor
        scale[m] = 1.0 / factor

    def gain_copy(r):
        return pltpu.make_async_remote_copy(
            src_ref=gains.at[line, pl.ds(group(r) * (1 << r), 1 << r)],
            dst_ref=gains.at[line, pl.ds(group(r) * (1 << r), 1 << r)],
            send_sem=norm_send.at[0],
            recv_sem=norm_recv.at[r],
            device_id={"shard": partner(r)},
            device_id_type=MESH,
        )

    def gain_arrival(r):
        theirs = gains.at[line, pl.ds(lax.div(partner(r), 1 << r) * (1 << r), 1 << r)]
        pltpu.make_async_copy(theirs, theirs, norm_recv.at[r]).wait()

    def line_copy(way, s):
        sign = 1 - 2 * way
        block = gains.at[line - sign * s]
        return pltpu.make_async_remote_copy(
            src_ref=block,
            dst_ref=block,
            send_sem=line_send.at[way],
            recv_sem=line_recv.at[way, s],
            device_id={"width": line + sign},
            device_id_type=MESH,
        )

    def inside(value):
        return (value >= 0) & (value < width)

    def line_start(way, s):
        sign = 1 - 2 * way

        @pl.when(inside(line - sign * s) & inside(line + sign))
        def _():
            line_copy(way, s).start()

    def line_finish(way, s):
        sign = 1 - 2 * way

        @pl.when(inside(line - sign * (s + 1)))
        def _():
            block = gains.at[line - sign * (s + 1)]
            pltpu.make_async_copy(block, block, line_recv.at[way, s]).wait()

        @pl.when(inside(line - sign * s) & inside(line + sign))
        def _():
            line_copy(way, s).wait_send()

    def gain_first():
        for copy in norm_loads:
            copy.wait()
        gains[line, me] = norm_mem[0] + norm_mem[1]
        gain_copy(0).start()

    def gain_round(r):
        gain_arrival(r)
        if r + 1 < rounds:
            gain_copy(r + 1).start()
        elif width > 1:
            for way in range(2):
                line_start(way, 0)

    def gain_line(s):
        for way in range(2):
            line_finish(way, s)
        if s + 1 < width - 1:
            for way in range(2):
                line_start(way, s + 1)

    errands = [gain_first]
    errands += [functools.partial(gain_round, r) for r in range(rounds)]
    errands += [functools.partial(gain_line, s) for s in range(width - 1)]

    def rows_of(letter, k):
        if k < 2 * count:
            return pl.ds((2 * (k % count) + letter) * piece, piece)
        return pl.ds((2 * (k - 2 * count) + letter) * value_piece, value_piece)

    def matrix_of(k):
        return min(k // count, 2)

    def finish(k):
        m = k // count
        at = pl.ds(2 * (k % count) * piece, 2 * piece)
        outs[m][me, at, :] = (latest[m, at, :] * scale[m]).astype(jnp.bfloat16)

    def view(k, letter, owner):
        return outs[matrix_of(k)].at[owner, rows_of(letter, k)]

    def landing(k, side, letter, hop):
        return ring_sem.at[k % ring_sem.shape[0], slots.index((side, letter, hop))]

    def ring_copy(k, side, letter, hop):
        sign = 1 - 2 * side
        owner = shard_at(-sign * hop)
        where = view(k, letter, owner)
        source = where
        if k < raw and hop == 0:
            source = w_mem.at[0, rows_of(letter, k)]
        sent = ring_send.at[matrix_of(k)]
        if k < raw:
            sent = ring_send.at[3]
            if hop > 0:
                sent = raw_send.at[k, slots.index((side, letter, hop))]
        return pltpu.make_async_remote_copy(
            src_ref=source,
            dst_ref=where,
            send_sem=sent,
            recv_sem=landing(k, side, letter, hop),
            device_id={"shard": shard_at(sign)},
            device_id_type=MESH,
        )

    def low_copy(side, hop):
        sign = 1 - 2 * side
        where = low_raw.at[shard_at(-sign * hop)]
        return pltpu.make_async_remote_copy(
            src_ref=low_turned.at[0, :, pl.ds(0, reach)] if hop == 0 else where,
            dst_ref=where,
            send_sem=low_send.at[0],
            recv_sem=low_recv.at[side * half + hop],
            device_id={"shard": shard_at(sign)},
            device_id_type=MESH,
        )

    def ring_start(k, side, letter, hop):
        ring_copy(k, side, letter, hop).start()

    def low_arrival(side, hop):
        sign = 1 - 2 * side
        owner = shard_at(-sign * (hop + 1))
        where = low_raw.at[owner]
        pltpu.make_async_copy(where, where, low_recv.at[side * half + hop]).wait()
        if hop + 1 < hops(side, 0):
            low_copy(side, hop + 1).start()
        low_far[owner] = low_raw[owner].T

    def ring_arrival(k, side, letter, hop):
        sign = 1 - 2 * side
        owner = shard_at(-sign * (hop + 1))
        where = view(k, letter, owner)
        pltpu.make_async_copy(where, where, landing(k, side, letter, hop)).wait()
        return owner

    def pair_copy(k, letter, owner):
        where = view(k, letter, owner)
        pltpu.make_async_remote_copy(
            src_ref=where,
            dst_ref=where,
            send_sem=pair_send.at[matrix_of(k) // 2 * 2],
            recv_sem=pair_sem.at[matrix_of(k) // 2 * 2],
            device_id={"shard": sibling},
            device_id_type=MESH,
        ).start()

    def pair_own():
        for k in range(2 * count, 3 * count):
            finish(k)
        return pltpu.make_async_remote_copy(
            src_ref=early.at[me],
            dst_ref=early.at[me],
            send_sem=pair_send.at[1],
            recv_sem=pair_sem.at[1],
            device_id={"shard": sibling},
            device_id_type=MESH,
        )

    def by_role(k):
        if k < shared:
            return lambda act: act()
        return pl.when(core != LEAD)

    def hops(side, letter):
        return half if side == letter else half - 1

    pending = []

    def landed(k, side, letter, hop, owner):
        if k < raw:
            pending.append((k, side, letter, hop, owner))
        elif k < shared:
            pair_copy(k, letter, owner)

    low_seen = set()

    def absorb():
        for k, side, letter, hop, owner in pending:
            if hop + 1 < hops(side, letter):
                ring_copy(k, side, letter, hop + 1).wait_send()
            from_side, from_hop = (side, hop) if hop < hops(side, 0) else (0, half - 1)
            for h in range(from_hop + 1):
                if (from_side, h) not in low_seen:
                    low_seen.add((from_side, h))
                    low_arrival(from_side, h)
            at = rows_of(letter, k)
            value = ready[0, owner, at, :].astype(jnp.float32) + mix_rate * jnp.dot(
                low_far[owner, at, :], high_mem[0], preferred_element_type=jnp.float32
            )
            ready[0, owner, at, :] = (value * scale[0]).astype(jnp.bfloat16)
            pair_copy(k, letter, owner)
        pending.clear()

    small_writes = [
        pltpu.make_async_copy(held, small_outs[0], out_sem.at[0]),
        pltpu.make_async_copy(gains, small_outs[1], out_sem.at[1]),
    ]
    first.wait()
    pl.semaphore_wait(
        barrier,
        2 + rounds + (line > 0).astype(jnp.int32) + (line < width - 1).astype(jnp.int32),
    )

    own_value = []
    closed = set()
    last_hops = [s for side in range(2) for s in slots[::-1] if s[0] == side and s[2] == hops(*s[0:2]) - 1]

    def pass_on(k, hop):
        for side in range(2):
            owner = ring_arrival(k, side, side, hop)
            ring_start(k, side, side, hop + 1)
            landed(k, side, side, hop, owner)

    def close(k, side, letter, hop):
        closed.add((k, side, letter))
        landed(k, side, letter, hop, ring_arrival(k, side, letter, hop))

    for j in range(shared + extra + half):
        def first_own():
            for side in range(2):
                if hops(side, side) > 0:
                    ring_start(j, side, side, 0)

        if j < shared + extra and j != shared:
            by_role(j)(first_own)
        if j == 0:
            merge(0)
            advance(0)
        for hop in range(half - 1):
            k = j - 1 - hop
            if (k, hop) == (0, 0):
                continue
            if 0 <= k < shared + extra:
                by_role(k)(functools.partial(pass_on, k, hop))

        if j == shared and extra > 0:
            by_role(j)(first_own)
        if j < shared + extra:

            @by_role(j)
            def _():
                for side in range(2):
                    if hops(side, 1 - side) > 0:
                        ring_start(j, side, 1 - side, 0)

        for hop in range(half - 2):
            k = j - 1 - hop
            if 0 <= k < shared + extra:

                @by_role(k)
                def _():
                    for side in range(2):
                        owner = ring_arrival(k, side, 1 - side, hop)
                        ring_start(k, side, 1 - side, hop + 1)
                        landed(k, side, 1 - side, hop, owner)

        if raw <= j < 2 * count:
            for letter in range(2):
                pair_copy(j, letter, me)
        if j == 0:
            for side in range(2):
                if hops(side, 0) > 0:
                    low_copy(side, 0).start()
            advance(0)
            if half > 1:
                pass_on(0, 0)
        if j in (1, 2):
            merge(j)
        for m in range(1, 3):
            if j > m and met[m] < rounds:
                advance(m)
        if 1 <= j < half:
            for side in range(2):
                if j - 1 < hops(side, 0):
                    low_seen.add((side, j - 1))
                    low_arrival(side, j - 1)
        if j > 0 and errands:
            errands.pop(0)()
        if j == min(raw + rounds + 2, 2 * count - 1):
            settle(2)
            own_value.append(pair_own())
            own_value[0].start()
        if j == 2 * count - 1:
            while errands:
                errands.pop(0)()
            for copy in small_writes:
                copy.start()
        if raw <= j + 1 < 2 * count:
            if j + 1 == raw:
                settle(0)
            if (j + 1) % count == 0:
                settle((j + 1) // count)
            finish(j + 1)
        for side, letter, hop in last_hops:
            k = j - 1 - hop
            if 0 <= k < shared + extra and (k, side, letter) not in closed:
                by_role(k)(functools.partial(close, k, side, letter, hop))
        if j == shared and half == 2:
            for side in range(2):
                close(shared - 1, side, side, half - 1)
        if j == raw:
            for k in range(raw):
                finish(k)
                for letter in range(2):
                    pair_copy(k, letter, me)
        if j >= raw:
            absorb()

    theirs = ready.at[:, pl.ds(0, chips)]
    pltpu.make_async_copy(theirs, theirs, pair_sem.at[0]).wait()
    pltpu.make_async_copy(theirs, theirs, pair_send.at[0]).wait()
    pltpu.make_async_copy(early.at[sibling], early.at[sibling], pair_sem.at[1]).wait()
    own_value[0].wait_send()

    def value_part(share):
        return early.at[pl.ds(0, chips - 1), pl.ds(0, share * 2 * value_piece)]

    if both > 0:
        theirs = value_part(both)
        pltpu.make_async_copy(theirs, theirs, pair_sem.at[2]).wait()
        pltpu.make_async_copy(theirs, theirs, pair_send.at[2]).wait()
    for m in range(2):
        kept = raw_rows if m == 0 else 0
        if kept < rows:
            sent = outs[m].at[pl.ds(0, chips - 1), pl.ds(kept, rows - kept)]
            pltpu.make_async_copy(sent, sent, ring_send.at[m]).wait()
    sent = ready.at[0, pl.ds(0, len([s for s in slots if s[2] == 0]) // 2), pl.ds(0, raw_rows)]
    pltpu.make_async_copy(sent, sent, ring_send.at[3]).wait()
    for share, mine in ((both, core == LEAD), (both + extra, core != LEAD)):
        if share > 0:

            @pl.when(mine)
            def _():
                sent = value_part(share)
                pltpu.make_async_copy(sent, sent, ring_send.at[2]).wait()

    pltpu.make_async_copy(max_in, max_in, max_send.at[0]).wait()
    sent = low_raw.at[pl.ds(0, chips - 1)]
    pltpu.make_async_copy(sent, sent, low_send.at[0]).wait()
    sent = gains.at[line, pl.ds(0, n - 1)]
    pltpu.make_async_copy(sent, sent, norm_send.at[0]).wait()
    for copy in small_writes:
        copy.wait()


def late_kernel(n, *refs):
    early, late = refs[0], refs[2]
    ring_send, pair_send, pair_sem, ring_sem, joined, last_sem = refs[3:9]
    parts = last_sem.shape[1]
    rows = early.shape[1]
    chips = n // 2
    half = chips // 2
    count, both, extra = value_split(rows)
    piece = rows // (2 * count)
    slots = ring_slots(half)

    me = lax.axis_index("shard")
    chip, core = me // 2, lax.rem(me, 2)
    sibling = me + 1 - 2 * core

    def turned(c):
        return jnp.where(c < half, c, chips + half - 1 - c)

    place = turned(chip)

    def shard_at(offset):
        return turned(lax.rem(place + offset + 2 * chips, chips)) * 2 + core

    def hops(side, letter):
        return half if side == letter else half - 1

    def view(ref, k, letter, owner, part=None):
        first, size = (2 * k + letter) * piece, piece
        if part is not None:
            size = piece // parts
            first += part * size
        return ref.at[owner, pl.ds(first, size)]

    def landing(k, side, letter, hop, part=None):
        if part is not None:
            return last_sem.at[side, part]
        return ring_sem.at[k % ring_sem.shape[0], slots.index((side, letter, hop))]

    def cut(k, side, letter, hop):
        if k == count - 1 and side == letter and hop == half - 1 and hop > 0 and parts > 1:
            return range(parts)
        return [None]

    def ring_start(k, side, letter, hop):
        sign = 1 - 2 * side
        owner = shard_at(-sign * hop)
        for part in cut(k, side, letter, hop):
            pltpu.make_async_remote_copy(
                src_ref=view(early if hop == 0 else late, k, letter, owner, part),
                dst_ref=view(late, k, letter, owner, part),
                send_sem=ring_send.at[0],
                recv_sem=landing(k, side, letter, hop, part),
                device_id={"shard": shard_at(sign)},
                device_id_type=MESH,
            ).start()

    def ring_arrival(k, side, letter, hop, part=None):
        sign = 1 - 2 * side
        where = view(late, k, letter, shard_at(-sign * (hop + 1)), part)
        pltpu.make_async_copy(where, where, landing(k, side, letter, hop, part)).wait()
        return where

    def to_sibling(source, target):
        pltpu.make_async_remote_copy(
            src_ref=source,
            dst_ref=target,
            send_sem=pair_send.at[0],
            recv_sem=pair_sem.at[0],
            device_id={"shard": sibling},
            device_id_type=MESH,
        ).start()

    barrier = pltpu.get_barrier_semaphore()
    for offset in (1, -1):
        pl.semaphore_signal(
            barrier, inc=1, device_id={"shard": shard_at(offset)}, device_id_type=MESH
        )

    def run(first, join):
        waiting = []

        def landed(where):
            if join is not None and not joined_at:
                waiting.append(where)
            else:
                to_sibling(where, where)

        joined_at = []
        for j in range(first, count + half):
            if j < count:
                for side in range(2):
                    if hops(side, side) > 0:
                        ring_start(j, side, side, 0)
            for hop in range(half - 1):
                k = j - 1 - hop
                if first <= k < count:
                    for side in range(2):
                        where = ring_arrival(k, side, side, hop)
                        ring_start(k, side, side, hop + 1)
                        landed(where)
            if j < count:
                for side in range(2):
                    if hops(side, 1 - side) > 0:
                        ring_start(j, side, 1 - side, 0)
            for hop in range(half - 2):
                k = j - 1 - hop
                if first <= k < count:
                    for side in range(2):
                        where = ring_arrival(k, side, 1 - side, hop)
                        ring_start(k, side, 1 - side, hop + 1)
                        landed(where)
            if j == join:
                pl.semaphore_wait(joined, 1)
                joined_at.append(j)
                for where in waiting:
                    to_sibling(where, where)
            ends = [
                (j - hops(side, letter), side, letter, hops(side, letter) - 1)
                for flip in range(2)
                for side in range(2)
                for letter in (side ^ flip,)
            ]
            ends = [s for s in ends if s[3] >= 0 and first <= s[0] < count]
            for part in range(parts):
                for s in ends:
                    if part < len(cut(*s)):
                        landed(ring_arrival(*s, cut(*s)[part]))
        if first < count:
            sent = late.at[pl.ds(0, chips - 1), pl.ds(0, 2 * piece * (count - first))]
            pltpu.make_async_copy(sent, sent, ring_send.at[0]).wait()

    @pl.when(core == LEAD)
    def _():
        pl.semaphore_signal(barrier, inc=1, device_id={"shard": sibling}, device_id_type=MESH)
        pl.semaphore_wait(barrier, 2)
        run(both, JOIN)

    @pl.when(core != LEAD)
    def _():
        pl.semaphore_wait(barrier, 3)
        pl.semaphore_signal(joined, inc=1, device_id={"shard": sibling}, device_id_type=MESH)
        if extra > 0:
            for offset in range(1, chips):
                owner = shard_at(offset)
                at = pl.ds(2 * piece * both, 2 * piece * extra)
                to_sibling(early.at[owner, at], late.at[owner, at])
        run(both + extra, None)

    theirs = late.at[pl.ds(0, chips - 1), pl.ds(0, 2 * piece * (count - both))]
    pltpu.make_async_copy(theirs, theirs, pair_sem.at[0]).wait()
    pltpu.make_async_copy(theirs, theirs, pair_send.at[0]).wait()


def place_first(*refs):
    source, early, small = refs[0], refs[1], refs[2:4]
    targets, finals, sem = refs[4:7], refs[7:11], refs[11]
    factors, gains, small_sem = refs[12], refs[13], refs[14]
    scales, serve = refs[15:18], refs[18]
    writes = [
        pltpu.make_async_copy(refs[15 + i], finals[i], small_sem.at[2 + i]) for i in range(4)
    ]
    loads = [
        pltpu.make_async_copy(small[i], refs[12 + i], small_sem.at[i]) for i in range(2)
    ]
    n, rows = early.shape[0], early.shape[1]
    value_count, both, _ = value_split(rows)
    both_rows = rows // value_count * both
    chip = lax.div(lax.axis_index("shard"), 2)
    copies = [
        pltpu.make_async_copy(source.at[m, i], targets[m].at[i], sem.at[2 if m else min(i, 1)])
        for m in range(2)
        for i in range(source.shape[1])
    ]
    for copy in loads + copies:
        copy.start()
    ours = pl.ds(2 * chip, 2)
    pltpu.make_async_copy(early.at[ours], targets[2].at[ours], sem.at[3]).start()
    if both_rows > 0:
        for offset in range(1, n // 2):
            where = pl.ds(2 * lax.rem(chip + offset, n // 2), 2), pl.ds(0, both_rows)
            pltpu.make_async_copy(early.at[where], targets[2].at[where], sem.at[4]).start()
    for copy in loads:
        copy.wait()
    for m in range(3):
        scales[m][...] = factors[m].reshape(scales[m].shape)
    blocks = [gains[k, i] for i in range(gains.shape[1]) for k in range(gains.shape[0])]
    line = jnp.concatenate(blocks, axis=1)
    serve[...] = line.reshape(serve.shape).astype(jnp.bfloat16)
    copies[0].wait()
    for copy in writes:
        copy.start()
    rest = source.at[0, pl.ds(1, source.shape[1] - 1)]
    second = source.at[1]
    pltpu.make_async_copy(rest, rest, sem.at[1]).wait()
    pltpu.make_async_copy(second, second, sem.at[2]).wait()
    pltpu.make_async_copy(early.at[ours], targets[2].at[ours], sem.at[3]).wait()
    if both_rows > 0:
        part = early.at[pl.ds(0, n - 2), pl.ds(0, both_rows)]
        pltpu.make_async_copy(part, part, sem.at[4]).wait()
    for copy in writes:
        copy.wait()


def place_last(early, late, before, target, sem):
    n, rows = early.shape[0], early.shape[1]
    chips = n // 2
    count, both, extra = value_split(rows)
    share = rows // count
    me = lax.axis_index("shard")
    chip, core = me // 2, lax.rem(me, 2)

    def put(source, owner, start, stop):
        if start < stop:
            where = owner, pl.ds(start * share, (stop - start) * share)
            pltpu.make_async_copy(source.at[where], target.at[where], sem.at[0]).start()

    for offset in range(1, chips):
        other = lax.rem(chip + offset, chips) * 2
        put(late, other + 1 - core, both, count)

        @pl.when(core == LEAD)
        def _():
            put(late, other + core, both, count)

        @pl.when(core != LEAD)
        def _():
            put(early, other + core, both, both + extra)
            put(late, other + core, both + extra, count)

    part = late.at[pl.ds(0, n - 2), pl.ds(both * share, rows - both * share)]
    pltpu.make_async_copy(part, part, sem.at[0]).wait()


def body(n, width, w_query, low_query, high_query, w_key, low_key, high_key, w_value, low_value, high_value, norm_train, norm_step):
    rows, columns = w_query.shape
    rank = low_query.shape[1]
    length = norm_train.shape[0]
    half = n // 4
    count = chunks_of(rows)
    raw = 1
    rounds = n.bit_length() - 1
    reach = min(rows, -(-(rows // count) * raw // 128) * 128)
    slots = len(ring_slots(half))
    block = jax.ShapeDtypeStruct((n, rows, columns), jnp.bfloat16)

    def near(value):
        return pltpu.with_memory_space_constraint(value, pltpu.VMEM)

    def far(value):
        return pltpu.with_memory_space_constraint(value, pltpu.HBM)

    ready, early, factors, gains = pl.pallas_call(
        functools.partial(gather_kernel, n, width),
        name="merge_gather",
        out_shape=[
            pltpu.VMEM((2, n, rows, columns), jnp.bfloat16),
            pltpu.VMEM((n, rows, columns), jnp.bfloat16),
            jax.ShapeDtypeStruct((3, 1, columns), jnp.float32),
            jax.ShapeDtypeStruct((width, n, 1, length), jnp.float32),
        ],
        in_specs=[ANY] * 11,
        out_specs=[pl.BlockSpec(memory_space=pltpu.VMEM)] * 2 + [HBM] * 2,
        scratch_shapes=[
            pltpu.VMEM((3, rows, columns), jnp.bfloat16),
            pltpu.VMEM((3, rows, rank), jnp.bfloat16),
            pltpu.VMEM((3, rank, columns), jnp.bfloat16),
            pltpu.VMEM((2, 1, length), jnp.float32),
            pltpu.VMEM((3, rows, columns), jnp.float32),
            pltpu.VMEM((3, 1, columns), jnp.float32),
            pltpu.VMEM((3, rounds + 1, 1, columns), jnp.float32),
            pltpu.SemaphoreType.DMA((4, 3)),
            pltpu.SemaphoreType.DMA((4,)),
            pltpu.SemaphoreType.DMA((3,)),
            pltpu.SemaphoreType.DMA((1,)),
            pltpu.SemaphoreType.DMA((3, rounds)),
            pltpu.SemaphoreType.DMA((1,)),
            pltpu.SemaphoreType.DMA((rounds,)),
            pltpu.SemaphoreType.DMA((5, slots)),
            pltpu.SemaphoreType.DMA((3,)),
            pltpu.VMEM((3, rank, rows), jnp.bfloat16),
            pltpu.VMEM((3, 1, columns), jnp.float32),
            pltpu.VMEM((width, n, 1, length), jnp.float32),
            pltpu.SemaphoreType.DMA((2,)),
            pltpu.VMEM((n, rank, reach), jnp.bfloat16),
            pltpu.VMEM((n, reach, rank), jnp.bfloat16),
            pltpu.SemaphoreType.DMA((raw, slots)),
            pltpu.SemaphoreType.DMA((1,)),
            pltpu.SemaphoreType.DMA((2 * half,)),
            pltpu.VMEM((3, rounds, 1, columns), jnp.float32),
            pltpu.SemaphoreType.DMA((2,)),
            pltpu.SemaphoreType.DMA((2, max(width - 1, 1))),
        ],
        compiler_params=pltpu.CompilerParams(
            collective_id=0, has_side_effects=True, vmem_limit_bytes=20 * 2**20
        ),
    )(
        w_query, w_key, w_value,
        low_query.T, low_key.T, low_value.T,
        high_query, high_key, high_value,
        norm_train.reshape(1, length), norm_step.reshape(1, length),
    )
    query, key, value, *small = pl.pallas_call(
        place_first,
        name="place_first",
        out_shape=[block] * 3
        + [jax.ShapeDtypeStruct((columns,), jnp.float32)] * 3
        + [jax.ShapeDtypeStruct((n * width * length,), jnp.bfloat16)],
        in_specs=[ANY] * 2 + [HBM] * 2,
        out_specs=[HBM] * 7,
        scratch_shapes=[
            pltpu.SemaphoreType.DMA((5,)),
            pltpu.VMEM((3, 1, columns), jnp.float32),
            pltpu.VMEM((width, n, 1, length), jnp.float32),
            pltpu.SemaphoreType.DMA((6,)),
            *[pltpu.VMEM((columns,), jnp.float32)] * 3,
            pltpu.VMEM((n * width * length,), jnp.bfloat16),
        ],
        compiler_params=pltpu.CompilerParams(vmem_limit_bytes=2**20),
    )(near(ready), near(early), far(factors), far(gains))
    late = pl.pallas_call(
        functools.partial(late_kernel, n),
        name="gather_late",
        out_shape=pltpu.VMEM((n, rows, columns), jnp.bfloat16),
        in_specs=[ANY, HBM],
        out_specs=pl.BlockSpec(memory_space=pltpu.VMEM),
        scratch_shapes=[
            pltpu.SemaphoreType.DMA((1,)),
            pltpu.SemaphoreType.DMA((1,)),
            pltpu.SemaphoreType.DMA((1,)),
            pltpu.SemaphoreType.DMA((5, slots)),
            pltpu.SemaphoreType.REGULAR,
            pltpu.SemaphoreType.DMA((2, max(rows // (2 * value_split(rows)[0] * LAST), 1))),
        ],
        compiler_params=pltpu.CompilerParams(
            collective_id=1, has_side_effects=True, vmem_limit_bytes=2**20
        ),
    )(near(early), far(small[0]))
    value = pl.pallas_call(
        place_last,
        name="place_last",
        out_shape=block,
        in_specs=[ANY] * 2 + [HBM],
        out_specs=HBM,
        scratch_shapes=[pltpu.SemaphoreType.DMA((1,))],
        input_output_aliases={2: 0},
        compiler_params=pltpu.CompilerParams(vmem_limit_bytes=2**20),
    )(near(early), near(late), far(value))
    return (
        *(ready.reshape(n * rows, columns) for ready in (query, key, value)),
        *small,
    )


def solution(mesh):
    n, width = mesh.shape["shard"], mesh.shape["width"]
    return jax.shard_map(
        functools.partial(body, n, width),
        mesh=mesh,
        in_specs=(
            P("shard", "width"),
            P("shard", None),
            P(None, "width"),
            P("shard", "width"),
            P("shard", None),
            P(None, "width"),
            P("shard", "width"),
            P("shard", None),
            P(None, "width"),
            P(("shard", "width")),
            P(("shard", "width")),
        ),
        out_specs=(
            P(None, "width"),
            P(None, "width"),
            P(None, "width"),
            P("width"),
            P("width"),
            P("width"),
            P(),
        ),
        check_vma=False,
    )
```

```python
import functools

import jax
import jax.numpy as jnp
from jax import lax
from jax.experimental import pallas as pl
from jax.experimental.pallas import tpu as pltpu
from jax.sharding import PartitionSpec as P

mix_rate = 0.5
LEAD = 1
SIZES = (2, 1, 2, 2, 2, 1)
JOIN = 6
BOTH = 2
EXTRA = 3
MESH = pl.DeviceIdType.MESH
ANY = pl.BlockSpec(memory_space=pl.ANY)
HBM = pl.BlockSpec(memory_space=pltpu.HBM)


def chunks_of(rows):
    for count in (5, 4, 2):
        if rows % (2 * count * 16) == 0:
            return count
    return 1


def value_split(rows):
    sizes = SIZES
    if rows % (sum(sizes) * 32) != 0:
        sizes = [1] * chunks_of(rows)
    unit = rows // sum(sizes)
    starts = [unit * sum(sizes[:i]) for i in range(len(sizes) + 1)]
    extra = min(EXTRA, len(sizes) - 1)
    return starts, min(BOTH, len(sizes) - extra), extra


def last_parts(rows):
    starts = value_split(rows)[0]
    return max((rows - starts[-2]) // 32, 1)


def ring_slots(half):
    return [
        (side, letter, hop)
        for side in range(2)
        for letter in range(2)
        for hop in range(half if side == letter else half - 1)
    ]


def gather_kernel(n, width, *refs):
    weights, lows, highs, norms = refs[0:3], refs[3:6], refs[6:9], refs[9:11]
    ready, early, small_outs = refs[11], refs[12], refs[13:15]
    w_mem, low_mem, high_mem, norm_mem, latest, scale, largest_of = refs[15:22]
    load_sem, ring_send, pair_send, max_send, max_recv, norm_send, norm_recv = refs[22:29]
    ring_sem, pair_sem, low_turned, held, gains, out_sem = refs[29:35]
    low_raw, low_far, raw_send, low_send, low_recv, max_in, line_send, line_recv = refs[35:43]
    outs = [ready.at[0], ready.at[1], early]

    rows = w_mem.shape[1]
    chips = n // 2
    half = chips // 2
    count = chunks_of(rows)
    piece = rows // (2 * count)
    starts, both, extra = value_split(rows)
    shared = 2 * count + both
    raw = 1
    raw_rows = 2 * piece * raw
    reach = low_raw.shape[2]
    rounds = n.bit_length() - 1
    assert n == 1 << rounds

    me = lax.axis_index("shard")
    line = lax.axis_index("width")
    chip, core = me // 2, lax.rem(me, 2)
    sibling = me + 1 - 2 * core
    slots = ring_slots(half)

    def turned(c):
        return jnp.where(c < half, c, chips + half - 1 - c)

    place = turned(chip)

    def shard_at(offset):
        return turned(lax.rem(place + offset + 2 * chips, chips)) * 2 + core

    def group(r):
        return lax.div(me, 1 << r)

    def partner(r):
        return me + (1 << r) * (1 - 2 * lax.rem(group(r), 2))

    def load(source, target, m, slot):
        return pltpu.make_async_copy(source, target, load_sem.at[m, slot])

    first = load(weights[0].at[pl.ds(0, raw_rows)], w_mem.at[0, pl.ds(0, raw_rows)], 3, 2)
    loads = []
    for m in range(3):
        parts = [load(lows[m], low_turned.at[m], m, 0), load(highs[m], high_mem.at[m], m, 1)]
        if m > 0:
            parts.append(load(weights[m], w_mem.at[m], m, 2))
        elif raw_rows < rows:
            rest = pl.ds(raw_rows, rows - raw_rows)
            parts.append(load(weights[0].at[rest], w_mem.at[0, rest], m, 2))
        loads.append(parts)
    norm_loads = [load(norms[i], norm_mem.at[i], 3, i) for i in range(2)]
    first.start()

    barrier = pltpu.get_barrier_semaphore()

    def greet(axis, index):
        pl.semaphore_signal(barrier, inc=1, device_id={axis: index}, device_id_type=MESH)

    greet("shard", shard_at(1))
    greet("shard", shard_at(-1))
    for r in range(rounds):
        greet("shard", partner(r))

    @pl.when(line > 0)
    def _():
        greet("width", line - 1)

    @pl.when(line < width - 1)
    def _():
        greet("width", line + 1)

    for parts in loads:
        for copy in parts:
            copy.start()
    for copy in norm_loads:
        copy.start()

    tile = piece

    def merge(m):
        for copy in loads[m]:
            copy.wait()
        low_mem[m] = low_turned[m].T

        def body(t, largest):
            at = pl.ds(pl.multiple_of(t * tile, tile), tile)
            value = w_mem[m, at, :].astype(jnp.float32) + mix_rate * jnp.dot(
                low_mem[m, at, :], high_mem[m], preferred_element_type=jnp.float32
            )
            latest[m, at, :] = value
            sizes = jnp.abs(value).reshape(tile // 8, 8, value.shape[1])
            return jnp.maximum(largest, jnp.max(sizes, axis=0))

        largest = lax.fori_loop(0, rows // tile, body, jnp.zeros((8, w_mem.shape[2]), jnp.float32))
        largest_of[m, 0] = jnp.max(largest, axis=0, keepdims=True)
        max_copy(m, 0).start()

    def max_copy(m, r):
        return pltpu.make_async_remote_copy(
            src_ref=largest_of.at[m, r],
            dst_ref=max_in.at[m, r],
            send_sem=max_send.at[0],
            recv_sem=max_recv.at[m, r],
            device_id={"shard": partner(r)},
            device_id_type=MESH,
        )

    met = [0, 0, 0]

    def advance(m):
        r = met[m]
        if r == rounds:
            return
        max_copy(m, r).wait_recv()
        largest_of[m, r + 1] = jnp.maximum(largest_of[m, r], max_in[m, r])
        met[m] = r + 1
        if r + 1 < rounds:
            max_copy(m, r + 1).start()

    def settle(m):
        while met[m] < rounds:
            advance(m)
        factor = largest_of[m, rounds]
        held[m] = factor
        scale[m] = 1.0 / factor

    def gain_copy(r):
        return pltpu.make_async_remote_copy(
            src_ref=gains.at[line, pl.ds(group(r) * (1 << r), 1 << r)],
            dst_ref=gains.at[line, pl.ds(group(r) * (1 << r), 1 << r)],
            send_sem=norm_send.at[0],
            recv_sem=norm_recv.at[r],
            device_id={"shard": partner(r)},
            device_id_type=MESH,
        )

    def gain_arrival(r):
        theirs = gains.at[line, pl.ds(lax.div(partner(r), 1 << r) * (1 << r), 1 << r)]
        pltpu.make_async_copy(theirs, theirs, norm_recv.at[r]).wait()

    def line_copy(way, s):
        sign = 1 - 2 * way
        block = gains.at[line - sign * s]
        return pltpu.make_async_remote_copy(
            src_ref=block,
            dst_ref=block,
            send_sem=line_send.at[way],
            recv_sem=line_recv.at[way, s],
            device_id={"width": line + sign},
            device_id_type=MESH,
        )

    def inside(value):
        return (value >= 0) & (value < width)

    def line_start(way, s):
        sign = 1 - 2 * way

        @pl.when(inside(line - sign * s) & inside(line + sign))
        def _():
            line_copy(way, s).start()

    def line_finish(way, s):
        sign = 1 - 2 * way

        @pl.when(inside(line - sign * (s + 1)))
        def _():
            block = gains.at[line - sign * (s + 1)]
            pltpu.make_async_copy(block, block, line_recv.at[way, s]).wait()

        @pl.when(inside(line - sign * s) & inside(line + sign))
        def _():
            line_copy(way, s).wait_send()

    def gain_first():
        for copy in norm_loads:
            copy.wait()
        gains[line, me] = norm_mem[0] + norm_mem[1]
        gain_copy(0).start()

    def gain_round(r):
        gain_arrival(r)
        if r + 1 < rounds:
            gain_copy(r + 1).start()
        elif width > 1:
            for way in range(2):
                line_start(way, 0)

    def gain_line(s):
        for way in range(2):
            line_finish(way, s)
        if s + 1 < width - 1:
            for way in range(2):
                line_start(way, s + 1)

    errands = [gain_first]
    errands += [functools.partial(gain_round, r) for r in range(rounds)]
    errands += [functools.partial(gain_line, s) for s in range(width - 1)]

    def rows_of(letter, k):
        if k < 2 * count:
            return pl.ds((2 * (k % count) + letter) * piece, piece)
        first, stop = starts[k - 2 * count : k - 2 * count + 2]
        return pl.ds(first + letter * (stop - first) // 2, (stop - first) // 2)

    def matrix_of(k):
        return min(k // count, 2)

    def finish(k):
        m = k // count
        at = pl.ds(2 * (k % count) * piece, 2 * piece)
        outs[m][me, at, :] = (latest[m, at, :] * scale[m]).astype(jnp.bfloat16)

    def view(k, letter, owner):
        return outs[matrix_of(k)].at[owner, rows_of(letter, k)]

    def landing(k, side, letter, hop):
        return ring_sem.at[k % ring_sem.shape[0], slots.index((side, letter, hop))]

    def ring_copy(k, side, letter, hop):
        sign = 1 - 2 * side
        owner = shard_at(-sign * hop)
        where = view(k, letter, owner)
        source = where
        if k < raw and hop == 0:
            source = w_mem.at[0, rows_of(letter, k)]
        sent = ring_send.at[matrix_of(k)]
        if k < raw:
            sent = ring_send.at[3]
            if hop > 0:
                sent = raw_send.at[k, slots.index((side, letter, hop))]
        return pltpu.make_async_remote_copy(
            src_ref=source,
            dst_ref=where,
            send_sem=sent,
            recv_sem=landing(k, side, letter, hop),
            device_id={"shard": shard_at(sign)},
            device_id_type=MESH,
        )

    def low_copy(side, hop):
        sign = 1 - 2 * side
        where = low_raw.at[shard_at(-sign * hop)]
        return pltpu.make_async_remote_copy(
            src_ref=low_turned.at[0, :, pl.ds(0, reach)] if hop == 0 else where,
            dst_ref=where,
            send_sem=low_send.at[0],
            recv_sem=low_recv.at[side * half + hop],
            device_id={"shard": shard_at(sign)},
            device_id_type=MESH,
        )

    def ring_start(k, side, letter, hop):
        ring_copy(k, side, letter, hop).start()

    def low_arrival(side, hop):
        sign = 1 - 2 * side
        owner = shard_at(-sign * (hop + 1))
        where = low_raw.at[owner]
        pltpu.make_async_copy(where, where, low_recv.at[side * half + hop]).wait()
        if hop + 1 < hops(side, 0):
            low_copy(side, hop + 1).start()
        low_far[owner] = low_raw[owner].T

    def ring_arrival(k, side, letter, hop):
        sign = 1 - 2 * side
        owner = shard_at(-sign * (hop + 1))
        where = view(k, letter, owner)
        pltpu.make_async_copy(where, where, landing(k, side, letter, hop)).wait()
        return owner

    def pair_copy(k, letter, owner):
        where = view(k, letter, owner)
        pltpu.make_async_remote_copy(
            src_ref=where,
            dst_ref=where,
            send_sem=pair_send.at[matrix_of(k) // 2 * 2],
            recv_sem=pair_sem.at[matrix_of(k) // 2 * 2],
            device_id={"shard": sibling},
            device_id_type=MESH,
        ).start()

    def pair_own():
        for k in range(2 * count, 3 * count):
            finish(k)
        return pltpu.make_async_remote_copy(
            src_ref=early.at[me],
            dst_ref=early.at[me],
            send_sem=pair_send.at[1],
            recv_sem=pair_sem.at[1],
            device_id={"shard": sibling},
            device_id_type=MESH,
        )

    def by_role(k):
        if k < shared:
            return lambda act: act()
        return pl.when(core != LEAD)

    def hops(side, letter):
        return half if side == letter else half - 1

    pending = []

    def landed(k, side, letter, hop, owner):
        if k < raw:
            pending.append((k, side, letter, hop, owner))
        elif k < shared:
            pair_copy(k, letter, owner)

    low_seen = set()

    def absorb():
        for k, side, letter, hop, owner in pending:
            if hop + 1 < hops(side, letter):
                ring_copy(k, side, letter, hop + 1).wait_send()
            from_side, from_hop = (side, hop) if hop < hops(side, 0) else (0, half - 1)
            for h in range(from_hop + 1):
                if (from_side, h) not in low_seen:
                    low_seen.add((from_side, h))
                    low_arrival(from_side, h)
            at = rows_of(letter, k)
            value = ready[0, owner, at, :].astype(jnp.float32) + mix_rate * jnp.dot(
                low_far[owner, at, :], high_mem[0], preferred_element_type=jnp.float32
            )
            ready[0, owner, at, :] = (value * scale[0]).astype(jnp.bfloat16)
            pair_copy(k, letter, owner)
        pending.clear()

    small_writes = [
        pltpu.make_async_copy(held, small_outs[0], out_sem.at[0]),
        pltpu.make_async_copy(gains, small_outs[1], out_sem.at[1]),
    ]
    first.wait()
    pl.semaphore_wait(
        barrier,
        2 + rounds + (line > 0).astype(jnp.int32) + (line < width - 1).astype(jnp.int32),
    )

    own_value = []
    closed = set()
    last_hops = [s for side in range(2) for s in slots[::-1] if s[0] == side and s[2] == hops(*s[0:2]) - 1]

    def pass_on(k, hop):
        for side in range(2):
            owner = ring_arrival(k, side, side, hop)
            ring_start(k, side, side, hop + 1)
            landed(k, side, side, hop, owner)

    def close(k, side, letter, hop):
        closed.add((k, side, letter))
        landed(k, side, letter, hop, ring_arrival(k, side, letter, hop))

    for j in range(shared + extra + half):
        def first_own():
            for side in range(2):
                if hops(side, side) > 0:
                    ring_start(j, side, side, 0)

        if j < shared + extra and j != shared:
            by_role(j)(first_own)
        if j == 0:
            merge(0)
            advance(0)
        for hop in range(half - 1):
            k = j - 1 - hop
            if (k, hop) == (0, 0):
                continue
            if 0 <= k < shared + extra:
                by_role(k)(functools.partial(pass_on, k, hop))

        if j == shared and extra > 0:
            by_role(j)(first_own)
        if j < shared + extra:

            @by_role(j)
            def _():
                for side in range(2):
                    if hops(side, 1 - side) > 0:
                        ring_start(j, side, 1 - side, 0)

        for hop in range(half - 2):
            k = j - 1 - hop
            if 0 <= k < shared + extra:

                @by_role(k)
                def _():
                    for side in range(2):
                        owner = ring_arrival(k, side, 1 - side, hop)
                        ring_start(k, side, 1 - side, hop + 1)
                        landed(k, side, 1 - side, hop, owner)

        if raw <= j < 2 * count:
            for letter in range(2):
                pair_copy(j, letter, me)
        if j == 0:
            for side in range(2):
                if hops(side, 0) > 0:
                    low_copy(side, 0).start()
            advance(0)
            if half > 1:
                pass_on(0, 0)
        if j in (1, 2):
            merge(j)
        for m in range(1, 3):
            if j > m and met[m] < rounds:
                advance(m)
        if 1 <= j < half:
            for side in range(2):
                if j - 1 < hops(side, 0):
                    low_seen.add((side, j - 1))
                    low_arrival(side, j - 1)
        if j > 0 and errands:
            errands.pop(0)()
        if j == min(raw + rounds + 2, 2 * count - 1):
            settle(2)
            own_value.append(pair_own())
            own_value[0].start()
        if j == 2 * count - 1:
            while errands:
                errands.pop(0)()
            for copy in small_writes:
                copy.start()
        if raw <= j + 1 < 2 * count:
            if j + 1 == raw:
                settle(0)
            if (j + 1) % count == 0:
                settle((j + 1) // count)
            finish(j + 1)
        for side, letter, hop in last_hops:
            k = j - 1 - hop
            if 0 <= k < shared + extra and (k, side, letter) not in closed:
                by_role(k)(functools.partial(close, k, side, letter, hop))
        if j == shared and half == 2:
            for side in range(2):
                close(shared - 1, side, side, half - 1)
        if j == raw:
            for k in range(raw):
                finish(k)
                for letter in range(2):
                    pair_copy(k, letter, me)
        if j >= raw:
            absorb()

    theirs = ready.at[:, pl.ds(0, chips)]
    pltpu.make_async_copy(theirs, theirs, pair_sem.at[0]).wait()
    pltpu.make_async_copy(theirs, theirs, pair_send.at[0]).wait()
    pltpu.make_async_copy(early.at[sibling], early.at[sibling], pair_sem.at[1]).wait()
    own_value[0].wait_send()

    def value_part(share):
        return early.at[pl.ds(0, chips - 1), pl.ds(0, starts[share])]

    if both > 0:
        theirs = value_part(both)
        pltpu.make_async_copy(theirs, theirs, pair_sem.at[2]).wait()
        pltpu.make_async_copy(theirs, theirs, pair_send.at[2]).wait()
    for m in range(2):
        kept = raw_rows if m == 0 else 0
        if kept < rows:
            sent = outs[m].at[pl.ds(0, chips - 1), pl.ds(kept, rows - kept)]
            pltpu.make_async_copy(sent, sent, ring_send.at[m]).wait()
    sent = ready.at[0, pl.ds(0, len([s for s in slots if s[2] == 0]) // 2), pl.ds(0, raw_rows)]
    pltpu.make_async_copy(sent, sent, ring_send.at[3]).wait()
    for share, mine in ((both, core == LEAD), (both + extra, core != LEAD)):
        if share > 0:

            @pl.when(mine)
            def _():
                sent = value_part(share)
                pltpu.make_async_copy(sent, sent, ring_send.at[2]).wait()

    pltpu.make_async_copy(max_in, max_in, max_send.at[0]).wait()
    sent = low_raw.at[pl.ds(0, chips - 1)]
    pltpu.make_async_copy(sent, sent, low_send.at[0]).wait()
    sent = gains.at[line, pl.ds(0, n - 1)]
    pltpu.make_async_copy(sent, sent, norm_send.at[0]).wait()
    for copy in small_writes:
        copy.wait()


def late_kernel(n, *refs):
    early, late = refs[0], refs[2]
    ring_send, pair_send, pair_sem, ring_sem, joined, last_sem = refs[3:9]
    parts = last_sem.shape[1]
    rows = early.shape[1]
    chips = n // 2
    half = chips // 2
    starts, both, extra = value_split(rows)
    count = len(starts) - 1
    slots = ring_slots(half)

    me = lax.axis_index("shard")
    chip, core = me // 2, lax.rem(me, 2)
    sibling = me + 1 - 2 * core

    def turned(c):
        return jnp.where(c < half, c, chips + half - 1 - c)

    place = turned(chip)

    def shard_at(offset):
        return turned(lax.rem(place + offset + 2 * chips, chips)) * 2 + core

    def hops(side, letter):
        return half if side == letter else half - 1

    def view(ref, k, letter, owner, part=None):
        size = (starts[k + 1] - starts[k]) // 2
        first = starts[k] + letter * size
        if part is not None:
            size = size // parts
            first += part * size
        return ref.at[owner, pl.ds(first, size)]

    def landing(k, side, letter, hop, part=None):
        if part is not None:
            return last_sem.at[side, part]
        return ring_sem.at[k % ring_sem.shape[0], slots.index((side, letter, hop))]

    def cut(k, side, letter, hop):
        if k == count - 1 and side == letter and hop == half - 1 and hop > 0 and parts > 1:
            return range(parts)
        return [None]

    def ring_start(k, side, letter, hop):
        sign = 1 - 2 * side
        owner = shard_at(-sign * hop)
        for part in cut(k, side, letter, hop):
            pltpu.make_async_remote_copy(
                src_ref=view(early if hop == 0 else late, k, letter, owner, part),
                dst_ref=view(late, k, letter, owner, part),
                send_sem=ring_send.at[0],
                recv_sem=landing(k, side, letter, hop, part),
                device_id={"shard": shard_at(sign)},
                device_id_type=MESH,
            ).start()

    def ring_arrival(k, side, letter, hop, part=None):
        sign = 1 - 2 * side
        where = view(late, k, letter, shard_at(-sign * (hop + 1)), part)
        pltpu.make_async_copy(where, where, landing(k, side, letter, hop, part)).wait()
        return where

    def to_sibling(source, target):
        pltpu.make_async_remote_copy(
            src_ref=source,
            dst_ref=target,
            send_sem=pair_send.at[0],
            recv_sem=pair_sem.at[0],
            device_id={"shard": sibling},
            device_id_type=MESH,
        ).start()

    barrier = pltpu.get_barrier_semaphore()
    for offset in (1, -1):
        pl.semaphore_signal(
            barrier, inc=1, device_id={"shard": shard_at(offset)}, device_id_type=MESH
        )

    def run(first, join):
        waiting = []

        def landed(where):
            if join is not None and not joined_at:
                waiting.append(where)
            else:
                to_sibling(where, where)

        joined_at = []
        for j in range(first, count + half):
            if j < count:
                for side in range(2):
                    if hops(side, side) > 0:
                        ring_start(j, side, side, 0)
            for hop in range(half - 1):
                k = j - 1 - hop
                if first <= k < count:
                    for side in range(2):
                        where = ring_arrival(k, side, side, hop)
                        ring_start(k, side, side, hop + 1)
                        landed(where)
            if j < count:
                for side in range(2):
                    if hops(side, 1 - side) > 0:
                        ring_start(j, side, 1 - side, 0)
            for hop in range(half - 2):
                k = j - 1 - hop
                if first <= k < count:
                    for side in range(2):
                        where = ring_arrival(k, side, 1 - side, hop)
                        ring_start(k, side, 1 - side, hop + 1)
                        landed(where)
            if j == join:
                pl.semaphore_wait(joined, 1)
                joined_at.append(j)
                for where in waiting:
                    to_sibling(where, where)
            ends = [
                (j - hops(side, letter), side, letter, hops(side, letter) - 1)
                for flip in range(2)
                for side in range(2)
                for letter in (side ^ flip,)
            ]
            ends = [s for s in ends if s[3] >= 0 and first <= s[0] < count]
            for part in range(parts):
                for s in ends:
                    if part < len(cut(*s)):
                        landed(ring_arrival(*s, cut(*s)[part]))
        if first < count:
            sent = late.at[pl.ds(0, chips - 1), pl.ds(0, rows - starts[first])]
            pltpu.make_async_copy(sent, sent, ring_send.at[0]).wait()

    @pl.when(core == LEAD)
    def _():
        pl.semaphore_signal(barrier, inc=1, device_id={"shard": sibling}, device_id_type=MESH)
        pl.semaphore_wait(barrier, 2)
        run(both, JOIN)

    @pl.when(core != LEAD)
    def _():
        pl.semaphore_wait(barrier, 3)
        pl.semaphore_signal(joined, inc=1, device_id={"shard": sibling}, device_id_type=MESH)
        if extra > 0:
            for offset in range(1, chips):
                owner = shard_at(offset)
                at = pl.ds(starts[both], starts[both + extra] - starts[both])
                to_sibling(early.at[owner, at], late.at[owner, at])
        run(both + extra, None)

    theirs = late.at[pl.ds(0, chips - 1), pl.ds(0, rows - starts[both])]
    pltpu.make_async_copy(theirs, theirs, pair_sem.at[0]).wait()
    pltpu.make_async_copy(theirs, theirs, pair_send.at[0]).wait()


def place_first(*refs):
    source, early, small = refs[0], refs[1], refs[2:4]
    targets, finals, sem = refs[4:7], refs[7:11], refs[11]
    factors, gains, small_sem = refs[12], refs[13], refs[14]
    scales, serve = refs[15:18], refs[18]
    writes = [
        pltpu.make_async_copy(refs[15 + i], finals[i], small_sem.at[2 + i]) for i in range(4)
    ]
    loads = [
        pltpu.make_async_copy(small[i], refs[12 + i], small_sem.at[i]) for i in range(2)
    ]
    n, rows = early.shape[0], early.shape[1]
    starts, both, _ = value_split(rows)
    both_rows = starts[both]
    chip = lax.div(lax.axis_index("shard"), 2)
    copies = [
        pltpu.make_async_copy(source.at[m, i], targets[m].at[i], sem.at[2 if m else min(i, 1)])
        for m in range(2)
        for i in range(source.shape[1])
    ]
    for copy in loads + copies:
        copy.start()
    ours = pl.ds(2 * chip, 2)
    pltpu.make_async_copy(early.at[ours], targets[2].at[ours], sem.at[3]).start()
    if both_rows > 0:
        for offset in range(1, n // 2):
            where = pl.ds(2 * lax.rem(chip + offset, n // 2), 2), pl.ds(0, both_rows)
            pltpu.make_async_copy(early.at[where], targets[2].at[where], sem.at[4]).start()
    for copy in loads:
        copy.wait()
    for m in range(3):
        scales[m][...] = factors[m].reshape(scales[m].shape)
    blocks = [gains[k, i] for i in range(gains.shape[1]) for k in range(gains.shape[0])]
    line = jnp.concatenate(blocks, axis=1)
    serve[...] = line.reshape(serve.shape).astype(jnp.bfloat16)
    copies[0].wait()
    for copy in writes:
        copy.start()
    rest = source.at[0, pl.ds(1, source.shape[1] - 1)]
    second = source.at[1]
    pltpu.make_async_copy(rest, rest, sem.at[1]).wait()
    pltpu.make_async_copy(second, second, sem.at[2]).wait()
    pltpu.make_async_copy(early.at[ours], targets[2].at[ours], sem.at[3]).wait()
    if both_rows > 0:
        part = early.at[pl.ds(0, n - 2), pl.ds(0, both_rows)]
        pltpu.make_async_copy(part, part, sem.at[4]).wait()
    for copy in writes:
        copy.wait()


def place_last(early, late, before, target, sem):
    n, rows = early.shape[0], early.shape[1]
    chips = n // 2
    starts, both, extra = value_split(rows)
    me = lax.axis_index("shard")
    chip, core = me // 2, lax.rem(me, 2)

    def put(source, owner, start, stop):
        if start < stop:
            where = owner, pl.ds(starts[start], starts[stop] - starts[start])
            pltpu.make_async_copy(source.at[where], target.at[where], sem.at[0]).start()

    count = len(starts) - 1
    for offset in range(1, chips):
        other = lax.rem(chip + offset, chips) * 2
        put(late, other + 1 - core, both, count)

        @pl.when(core == LEAD)
        def _():
            put(late, other + core, both, count)

        @pl.when(core != LEAD)
        def _():
            put(early, other + core, both, both + extra)
            put(late, other + core, both + extra, count)

    part = late.at[pl.ds(0, n - 2), pl.ds(starts[both], rows - starts[both])]
    pltpu.make_async_copy(part, part, sem.at[0]).wait()


def body(n, width, w_query, low_query, high_query, w_key, low_key, high_key, w_value, low_value, high_value, norm_train, norm_step):
    rows, columns = w_query.shape
    rank = low_query.shape[1]
    length = norm_train.shape[0]
    half = n // 4
    count = chunks_of(rows)
    raw = 1
    rounds = n.bit_length() - 1
    reach = min(rows, -(-(rows // count) * raw // 128) * 128)
    slots = len(ring_slots(half))
    starts, both, _ = value_split(rows)
    block = jax.ShapeDtypeStruct((n, rows, columns), jnp.bfloat16)

    def near(value):
        return pltpu.with_memory_space_constraint(value, pltpu.VMEM)

    def far(value):
        return pltpu.with_memory_space_constraint(value, pltpu.HBM)

    ready, early, factors, gains = pl.pallas_call(
        functools.partial(gather_kernel, n, width),
        name="merge_gather",
        out_shape=[
            pltpu.VMEM((2, n, rows, columns), jnp.bfloat16),
            pltpu.VMEM((n, rows, columns), jnp.bfloat16),
            jax.ShapeDtypeStruct((3, 1, columns), jnp.float32),
            jax.ShapeDtypeStruct((width, n, 1, length), jnp.float32),
        ],
        in_specs=[ANY] * 11,
        out_specs=[pl.BlockSpec(memory_space=pltpu.VMEM)] * 2 + [HBM] * 2,
        scratch_shapes=[
            pltpu.VMEM((3, rows, columns), jnp.bfloat16),
            pltpu.VMEM((3, rows, rank), jnp.bfloat16),
            pltpu.VMEM((3, rank, columns), jnp.bfloat16),
            pltpu.VMEM((2, 1, length), jnp.float32),
            pltpu.VMEM((3, rows, columns), jnp.float32),
            pltpu.VMEM((3, 1, columns), jnp.float32),
            pltpu.VMEM((3, rounds + 1, 1, columns), jnp.float32),
            pltpu.SemaphoreType.DMA((4, 3)),
            pltpu.SemaphoreType.DMA((4,)),
            pltpu.SemaphoreType.DMA((3,)),
            pltpu.SemaphoreType.DMA((1,)),
            pltpu.SemaphoreType.DMA((3, rounds)),
            pltpu.SemaphoreType.DMA((1,)),
            pltpu.SemaphoreType.DMA((rounds,)),
            pltpu.SemaphoreType.DMA((5, slots)),
            pltpu.SemaphoreType.DMA((3,)),
            pltpu.VMEM((3, rank, rows), jnp.bfloat16),
            pltpu.VMEM((3, 1, columns), jnp.float32),
            pltpu.VMEM((width, n, 1, length), jnp.float32),
            pltpu.SemaphoreType.DMA((2,)),
            pltpu.VMEM((n, rank, reach), jnp.bfloat16),
            pltpu.VMEM((n, reach, rank), jnp.bfloat16),
            pltpu.SemaphoreType.DMA((raw, slots)),
            pltpu.SemaphoreType.DMA((1,)),
            pltpu.SemaphoreType.DMA((2 * half,)),
            pltpu.VMEM((3, rounds, 1, columns), jnp.float32),
            pltpu.SemaphoreType.DMA((2,)),
            pltpu.SemaphoreType.DMA((2, max(width - 1, 1))),
        ],
        compiler_params=pltpu.CompilerParams(
            collective_id=0, has_side_effects=True, vmem_limit_bytes=20 * 2**20
        ),
    )(
        w_query, w_key, w_value,
        low_query.T, low_key.T, low_value.T,
        high_query, high_key, high_value,
        norm_train.reshape(1, length), norm_step.reshape(1, length),
    )
    query, key, value, *small = pl.pallas_call(
        place_first,
        name="place_first",
        out_shape=[block] * 3
        + [jax.ShapeDtypeStruct((columns,), jnp.float32)] * 3
        + [jax.ShapeDtypeStruct((n * width * length,), jnp.bfloat16)],
        in_specs=[ANY] * 2 + [HBM] * 2,
        out_specs=[HBM] * 7,
        scratch_shapes=[
            pltpu.SemaphoreType.DMA((5,)),
            pltpu.VMEM((3, 1, columns), jnp.float32),
            pltpu.VMEM((width, n, 1, length), jnp.float32),
            pltpu.SemaphoreType.DMA((6,)),
            *[pltpu.VMEM((columns,), jnp.float32)] * 3,
            pltpu.VMEM((n * width * length,), jnp.bfloat16),
        ],
        compiler_params=pltpu.CompilerParams(vmem_limit_bytes=2**20),
    )(near(ready), near(early), far(factors), far(gains))
    late = pl.pallas_call(
        functools.partial(late_kernel, n),
        name="gather_late",
        out_shape=pltpu.VMEM((n, rows, columns), jnp.bfloat16),
        in_specs=[ANY, HBM],
        out_specs=pl.BlockSpec(memory_space=pltpu.VMEM),
        scratch_shapes=[
            pltpu.SemaphoreType.DMA((1,)),
            pltpu.SemaphoreType.DMA((1,)),
            pltpu.SemaphoreType.DMA((1,)),
            pltpu.SemaphoreType.DMA((len(starts) - 1 - both, slots)),
            pltpu.SemaphoreType.REGULAR,
            pltpu.SemaphoreType.DMA((2, last_parts(rows))),
        ],
        compiler_params=pltpu.CompilerParams(
            collective_id=1, has_side_effects=True, vmem_limit_bytes=2**20
        ),
    )(near(early), far(small[0]))
    value = pl.pallas_call(
        place_last,
        name="place_last",
        out_shape=block,
        in_specs=[ANY] * 2 + [HBM],
        out_specs=HBM,
        scratch_shapes=[pltpu.SemaphoreType.DMA((1,))],
        input_output_aliases={2: 0},
        compiler_params=pltpu.CompilerParams(vmem_limit_bytes=2**20),
    )(near(early), near(late), far(value))
    return (
        *(ready.reshape(n * rows, columns) for ready in (query, key, value)),
        *small,
    )


def solution(mesh):
    n, width = mesh.shape["shard"], mesh.shape["width"]
    return jax.shard_map(
        functools.partial(body, n, width),
        mesh=mesh,
        in_specs=(
            P("shard", "width"),
            P("shard", None),
            P(None, "width"),
            P("shard", "width"),
            P("shard", None),
            P(None, "width"),
            P("shard", "width"),
            P("shard", None),
            P(None, "width"),
            P(("shard", "width")),
            P(("shard", "width")),
        ),
        out_specs=(
            P(None, "width"),
            P(None, "width"),
            P(None, "width"),
            P("width"),
            P("width"),
            P("width"),
            P(),
        ),
        check_vma=False,
    )
```

```python
import functools

import jax
import jax.numpy as jnp
from jax import lax
from jax.experimental import pallas as pl
from jax.experimental.pallas import tpu as pltpu
from jax.sharding import PartitionSpec as P

mix_rate = 0.5
LEAD = 1
SIZES = (2, 1, 2, 2, 2, 1)
JOIN = 6
BOTH = 2
EXTRA = 3
MESH = pl.DeviceIdType.MESH
ANY = pl.BlockSpec(memory_space=pl.ANY)
HBM = pl.BlockSpec(memory_space=pltpu.HBM)


def chunks_of(rows):
    for count in (5, 4, 2):
        if rows % (2 * count * 16) == 0:
            return count
    return 1


def value_split(rows):
    sizes = SIZES
    if rows % (sum(sizes) * 32) != 0:
        sizes = [1] * chunks_of(rows)
    unit = rows // sum(sizes)
    starts = [unit * sum(sizes[:i]) for i in range(len(sizes) + 1)]
    extra = min(EXTRA, len(sizes) - 1)
    return starts, min(BOTH, len(sizes) - extra), extra


def last_parts(rows):
    starts = value_split(rows)[0]
    return max((rows - starts[-2]) // 32, 1)


def ring_slots(half):
    return [
        (side, letter, hop)
        for side in range(2)
        for letter in range(2)
        for hop in range(half if side == letter else half - 1)
    ]


def gather_kernel(n, width, *refs):
    weights, lows, highs, norms = refs[0:3], refs[3:6], refs[6:9], refs[9:11]
    ready, early, small_outs = refs[11], refs[12], refs[13:15]
    w_mem, low_mem, high_mem, norm_mem, latest, scale, largest_of = refs[15:22]
    load_sem, ring_send, pair_send, max_send, max_recv, norm_send, norm_recv = refs[22:29]
    ring_sem, pair_sem, low_turned, held, gains, out_sem = refs[29:35]
    low_raw, low_far, raw_send, low_send, low_recv, max_in, line_send, line_recv = refs[35:43]
    outs = [ready.at[0], ready.at[1], early]

    rows = w_mem.shape[1]
    chips = n // 2
    half = chips // 2
    count = chunks_of(rows)
    piece = rows // (2 * count)
    starts, both, extra = value_split(rows)
    shared = 2 * count + both
    raw = 1
    raw_rows = 2 * piece * raw
    reach = low_raw.shape[2]
    rounds = n.bit_length() - 1
    assert n == 1 << rounds

    me = lax.axis_index("shard")
    line = lax.axis_index("width")
    chip, core = me // 2, lax.rem(me, 2)
    sibling = me + 1 - 2 * core
    slots = ring_slots(half)

    def turned(c):
        return jnp.where(c < half, c, chips + half - 1 - c)

    place = turned(chip)

    def shard_at(offset):
        return turned(lax.rem(place + offset + 2 * chips, chips)) * 2 + core

    def group(r):
        return lax.div(me, 1 << r)

    def partner(r):
        return me + (1 << r) * (1 - 2 * lax.rem(group(r), 2))

    def load(source, target, m, slot):
        return pltpu.make_async_copy(source, target, load_sem.at[m, slot])

    first = load(weights[0].at[pl.ds(0, raw_rows)], w_mem.at[0, pl.ds(0, raw_rows)], 3, 2)
    loads = []
    for m in range(3):
        parts = [load(lows[m], low_turned.at[m], m, 0), load(highs[m], high_mem.at[m], m, 1)]
        if m > 0:
            parts.append(load(weights[m], w_mem.at[m], m, 2))
        elif raw_rows < rows:
            rest = pl.ds(raw_rows, rows - raw_rows)
            parts.append(load(weights[0].at[rest], w_mem.at[0, rest], m, 2))
        loads.append(parts)
    norm_loads = [load(norms[i], norm_mem.at[i], 3, i) for i in range(2)]
    barrier = pltpu.get_barrier_semaphore()

    def greet(axis, index):
        pl.semaphore_signal(barrier, inc=1, device_id={axis: index}, device_id_type=MESH)

    greet("shard", shard_at(1))
    greet("shard", shard_at(-1))
    for r in range(rounds):
        greet("shard", partner(r))

    @pl.when(line > 0)
    def _():
        greet("width", line - 1)

    @pl.when(line < width - 1)
    def _():
        greet("width", line + 1)

    first.start()
    for parts in loads:
        for copy in parts:
            copy.start()
    for copy in norm_loads:
        copy.start()

    tile = piece

    def merge(m):
        for copy in loads[m]:
            copy.wait()
        low_mem[m] = low_turned[m].T

        def body(t, largest):
            at = pl.ds(pl.multiple_of(t * tile, tile), tile)
            value = w_mem[m, at, :].astype(jnp.float32) + mix_rate * jnp.dot(
                low_mem[m, at, :], high_mem[m], preferred_element_type=jnp.float32
            )
            latest[m, at, :] = value
            sizes = jnp.abs(value).reshape(tile // 8, 8, value.shape[1])
            return jnp.maximum(largest, jnp.max(sizes, axis=0))

        largest = lax.fori_loop(0, rows // tile, body, jnp.zeros((8, w_mem.shape[2]), jnp.float32))
        largest_of[m, 0] = jnp.max(largest, axis=0, keepdims=True)
        max_copy(m, 0).start()

    def max_copy(m, r):
        return pltpu.make_async_remote_copy(
            src_ref=largest_of.at[m, r],
            dst_ref=max_in.at[m, r],
            send_sem=max_send.at[0],
            recv_sem=max_recv.at[m, r],
            device_id={"shard": partner(r)},
            device_id_type=MESH,
        )

    met = [0, 0, 0]

    def advance(m):
        r = met[m]
        if r == rounds:
            return
        max_copy(m, r).wait_recv()
        largest_of[m, r + 1] = jnp.maximum(largest_of[m, r], max_in[m, r])
        met[m] = r + 1
        if r + 1 < rounds:
            max_copy(m, r + 1).start()

    def settle(m):
        while met[m] < rounds:
            advance(m)
        factor = largest_of[m, rounds]
        held[m] = factor
        scale[m] = 1.0 / factor

    def gain_copy(r):
        return pltpu.make_async_remote_copy(
            src_ref=gains.at[line, pl.ds(group(r) * (1 << r), 1 << r)],
            dst_ref=gains.at[line, pl.ds(group(r) * (1 << r), 1 << r)],
            send_sem=norm_send.at[0],
            recv_sem=norm_recv.at[r],
            device_id={"shard": partner(r)},
            device_id_type=MESH,
        )

    def gain_arrival(r):
        theirs = gains.at[line, pl.ds(lax.div(partner(r), 1 << r) * (1 << r), 1 << r)]
        pltpu.make_async_copy(theirs, theirs, norm_recv.at[r]).wait()

    def line_copy(way, s):
        sign = 1 - 2 * way
        block = gains.at[line - sign * s]
        return pltpu.make_async_remote_copy(
            src_ref=block,
            dst_ref=block,
            send_sem=line_send.at[way],
            recv_sem=line_recv.at[way, s],
            device_id={"width": line + sign},
            device_id_type=MESH,
        )

    def inside(value):
        return (value >= 0) & (value < width)

    def line_start(way, s):
        sign = 1 - 2 * way

        @pl.when(inside(line - sign * s) & inside(line + sign))
        def _():
            line_copy(way, s).start()

    def line_finish(way, s):
        sign = 1 - 2 * way

        @pl.when(inside(line - sign * (s + 1)))
        def _():
            block = gains.at[line - sign * (s + 1)]
            pltpu.make_async_copy(block, block, line_recv.at[way, s]).wait()

        @pl.when(inside(line - sign * s) & inside(line + sign))
        def _():
            line_copy(way, s).wait_send()

    def gain_first():
        for copy in norm_loads:
            copy.wait()
        gains[line, me] = norm_mem[0] + norm_mem[1]
        gain_copy(0).start()

    def gain_round(r):
        gain_arrival(r)
        if r + 1 < rounds:
            gain_copy(r + 1).start()
        elif width > 1:
            for way in range(2):
                line_start(way, 0)

    def gain_line(s):
        for way in range(2):
            line_finish(way, s)
        if s + 1 < width - 1:
            for way in range(2):
                line_start(way, s + 1)

    errands = [gain_first]
    errands += [functools.partial(gain_round, r) for r in range(rounds)]
    errands += [functools.partial(gain_line, s) for s in range(width - 1)]

    def rows_of(letter, k):
        if k < 2 * count:
            return pl.ds((2 * (k % count) + letter) * piece, piece)
        first, stop = starts[k - 2 * count : k - 2 * count + 2]
        return pl.ds(first + letter * (stop - first) // 2, (stop - first) // 2)

    def matrix_of(k):
        return min(k // count, 2)

    def finish(k):
        m = k // count
        at = pl.ds(2 * (k % count) * piece, 2 * piece)
        outs[m][me, at, :] = (latest[m, at, :] * scale[m]).astype(jnp.bfloat16)

    def view(k, letter, owner):
        return outs[matrix_of(k)].at[owner, rows_of(letter, k)]

    def landing(k, side, letter, hop):
        return ring_sem.at[k % ring_sem.shape[0], slots.index((side, letter, hop))]

    def ring_copy(k, side, letter, hop):
        sign = 1 - 2 * side
        owner = shard_at(-sign * hop)
        where = view(k, letter, owner)
        source = where
        if k < raw and hop == 0:
            source = w_mem.at[0, rows_of(letter, k)]
        sent = ring_send.at[matrix_of(k)]
        if k < raw:
            sent = ring_send.at[3]
            if hop > 0:
                sent = raw_send.at[k, slots.index((side, letter, hop))]
        return pltpu.make_async_remote_copy(
            src_ref=source,
            dst_ref=where,
            send_sem=sent,
            recv_sem=landing(k, side, letter, hop),
            device_id={"shard": shard_at(sign)},
            device_id_type=MESH,
        )

    def low_copy(side, hop):
        sign = 1 - 2 * side
        where = low_raw.at[shard_at(-sign * hop)]
        return pltpu.make_async_remote_copy(
            src_ref=low_turned.at[0, :, pl.ds(0, reach)] if hop == 0 else where,
            dst_ref=where,
            send_sem=low_send.at[0],
            recv_sem=low_recv.at[side * half + hop],
            device_id={"shard": shard_at(sign)},
            device_id_type=MESH,
        )

    def ring_start(k, side, letter, hop):
        ring_copy(k, side, letter, hop).start()

    def low_arrival(side, hop):
        sign = 1 - 2 * side
        owner = shard_at(-sign * (hop + 1))
        where = low_raw.at[owner]
        pltpu.make_async_copy(where, where, low_recv.at[side * half + hop]).wait()
        if hop + 1 < hops(side, 0):
            low_copy(side, hop + 1).start()
        low_far[owner] = low_raw[owner].T

    def ring_arrival(k, side, letter, hop):
        sign = 1 - 2 * side
        owner = shard_at(-sign * (hop + 1))
        where = view(k, letter, owner)
        pltpu.make_async_copy(where, where, landing(k, side, letter, hop)).wait()
        return owner

    def pair_copy(k, letter, owner):
        where = view(k, letter, owner)
        pltpu.make_async_remote_copy(
            src_ref=where,
            dst_ref=where,
            send_sem=pair_send.at[matrix_of(k) // 2 * 2],
            recv_sem=pair_sem.at[matrix_of(k) // 2 * 2],
            device_id={"shard": sibling},
            device_id_type=MESH,
        ).start()

    def pair_own():
        for k in range(2 * count, 3 * count):
            finish(k)
        return pltpu.make_async_remote_copy(
            src_ref=early.at[me],
            dst_ref=early.at[me],
            send_sem=pair_send.at[1],
            recv_sem=pair_sem.at[1],
            device_id={"shard": sibling},
            device_id_type=MESH,
        )

    def by_role(k):
        if k < shared:
            return lambda act: act()
        return pl.when(core != LEAD)

    def hops(side, letter):
        return half if side == letter else half - 1

    pending = []

    def landed(k, side, letter, hop, owner):
        if k < raw:
            pending.append((k, side, letter, hop, owner))
        elif k < shared:
            pair_copy(k, letter, owner)

    low_seen = set()

    def absorb():
        for k, side, letter, hop, owner in pending:
            if hop + 1 < hops(side, letter):
                ring_copy(k, side, letter, hop + 1).wait_send()
            from_side, from_hop = (side, hop) if hop < hops(side, 0) else (0, half - 1)
            for h in range(from_hop + 1):
                if (from_side, h) not in low_seen:
                    low_seen.add((from_side, h))
                    low_arrival(from_side, h)
            at = rows_of(letter, k)
            value = ready[0, owner, at, :].astype(jnp.float32) + mix_rate * jnp.dot(
                low_far[owner, at, :], high_mem[0], preferred_element_type=jnp.float32
            )
            ready[0, owner, at, :] = (value * scale[0]).astype(jnp.bfloat16)
            pair_copy(k, letter, owner)
        pending.clear()

    small_writes = [
        pltpu.make_async_copy(held, small_outs[0], out_sem.at[0]),
        pltpu.make_async_copy(gains, small_outs[1], out_sem.at[1]),
    ]
    first.wait()
    pl.semaphore_wait(
        barrier,
        2 + rounds + (line > 0).astype(jnp.int32) + (line < width - 1).astype(jnp.int32),
    )

    own_value = []
    closed = set()
    last_hops = [s for side in range(2) for s in slots[::-1] if s[0] == side and s[2] == hops(*s[0:2]) - 1]

    def pass_on(k, hop):
        for side in range(2):
            owner = ring_arrival(k, side, side, hop)
            ring_start(k, side, side, hop + 1)
            landed(k, side, side, hop, owner)

    def close(k, side, letter, hop):
        closed.add((k, side, letter))
        landed(k, side, letter, hop, ring_arrival(k, side, letter, hop))

    for j in range(shared + extra + half):
        def first_own():
            for side in range(2):
                if hops(side, side) > 0:
                    ring_start(j, side, side, 0)

        if j < shared + extra and j != shared:
            by_role(j)(first_own)
        if j == 0:
            merge(0)
            advance(0)
        for hop in range(half - 1):
            k = j - 1 - hop
            if (k, hop) == (0, 0):
                continue
            if 0 <= k < shared + extra:
                by_role(k)(functools.partial(pass_on, k, hop))

        if j == shared and extra > 0:
            by_role(j)(first_own)
        if j < shared + extra:

            @by_role(j)
            def _():
                for side in range(2):
                    if hops(side, 1 - side) > 0:
                        ring_start(j, side, 1 - side, 0)

        for hop in range(half - 2):
            k = j - 1 - hop
            if 0 <= k < shared + extra:

                @by_role(k)
                def _():
                    for side in range(2):
                        owner = ring_arrival(k, side, 1 - side, hop)
                        ring_start(k, side, 1 - side, hop + 1)
                        landed(k, side, 1 - side, hop, owner)

        if raw <= j < 2 * count:
            for letter in range(2):
                pair_copy(j, letter, me)
        if j == 0:
            for side in range(2):
                if hops(side, 0) > 0:
                    low_copy(side, 0).start()
            advance(0)
            if half > 1:
                pass_on(0, 0)
        if j in (1, 2):
            merge(j)
        for m in range(1, 3):
            if j > m and met[m] < rounds:
                advance(m)
        if 1 <= j < half:
            for side in range(2):
                if j - 1 < hops(side, 0):
                    low_seen.add((side, j - 1))
                    low_arrival(side, j - 1)
        if j > 0 and errands:
            errands.pop(0)()
        if j == min(raw + rounds + 2, 2 * count - 1):
            settle(2)
            own_value.append(pair_own())
            own_value[0].start()
        if j == 2 * count - 1:
            while errands:
                errands.pop(0)()
            for copy in small_writes:
                copy.start()
        if raw <= j + 1 < 2 * count:
            if j + 1 == raw:
                settle(0)
            if (j + 1) % count == 0:
                settle((j + 1) // count)
            finish(j + 1)
        for side, letter, hop in last_hops:
            k = j - 1 - hop
            if 0 <= k < shared + extra and (k, side, letter) not in closed:
                by_role(k)(functools.partial(close, k, side, letter, hop))
        if j == shared and half == 2:
            for side in range(2):
                close(shared - 1, side, side, half - 1)
        if j == raw:
            for k in range(raw):
                finish(k)
                for letter in range(2):
                    pair_copy(k, letter, me)
        if j >= raw:
            absorb()

    theirs = ready.at[:, pl.ds(0, chips)]
    pltpu.make_async_copy(theirs, theirs, pair_sem.at[0]).wait()
    pltpu.make_async_copy(theirs, theirs, pair_send.at[0]).wait()
    pltpu.make_async_copy(early.at[sibling], early.at[sibling], pair_sem.at[1]).wait()
    own_value[0].wait_send()

    def value_part(share):
        return early.at[pl.ds(0, chips - 1), pl.ds(0, starts[share])]

    if both > 0:
        theirs = value_part(both)
        pltpu.make_async_copy(theirs, theirs, pair_sem.at[2]).wait()
        pltpu.make_async_copy(theirs, theirs, pair_send.at[2]).wait()
    for m in range(2):
        kept = raw_rows if m == 0 else 0
        if kept < rows:
            sent = outs[m].at[pl.ds(0, chips - 1), pl.ds(kept, rows - kept)]
            pltpu.make_async_copy(sent, sent, ring_send.at[m]).wait()
    sent = ready.at[0, pl.ds(0, len([s for s in slots if s[2] == 0]) // 2), pl.ds(0, raw_rows)]
    pltpu.make_async_copy(sent, sent, ring_send.at[3]).wait()
    for share, mine in ((both, core == LEAD), (both + extra, core != LEAD)):
        if share > 0:

            @pl.when(mine)
            def _():
                sent = value_part(share)
                pltpu.make_async_copy(sent, sent, ring_send.at[2]).wait()

    pltpu.make_async_copy(max_in, max_in, max_send.at[0]).wait()
    sent = low_raw.at[pl.ds(0, chips - 1)]
    pltpu.make_async_copy(sent, sent, low_send.at[0]).wait()
    sent = gains.at[line, pl.ds(0, n - 1)]
    pltpu.make_async_copy(sent, sent, norm_send.at[0]).wait()
    for copy in small_writes:
        copy.wait()


def late_kernel(n, *refs):
    early, late = refs[0], refs[2]
    ring_send, pair_send, pair_sem, ring_sem, joined, last_sem = refs[3:9]
    parts = last_sem.shape[1]
    rows = early.shape[1]
    chips = n // 2
    half = chips // 2
    starts, both, extra = value_split(rows)
    count = len(starts) - 1
    slots = ring_slots(half)

    me = lax.axis_index("shard")
    chip, core = me // 2, lax.rem(me, 2)
    sibling = me + 1 - 2 * core

    def turned(c):
        return jnp.where(c < half, c, chips + half - 1 - c)

    place = turned(chip)

    def shard_at(offset):
        return turned(lax.rem(place + offset + 2 * chips, chips)) * 2 + core

    def hops(side, letter):
        return half if side == letter else half - 1

    def view(ref, k, letter, owner, part=None):
        size = (starts[k + 1] - starts[k]) // 2
        first = starts[k] + letter * size
        if part is not None:
            size = size // parts
            first += part * size
        return ref.at[owner, pl.ds(first, size)]

    def landing(k, side, letter, hop, part=None):
        if part is not None:
            return last_sem.at[side, part]
        return ring_sem.at[k % ring_sem.shape[0], slots.index((side, letter, hop))]

    def cut(k, side, letter, hop):
        if k == count - 1 and side == letter and hop == half - 1 and hop > 0 and parts > 1:
            return range(parts)
        return [None]

    def ring_start(k, side, letter, hop):
        sign = 1 - 2 * side
        owner = shard_at(-sign * hop)
        for part in cut(k, side, letter, hop):
            pltpu.make_async_remote_copy(
                src_ref=view(early if hop == 0 else late, k, letter, owner, part),
                dst_ref=view(late, k, letter, owner, part),
                send_sem=ring_send.at[0],
                recv_sem=landing(k, side, letter, hop, part),
                device_id={"shard": shard_at(sign)},
                device_id_type=MESH,
            ).start()

    def ring_arrival(k, side, letter, hop, part=None):
        sign = 1 - 2 * side
        where = view(late, k, letter, shard_at(-sign * (hop + 1)), part)
        pltpu.make_async_copy(where, where, landing(k, side, letter, hop, part)).wait()
        return where

    def to_sibling(source, target):
        pltpu.make_async_remote_copy(
            src_ref=source,
            dst_ref=target,
            send_sem=pair_send.at[0],
            recv_sem=pair_sem.at[0],
            device_id={"shard": sibling},
            device_id_type=MESH,
        ).start()

    barrier = pltpu.get_barrier_semaphore()
    for offset in (1, -1):
        pl.semaphore_signal(
            barrier, inc=1, device_id={"shard": shard_at(offset)}, device_id_type=MESH
        )

    def run(first, join):
        waiting = []

        def landed(where):
            if join is not None and not joined_at:
                waiting.append(where)
            else:
                to_sibling(where, where)

        joined_at = []
        for j in range(first, count + half):
            if j < count:
                for side in range(2):
                    if hops(side, side) > 0:
                        ring_start(j, side, side, 0)
            for hop in range(half - 1):
                k = j - 1 - hop
                if first <= k < count:
                    for side in range(2):
                        where = ring_arrival(k, side, side, hop)
                        ring_start(k, side, side, hop + 1)
                        landed(where)
            if j < count:
                for side in range(2):
                    if hops(side, 1 - side) > 0:
                        ring_start(j, side, 1 - side, 0)
            for hop in range(half - 2):
                k = j - 1 - hop
                if first <= k < count:
                    for side in range(2):
                        where = ring_arrival(k, side, 1 - side, hop)
                        ring_start(k, side, 1 - side, hop + 1)
                        landed(where)
            if j == join:
                pl.semaphore_wait(joined, 1)
                joined_at.append(j)
                for where in waiting:
                    to_sibling(where, where)
            ends = [
                (j - hops(side, letter), side, letter, hops(side, letter) - 1)
                for flip in range(2)
                for side in range(2)
                for letter in (side ^ flip,)
            ]
            ends = [s for s in ends if s[3] >= 0 and first <= s[0] < count]
            for part in range(parts):
                for s in ends:
                    if part < len(cut(*s)):
                        landed(ring_arrival(*s, cut(*s)[part]))
        if first < count:
            sent = late.at[pl.ds(0, chips - 1), pl.ds(0, rows - starts[first])]
            pltpu.make_async_copy(sent, sent, ring_send.at[0]).wait()

    @pl.when(core == LEAD)
    def _():
        pl.semaphore_signal(barrier, inc=1, device_id={"shard": sibling}, device_id_type=MESH)
        pl.semaphore_wait(barrier, 2)
        run(both, JOIN)

    @pl.when(core != LEAD)
    def _():
        pl.semaphore_wait(barrier, 3)
        pl.semaphore_signal(joined, inc=1, device_id={"shard": sibling}, device_id_type=MESH)
        if extra > 0:
            for offset in range(1, chips):
                owner = shard_at(offset)
                at = pl.ds(starts[both], starts[both + extra] - starts[both])
                to_sibling(early.at[owner, at], late.at[owner, at])
        run(both + extra, None)

    theirs = late.at[pl.ds(0, chips - 1), pl.ds(0, rows - starts[both])]
    pltpu.make_async_copy(theirs, theirs, pair_sem.at[0]).wait()
    pltpu.make_async_copy(theirs, theirs, pair_send.at[0]).wait()


def place_first(*refs):
    source, early, small = refs[0], refs[1], refs[2:4]
    targets, finals, sem = refs[4:7], refs[7:11], refs[11]
    factors, gains, small_sem = refs[12], refs[13], refs[14]
    scales, serve = refs[15:18], refs[18]
    writes = [
        pltpu.make_async_copy(refs[15 + i], finals[i], small_sem.at[2 + i]) for i in range(4)
    ]
    loads = [
        pltpu.make_async_copy(small[i], refs[12 + i], small_sem.at[i]) for i in range(2)
    ]
    n, rows = early.shape[0], early.shape[1]
    starts, both, _ = value_split(rows)
    both_rows = starts[both]
    chip = lax.div(lax.axis_index("shard"), 2)
    copies = [
        pltpu.make_async_copy(source.at[m, i], targets[m].at[i], sem.at[2 if m else min(i, 1)])
        for m in range(2)
        for i in range(source.shape[1])
    ]
    for copy in loads + copies:
        copy.start()
    ours = pl.ds(2 * chip, 2)
    pltpu.make_async_copy(early.at[ours], targets[2].at[ours], sem.at[3]).start()
    if both_rows > 0:
        for offset in range(1, n // 2):
            where = pl.ds(2 * lax.rem(chip + offset, n // 2), 2), pl.ds(0, both_rows)
            pltpu.make_async_copy(early.at[where], targets[2].at[where], sem.at[4]).start()
    for copy in loads:
        copy.wait()
    for m in range(3):
        scales[m][...] = factors[m].reshape(scales[m].shape)
    blocks = [gains[k, i] for i in range(gains.shape[1]) for k in range(gains.shape[0])]
    line = jnp.concatenate(blocks, axis=1)
    serve[...] = line.reshape(serve.shape).astype(jnp.bfloat16)
    copies[0].wait()
    for copy in writes:
        copy.start()
    rest = source.at[0, pl.ds(1, source.shape[1] - 1)]
    second = source.at[1]
    pltpu.make_async_copy(rest, rest, sem.at[1]).wait()
    pltpu.make_async_copy(second, second, sem.at[2]).wait()
    pltpu.make_async_copy(early.at[ours], targets[2].at[ours], sem.at[3]).wait()
    if both_rows > 0:
        part = early.at[pl.ds(0, n - 2), pl.ds(0, both_rows)]
        pltpu.make_async_copy(part, part, sem.at[4]).wait()
    for copy in writes:
        copy.wait()


def place_last(early, late, before, target, sem):
    n, rows = early.shape[0], early.shape[1]
    chips = n // 2
    starts, both, extra = value_split(rows)
    me = lax.axis_index("shard")
    chip, core = me // 2, lax.rem(me, 2)

    def put(source, owner, start, stop):
        if start < stop:
            size = (starts[stop] - starts[start]) // 2
            for part in range(2):
                where = owner, pl.ds(starts[start] + part * size, size)
                pltpu.make_async_copy(source.at[where], target.at[where], sem.at[0]).start()

    count = len(starts) - 1
    for offset in range(1, chips):
        other = lax.rem(chip + offset, chips) * 2
        put(late, other + 1 - core, both, count)

        @pl.when(core == LEAD)
        def _():
            put(late, other + core, both, count)

        @pl.when(core != LEAD)
        def _():
            put(early, other + core, both, both + extra)
            put(late, other + core, both + extra, count)

    part = late.at[pl.ds(0, n - 2), pl.ds(starts[both], rows - starts[both])]
    pltpu.make_async_copy(part, part, sem.at[0]).wait()


def body(n, width, w_query, low_query, high_query, w_key, low_key, high_key, w_value, low_value, high_value, norm_train, norm_step):
    rows, columns = w_query.shape
    rank = low_query.shape[1]
    length = norm_train.shape[0]
    half = n // 4
    count = chunks_of(rows)
    raw = 1
    rounds = n.bit_length() - 1
    reach = min(rows, -(-(rows // count) * raw // 128) * 128)
    slots = len(ring_slots(half))
    starts, both, _ = value_split(rows)
    block = jax.ShapeDtypeStruct((n, rows, columns), jnp.bfloat16)

    def near(value):
        return pltpu.with_memory_space_constraint(value, pltpu.VMEM)

    def far(value):
        return pltpu.with_memory_space_constraint(value, pltpu.HBM)

    ready, early, factors, gains = pl.pallas_call(
        functools.partial(gather_kernel, n, width),
        name="merge_gather",
        out_shape=[
            pltpu.VMEM((2, n, rows, columns), jnp.bfloat16),
            pltpu.VMEM((n, rows, columns), jnp.bfloat16),
            jax.ShapeDtypeStruct((3, 1, columns), jnp.float32),
            jax.ShapeDtypeStruct((width, n, 1, length), jnp.float32),
        ],
        in_specs=[ANY] * 11,
        out_specs=[pl.BlockSpec(memory_space=pltpu.VMEM)] * 2 + [HBM] * 2,
        scratch_shapes=[
            pltpu.VMEM((3, rows, columns), jnp.bfloat16),
            pltpu.VMEM((3, rows, rank), jnp.bfloat16),
            pltpu.VMEM((3, rank, columns), jnp.bfloat16),
            pltpu.VMEM((2, 1, length), jnp.float32),
            pltpu.VMEM((3, rows, columns), jnp.float32),
            pltpu.VMEM((3, 1, columns), jnp.float32),
            pltpu.VMEM((3, rounds + 1, 1, columns), jnp.float32),
            pltpu.SemaphoreType.DMA((4, 3)),
            pltpu.SemaphoreType.DMA((4,)),
            pltpu.SemaphoreType.DMA((3,)),
            pltpu.SemaphoreType.DMA((1,)),
            pltpu.SemaphoreType.DMA((3, rounds)),
            pltpu.SemaphoreType.DMA((1,)),
            pltpu.SemaphoreType.DMA((rounds,)),
            pltpu.SemaphoreType.DMA((5, slots)),
            pltpu.SemaphoreType.DMA((3,)),
            pltpu.VMEM((3, rank, rows), jnp.bfloat16),
            pltpu.VMEM((3, 1, columns), jnp.float32),
            pltpu.VMEM((width, n, 1, length), jnp.float32),
            pltpu.SemaphoreType.DMA((2,)),
            pltpu.VMEM((n, rank, reach), jnp.bfloat16),
            pltpu.VMEM((n, reach, rank), jnp.bfloat16),
            pltpu.SemaphoreType.DMA((raw, slots)),
            pltpu.SemaphoreType.DMA((1,)),
            pltpu.SemaphoreType.DMA((2 * half,)),
            pltpu.VMEM((3, rounds, 1, columns), jnp.float32),
            pltpu.SemaphoreType.DMA((2,)),
            pltpu.SemaphoreType.DMA((2, max(width - 1, 1))),
        ],
        compiler_params=pltpu.CompilerParams(
            collective_id=0, has_side_effects=True, vmem_limit_bytes=20 * 2**20
        ),
    )(
        w_query, w_key, w_value,
        low_query.T, low_key.T, low_value.T,
        high_query, high_key, high_value,
        norm_train.reshape(1, length), norm_step.reshape(1, length),
    )
    query, key, value, *small = pl.pallas_call(
        place_first,
        name="place_first",
        out_shape=[block] * 3
        + [jax.ShapeDtypeStruct((columns,), jnp.float32)] * 3
        + [jax.ShapeDtypeStruct((n * width * length,), jnp.bfloat16)],
        in_specs=[ANY] * 2 + [HBM] * 2,
        out_specs=[HBM] * 7,
        scratch_shapes=[
            pltpu.SemaphoreType.DMA((5,)),
            pltpu.VMEM((3, 1, columns), jnp.float32),
            pltpu.VMEM((width, n, 1, length), jnp.float32),
            pltpu.SemaphoreType.DMA((6,)),
            *[pltpu.VMEM((columns,), jnp.float32)] * 3,
            pltpu.VMEM((n * width * length,), jnp.bfloat16),
        ],
        compiler_params=pltpu.CompilerParams(vmem_limit_bytes=2**20),
    )(near(ready), near(early), far(factors), far(gains))
    late = pl.pallas_call(
        functools.partial(late_kernel, n),
        name="gather_late",
        out_shape=pltpu.VMEM((n, rows, columns), jnp.bfloat16),
        in_specs=[ANY, HBM],
        out_specs=pl.BlockSpec(memory_space=pltpu.VMEM),
        scratch_shapes=[
            pltpu.SemaphoreType.DMA((1,)),
            pltpu.SemaphoreType.DMA((1,)),
            pltpu.SemaphoreType.DMA((1,)),
            pltpu.SemaphoreType.DMA((len(starts) - 1 - both, slots)),
            pltpu.SemaphoreType.REGULAR,
            pltpu.SemaphoreType.DMA((2, last_parts(rows))),
        ],
        compiler_params=pltpu.CompilerParams(
            collective_id=1, has_side_effects=True, vmem_limit_bytes=2**20
        ),
    )(near(early), far(small[0]))
    value = pl.pallas_call(
        place_last,
        name="place_last",
        out_shape=block,
        in_specs=[ANY] * 2 + [HBM],
        out_specs=HBM,
        scratch_shapes=[pltpu.SemaphoreType.DMA((1,))],
        input_output_aliases={2: 0},
        compiler_params=pltpu.CompilerParams(vmem_limit_bytes=2**20),
    )(near(early), near(late), far(value))
    return (
        *(ready.reshape(n * rows, columns) for ready in (query, key, value)),
        *small,
    )


def solution(mesh):
    n, width = mesh.shape["shard"], mesh.shape["width"]
    return jax.shard_map(
        functools.partial(body, n, width),
        mesh=mesh,
        in_specs=(
            P("shard", "width"),
            P("shard", None),
            P(None, "width"),
            P("shard", "width"),
            P("shard", None),
            P(None, "width"),
            P("shard", "width"),
            P("shard", None),
            P(None, "width"),
            P(("shard", "width")),
            P(("shard", "width")),
        ),
        out_specs=(
            P(None, "width"),
            P(None, "width"),
            P(None, "width"),
            P("width"),
            P("width"),
            P("width"),
            P(),
        ),
        check_vma=False,
    )
```

```python
import functools

import jax
import jax.numpy as jnp
from jax import lax
from jax.experimental import pallas as pl
from jax.experimental.pallas import tpu as pltpu
from jax.sharding import PartitionSpec as P

mix_rate = 0.5
LEAD = 1
SIZES = (2, 1, 2, 2, 2, 1)
JOIN = 6
BOTH = 2
EXTRA = 3
MESH = pl.DeviceIdType.MESH
ANY = pl.BlockSpec(memory_space=pl.ANY)
HBM = pl.BlockSpec(memory_space=pltpu.HBM)


def chunks_of(rows):
    for count in (5, 4, 2):
        if rows % (2 * count * 16) == 0:
            return count
    return 1


def value_split(rows):
    sizes = SIZES
    if rows % (sum(sizes) * 32) != 0:
        sizes = [1] * chunks_of(rows)
    unit = rows // sum(sizes)
    starts = [unit * sum(sizes[:i]) for i in range(len(sizes) + 1)]
    extra = min(EXTRA, len(sizes) - 1)
    return starts, min(BOTH, len(sizes) - extra), extra


def last_parts(rows):
    starts = value_split(rows)[0]
    return max((rows - starts[-2]) // 32, 1)


def ring_slots(half):
    return [
        (side, letter, hop)
        for side in range(2)
        for letter in range(2)
        for hop in range(half if side == letter else half - 1)
    ]


def gather_kernel(n, width, *refs):
    weights, lows, highs, norms = refs[0:3], refs[3:6], refs[6:9], refs[9:11]
    ready, early, small_outs = refs[11], refs[12], refs[13:15]
    w_mem, low_mem, high_mem, norm_mem, latest, scale, largest_of = refs[15:22]
    load_sem, ring_send, pair_send, max_send, max_recv, norm_send, norm_recv = refs[22:29]
    ring_sem, pair_sem, low_turned, held, gains, out_sem = refs[29:35]
    low_raw, low_far, raw_send, low_send, low_recv, max_in, line_send, line_recv = refs[35:43]
    outs = [ready.at[0], ready.at[1], early]

    rows = w_mem.shape[1]
    chips = n // 2
    half = chips // 2
    count = chunks_of(rows)
    piece = rows // (2 * count)
    starts, both, extra = value_split(rows)
    shared = 2 * count + both
    raw = 1
    raw_rows = 2 * piece * raw
    reach = low_raw.shape[2]
    rounds = n.bit_length() - 1
    assert n == 1 << rounds

    me = lax.axis_index("shard")
    line = lax.axis_index("width")
    chip, core = me // 2, lax.rem(me, 2)
    sibling = me + 1 - 2 * core
    slots = ring_slots(half)

    def turned(c):
        return jnp.where(c < half, c, chips + half - 1 - c)

    place = turned(chip)

    def shard_at(offset):
        return turned(lax.rem(place + offset + 2 * chips, chips)) * 2 + core

    def group(r):
        return lax.div(me, 1 << r)

    def partner(r):
        return me + (1 << r) * (1 - 2 * lax.rem(group(r), 2))

    def load(source, target, m, slot):
        return pltpu.make_async_copy(source, target, load_sem.at[m, slot])

    first = load(weights[0].at[pl.ds(0, raw_rows)], w_mem.at[0, pl.ds(0, raw_rows)], 3, 2)
    loads = []
    for m in range(3):
        parts = [load(lows[m], low_turned.at[m], m, 0), load(highs[m], high_mem.at[m], m, 1)]
        if m > 0:
            parts.append(load(weights[m], w_mem.at[m], m, 2))
        elif raw_rows < rows:
            rest = pl.ds(raw_rows, rows - raw_rows)
            parts.append(load(weights[0].at[rest], w_mem.at[0, rest], m, 2))
        loads.append(parts)
    norm_loads = [load(norms[i], norm_mem.at[i], 3, i) for i in range(2)]
    barrier = pltpu.get_barrier_semaphore()

    def greet(axis, index):
        pl.semaphore_signal(barrier, inc=1, device_id={axis: index}, device_id_type=MESH)

    ring_greets = 0 if chips == 4 else 2
    for offset in (1, -1)[:ring_greets]:
        greet("shard", shard_at(offset))
    for r in range(rounds):
        greet("shard", partner(r))

    @pl.when(line > 0)
    def _():
        greet("width", line - 1)

    @pl.when(line < width - 1)
    def _():
        greet("width", line + 1)

    first.start()
    for parts in loads:
        for copy in parts:
            copy.start()
    for copy in norm_loads:
        copy.start()

    tile = piece

    def merge(m):
        for copy in loads[m]:
            copy.wait()
        low_mem[m] = low_turned[m].T

        def body(t, largest):
            at = pl.ds(pl.multiple_of(t * tile, tile), tile)
            value = w_mem[m, at, :].astype(jnp.float32) + mix_rate * jnp.dot(
                low_mem[m, at, :], high_mem[m], preferred_element_type=jnp.float32
            )
            latest[m, at, :] = value
            sizes = jnp.abs(value).reshape(tile // 8, 8, value.shape[1])
            return jnp.maximum(largest, jnp.max(sizes, axis=0))

        largest = lax.fori_loop(0, rows // tile, body, jnp.zeros((8, w_mem.shape[2]), jnp.float32))
        largest_of[m, 0] = jnp.max(largest, axis=0, keepdims=True)
        max_copy(m, 0).start()

    def max_copy(m, r):
        return pltpu.make_async_remote_copy(
            src_ref=largest_of.at[m, r],
            dst_ref=max_in.at[m, r],
            send_sem=max_send.at[0],
            recv_sem=max_recv.at[m, r],
            device_id={"shard": partner(r)},
            device_id_type=MESH,
        )

    met = [0, 0, 0]

    def advance(m):
        r = met[m]
        if r == rounds:
            return
        max_copy(m, r).wait_recv()
        largest_of[m, r + 1] = jnp.maximum(largest_of[m, r], max_in[m, r])
        met[m] = r + 1
        if r + 1 < rounds:
            max_copy(m, r + 1).start()

    def settle(m):
        while met[m] < rounds:
            advance(m)
        factor = largest_of[m, rounds]
        held[m] = factor
        scale[m] = 1.0 / factor

    def gain_copy(r):
        return pltpu.make_async_remote_copy(
            src_ref=gains.at[line, pl.ds(group(r) * (1 << r), 1 << r)],
            dst_ref=gains.at[line, pl.ds(group(r) * (1 << r), 1 << r)],
            send_sem=norm_send.at[0],
            recv_sem=norm_recv.at[r],
            device_id={"shard": partner(r)},
            device_id_type=MESH,
        )

    def gain_arrival(r):
        theirs = gains.at[line, pl.ds(lax.div(partner(r), 1 << r) * (1 << r), 1 << r)]
        pltpu.make_async_copy(theirs, theirs, norm_recv.at[r]).wait()

    def line_copy(way, s):
        sign = 1 - 2 * way
        block = gains.at[line - sign * s]
        return pltpu.make_async_remote_copy(
            src_ref=block,
            dst_ref=block,
            send_sem=line_send.at[way],
            recv_sem=line_recv.at[way, s],
            device_id={"width": line + sign},
            device_id_type=MESH,
        )

    def inside(value):
        return (value >= 0) & (value < width)

    def line_start(way, s):
        sign = 1 - 2 * way

        @pl.when(inside(line - sign * s) & inside(line + sign))
        def _():
            line_copy(way, s).start()

    def line_finish(way, s):
        sign = 1 - 2 * way

        @pl.when(inside(line - sign * (s + 1)))
        def _():
            block = gains.at[line - sign * (s + 1)]
            pltpu.make_async_copy(block, block, line_recv.at[way, s]).wait()

        @pl.when(inside(line - sign * s) & inside(line + sign))
        def _():
            line_copy(way, s).wait_send()

    def gain_first():
        for copy in norm_loads:
            copy.wait()
        gains[line, me] = norm_mem[0] + norm_mem[1]
        gain_copy(0).start()

    def gain_round(r):
        gain_arrival(r)
        if r + 1 < rounds:
            gain_copy(r + 1).start()
        elif width > 1:
            for way in range(2):
                line_start(way, 0)

    def gain_line(s):
        for way in range(2):
            line_finish(way, s)
        if s + 1 < width - 1:
            for way in range(2):
                line_start(way, s + 1)

    errands = [gain_first]
    errands += [functools.partial(gain_round, r) for r in range(rounds)]
    errands += [functools.partial(gain_line, s) for s in range(width - 1)]

    def rows_of(letter, k):
        if k < 2 * count:
            return pl.ds((2 * (k % count) + letter) * piece, piece)
        first, stop = starts[k - 2 * count : k - 2 * count + 2]
        return pl.ds(first + letter * (stop - first) // 2, (stop - first) // 2)

    def matrix_of(k):
        return min(k // count, 2)

    def finish(k):
        m = k // count
        at = pl.ds(2 * (k % count) * piece, 2 * piece)
        outs[m][me, at, :] = (latest[m, at, :] * scale[m]).astype(jnp.bfloat16)

    def view(k, letter, owner):
        return outs[matrix_of(k)].at[owner, rows_of(letter, k)]

    def landing(k, side, letter, hop):
        return ring_sem.at[k % ring_sem.shape[0], slots.index((side, letter, hop))]

    def ring_copy(k, side, letter, hop):
        sign = 1 - 2 * side
        owner = shard_at(-sign * hop)
        where = view(k, letter, owner)
        source = where
        if k < raw and hop == 0:
            source = w_mem.at[0, rows_of(letter, k)]
        sent = ring_send.at[matrix_of(k)]
        if k < raw:
            sent = ring_send.at[3]
            if hop > 0:
                sent = raw_send.at[k, slots.index((side, letter, hop))]
        return pltpu.make_async_remote_copy(
            src_ref=source,
            dst_ref=where,
            send_sem=sent,
            recv_sem=landing(k, side, letter, hop),
            device_id={"shard": shard_at(sign)},
            device_id_type=MESH,
        )

    def low_copy(side, hop):
        sign = 1 - 2 * side
        where = low_raw.at[shard_at(-sign * hop)]
        return pltpu.make_async_remote_copy(
            src_ref=low_turned.at[0, :, pl.ds(0, reach)] if hop == 0 else where,
            dst_ref=where,
            send_sem=low_send.at[0],
            recv_sem=low_recv.at[side * half + hop],
            device_id={"shard": shard_at(sign)},
            device_id_type=MESH,
        )

    def ring_start(k, side, letter, hop):
        ring_copy(k, side, letter, hop).start()

    def low_arrival(side, hop):
        sign = 1 - 2 * side
        owner = shard_at(-sign * (hop + 1))
        where = low_raw.at[owner]
        pltpu.make_async_copy(where, where, low_recv.at[side * half + hop]).wait()
        if hop + 1 < hops(side, 0):
            low_copy(side, hop + 1).start()
        low_far[owner] = low_raw[owner].T

    def ring_arrival(k, side, letter, hop):
        sign = 1 - 2 * side
        owner = shard_at(-sign * (hop + 1))
        where = view(k, letter, owner)
        pltpu.make_async_copy(where, where, landing(k, side, letter, hop)).wait()
        return owner

    def pair_copy(k, letter, owner):
        where = view(k, letter, owner)
        pltpu.make_async_remote_copy(
            src_ref=where,
            dst_ref=where,
            send_sem=pair_send.at[matrix_of(k) // 2 * 2],
            recv_sem=pair_sem.at[matrix_of(k) // 2 * 2],
            device_id={"shard": sibling},
            device_id_type=MESH,
        ).start()

    def pair_own():
        for k in range(2 * count, 3 * count):
            finish(k)
        return pltpu.make_async_remote_copy(
            src_ref=early.at[me],
            dst_ref=early.at[me],
            send_sem=pair_send.at[1],
            recv_sem=pair_sem.at[1],
            device_id={"shard": sibling},
            device_id_type=MESH,
        )

    def by_role(k):
        if k < shared:
            return lambda act: act()
        return pl.when(core != LEAD)

    def hops(side, letter):
        return half if side == letter else half - 1

    pending = []

    def landed(k, side, letter, hop, owner):
        if k < raw:
            pending.append((k, side, letter, hop, owner))
        elif k < shared:
            pair_copy(k, letter, owner)

    low_seen = set()

    def absorb():
        for k, side, letter, hop, owner in pending:
            if hop + 1 < hops(side, letter):
                ring_copy(k, side, letter, hop + 1).wait_send()
            from_side, from_hop = (side, hop) if hop < hops(side, 0) else (0, half - 1)
            for h in range(from_hop + 1):
                if (from_side, h) not in low_seen:
                    low_seen.add((from_side, h))
                    low_arrival(from_side, h)
            at = rows_of(letter, k)
            value = ready[0, owner, at, :].astype(jnp.float32) + mix_rate * jnp.dot(
                low_far[owner, at, :], high_mem[0], preferred_element_type=jnp.float32
            )
            ready[0, owner, at, :] = (value * scale[0]).astype(jnp.bfloat16)
            pair_copy(k, letter, owner)
        pending.clear()

    small_writes = [
        pltpu.make_async_copy(held, small_outs[0], out_sem.at[0]),
        pltpu.make_async_copy(gains, small_outs[1], out_sem.at[1]),
    ]
    first.wait()
    pl.semaphore_wait(
        barrier,
        ring_greets + rounds + (line > 0).astype(jnp.int32) + (line < width - 1).astype(jnp.int32),
    )

    own_value = []
    closed = set()
    last_hops = [s for side in range(2) for s in slots[::-1] if s[0] == side and s[2] == hops(*s[0:2]) - 1]

    def pass_on(k, hop):
        for side in range(2):
            owner = ring_arrival(k, side, side, hop)
            ring_start(k, side, side, hop + 1)
            landed(k, side, side, hop, owner)

    def close(k, side, letter, hop):
        closed.add((k, side, letter))
        landed(k, side, letter, hop, ring_arrival(k, side, letter, hop))

    for j in range(shared + extra + half):
        def first_own():
            for side in range(2):
                if hops(side, side) > 0:
                    ring_start(j, side, side, 0)

        if j < shared + extra and j != shared:
            by_role(j)(first_own)
        if j == 0:
            merge(0)
            advance(0)
        for hop in range(half - 1):
            k = j - 1 - hop
            if (k, hop) == (0, 0):
                continue
            if 0 <= k < shared + extra:
                by_role(k)(functools.partial(pass_on, k, hop))

        if j == shared and extra > 0:
            by_role(j)(first_own)
        if j < shared + extra:

            @by_role(j)
            def _():
                for side in range(2):
                    if hops(side, 1 - side) > 0:
                        ring_start(j, side, 1 - side, 0)

        for hop in range(half - 2):
            k = j - 1 - hop
            if 0 <= k < shared + extra:

                @by_role(k)
                def _():
                    for side in range(2):
                        owner = ring_arrival(k, side, 1 - side, hop)
                        ring_start(k, side, 1 - side, hop + 1)
                        landed(k, side, 1 - side, hop, owner)

        if raw <= j < 2 * count:
            for letter in range(2):
                pair_copy(j, letter, me)
        if j == 0:
            for side in range(2):
                if hops(side, 0) > 0:
                    low_copy(side, 0).start()
            advance(0)
            if half > 1:
                pass_on(0, 0)
        if j in (1, 2):
            merge(j)
        for m in range(1, 3):
            if j > m and met[m] < rounds:
                advance(m)
        if 1 <= j < half:
            for side in range(2):
                if j - 1 < hops(side, 0):
                    low_seen.add((side, j - 1))
                    low_arrival(side, j - 1)
        if j > 0 and errands:
            errands.pop(0)()
        if j == min(raw + rounds + 2, 2 * count - 1):
            settle(2)
            own_value.append(pair_own())
            own_value[0].start()
        if j == 2 * count - 1:
            while errands:
                errands.pop(0)()
            for copy in small_writes:
                copy.start()
        if raw <= j + 1 < 2 * count:
            if j + 1 == raw:
                settle(0)
            if (j + 1) % count == 0:
                settle((j + 1) // count)
            finish(j + 1)
        for side, letter, hop in last_hops:
            k = j - 1 - hop
            if 0 <= k < shared + extra and (k, side, letter) not in closed:
                by_role(k)(functools.partial(close, k, side, letter, hop))
        if j == shared and half == 2:
            for side in range(2):
                close(shared - 1, side, side, half - 1)
        if j == raw:
            for k in range(raw):
                finish(k)
                for letter in range(2):
                    pair_copy(k, letter, me)
        if j >= raw:
            absorb()

    theirs = ready.at[:, pl.ds(0, chips)]
    pltpu.make_async_copy(theirs, theirs, pair_sem.at[0]).wait()
    pltpu.make_async_copy(theirs, theirs, pair_send.at[0]).wait()
    pltpu.make_async_copy(early.at[sibling], early.at[sibling], pair_sem.at[1]).wait()
    own_value[0].wait_send()

    def value_part(share):
        return early.at[pl.ds(0, chips - 1), pl.ds(0, starts[share])]

    if both > 0:
        theirs = value_part(both)
        pltpu.make_async_copy(theirs, theirs, pair_sem.at[2]).wait()
        pltpu.make_async_copy(theirs, theirs, pair_send.at[2]).wait()
    for m in range(2):
        kept = raw_rows if m == 0 else 0
        if kept < rows:
            sent = outs[m].at[pl.ds(0, chips - 1), pl.ds(kept, rows - kept)]
            pltpu.make_async_copy(sent, sent, ring_send.at[m]).wait()
    sent = ready.at[0, pl.ds(0, len([s for s in slots if s[2] == 0]) // 2), pl.ds(0, raw_rows)]
    pltpu.make_async_copy(sent, sent, ring_send.at[3]).wait()
    for share, mine in ((both, core == LEAD), (both + extra, core != LEAD)):
        if share > 0:

            @pl.when(mine)
            def _():
                sent = value_part(share)
                pltpu.make_async_copy(sent, sent, ring_send.at[2]).wait()

    pltpu.make_async_copy(max_in, max_in, max_send.at[0]).wait()
    sent = low_raw.at[pl.ds(0, chips - 1)]
    pltpu.make_async_copy(sent, sent, low_send.at[0]).wait()
    sent = gains.at[line, pl.ds(0, n - 1)]
    pltpu.make_async_copy(sent, sent, norm_send.at[0]).wait()
    for copy in small_writes:
        copy.wait()


def late_kernel(n, *refs):
    early, late = refs[0], refs[2]
    ring_send, pair_send, pair_sem, ring_sem, joined, last_sem = refs[3:9]
    parts = last_sem.shape[1]
    rows = early.shape[1]
    chips = n // 2
    half = chips // 2
    starts, both, extra = value_split(rows)
    count = len(starts) - 1
    slots = ring_slots(half)

    me = lax.axis_index("shard")
    chip, core = me // 2, lax.rem(me, 2)
    sibling = me + 1 - 2 * core

    def turned(c):
        return jnp.where(c < half, c, chips + half - 1 - c)

    place = turned(chip)

    def shard_at(offset):
        return turned(lax.rem(place + offset + 2 * chips, chips)) * 2 + core

    def hops(side, letter):
        return half if side == letter else half - 1

    def view(ref, k, letter, owner, part=None):
        size = (starts[k + 1] - starts[k]) // 2
        first = starts[k] + letter * size
        if part is not None:
            size = size // parts
            first += part * size
        return ref.at[owner, pl.ds(first, size)]

    def landing(k, side, letter, hop, part=None):
        if part is not None:
            return last_sem.at[side, part]
        return ring_sem.at[k % ring_sem.shape[0], slots.index((side, letter, hop))]

    def cut(k, side, letter, hop):
        if k == count - 1 and side == letter and hop == half - 1 and hop > 0 and parts > 1:
            return range(parts)
        return [None]

    def ring_start(k, side, letter, hop):
        sign = 1 - 2 * side
        owner = shard_at(-sign * hop)
        for part in cut(k, side, letter, hop):
            pltpu.make_async_remote_copy(
                src_ref=view(early if hop == 0 else late, k, letter, owner, part),
                dst_ref=view(late, k, letter, owner, part),
                send_sem=ring_send.at[0],
                recv_sem=landing(k, side, letter, hop, part),
                device_id={"shard": shard_at(sign)},
                device_id_type=MESH,
            ).start()

    def ring_arrival(k, side, letter, hop, part=None):
        sign = 1 - 2 * side
        where = view(late, k, letter, shard_at(-sign * (hop + 1)), part)
        pltpu.make_async_copy(where, where, landing(k, side, letter, hop, part)).wait()
        return where

    def to_sibling(source, target):
        pltpu.make_async_remote_copy(
            src_ref=source,
            dst_ref=target,
            send_sem=pair_send.at[0],
            recv_sem=pair_sem.at[0],
            device_id={"shard": sibling},
            device_id_type=MESH,
        ).start()

    barrier = pltpu.get_barrier_semaphore()
    for offset in (1, -1):
        pl.semaphore_signal(
            barrier, inc=1, device_id={"shard": shard_at(offset)}, device_id_type=MESH
        )

    def run(first, join):
        waiting = []

        def landed(where):
            if join is not None and not joined_at:
                waiting.append(where)
            else:
                to_sibling(where, where)

        joined_at = []
        for j in range(first, count + half):
            if j < count:
                for side in range(2):
                    if hops(side, side) > 0:
                        ring_start(j, side, side, 0)
            for hop in range(half - 1):
                k = j - 1 - hop
                if first <= k < count:
                    for side in range(2):
                        where = ring_arrival(k, side, side, hop)
                        ring_start(k, side, side, hop + 1)
                        landed(where)
            if j < count:
                for side in range(2):
                    if hops(side, 1 - side) > 0:
                        ring_start(j, side, 1 - side, 0)
            for hop in range(half - 2):
                k = j - 1 - hop
                if first <= k < count:
                    for side in range(2):
                        where = ring_arrival(k, side, 1 - side, hop)
                        ring_start(k, side, 1 - side, hop + 1)
                        landed(where)
            if j == join:
                pl.semaphore_wait(joined, 1)
                joined_at.append(j)
                for where in waiting:
                    to_sibling(where, where)
            ends = [
                (j - hops(side, letter), side, letter, hops(side, letter) - 1)
                for flip in range(2)
                for side in range(2)
                for letter in (side ^ flip,)
            ]
            ends = [s for s in ends if s[3] >= 0 and first <= s[0] < count]
            for part in range(parts):
                for s in ends:
                    if part < len(cut(*s)):
                        landed(ring_arrival(*s, cut(*s)[part]))
        if first < count:
            sent = late.at[pl.ds(0, chips - 1), pl.ds(0, rows - starts[first])]
            pltpu.make_async_copy(sent, sent, ring_send.at[0]).wait()

    @pl.when(core == LEAD)
    def _():
        pl.semaphore_signal(barrier, inc=1, device_id={"shard": sibling}, device_id_type=MESH)
        pl.semaphore_wait(barrier, 2)
        run(both, JOIN)

    @pl.when(core != LEAD)
    def _():
        pl.semaphore_wait(barrier, 3)
        pl.semaphore_signal(joined, inc=1, device_id={"shard": sibling}, device_id_type=MESH)
        if extra > 0:
            for offset in range(1, chips):
                owner = shard_at(offset)
                at = pl.ds(starts[both], starts[both + extra] - starts[both])
                to_sibling(early.at[owner, at], late.at[owner, at])
        run(both + extra, None)

    theirs = late.at[pl.ds(0, chips - 1), pl.ds(0, rows - starts[both])]
    pltpu.make_async_copy(theirs, theirs, pair_sem.at[0]).wait()
    pltpu.make_async_copy(theirs, theirs, pair_send.at[0]).wait()


def place_first(*refs):
    source, early, small = refs[0], refs[1], refs[2:4]
    targets, finals, sem = refs[4:7], refs[7:11], refs[11]
    factors, gains, small_sem = refs[12], refs[13], refs[14]
    scales, serve = refs[15:18], refs[18]
    writes = [
        pltpu.make_async_copy(refs[15 + i], finals[i], small_sem.at[2 + i]) for i in range(4)
    ]
    loads = [
        pltpu.make_async_copy(small[i], refs[12 + i], small_sem.at[i]) for i in range(2)
    ]
    n, rows = early.shape[0], early.shape[1]
    starts, both, _ = value_split(rows)
    both_rows = starts[both]
    chip = lax.div(lax.axis_index("shard"), 2)
    copies = [
        pltpu.make_async_copy(source.at[m, i], targets[m].at[i], sem.at[2 if m else min(i, 1)])
        for m in range(2)
        for i in range(source.shape[1])
    ]
    for copy in loads + copies:
        copy.start()
    ours = pl.ds(2 * chip, 2)
    pltpu.make_async_copy(early.at[ours], targets[2].at[ours], sem.at[3]).start()
    if both_rows > 0:
        for offset in range(1, n // 2):
            where = pl.ds(2 * lax.rem(chip + offset, n // 2), 2), pl.ds(0, both_rows)
            pltpu.make_async_copy(early.at[where], targets[2].at[where], sem.at[4]).start()
    for copy in loads:
        copy.wait()
    for m in range(3):
        scales[m][...] = factors[m].reshape(scales[m].shape)
    blocks = [gains[k, i] for i in range(gains.shape[1]) for k in range(gains.shape[0])]
    line = jnp.concatenate(blocks, axis=1)
    serve[...] = line.reshape(serve.shape).astype(jnp.bfloat16)
    copies[0].wait()
    for copy in writes:
        copy.start()
    rest = source.at[0, pl.ds(1, source.shape[1] - 1)]
    second = source.at[1]
    pltpu.make_async_copy(rest, rest, sem.at[1]).wait()
    pltpu.make_async_copy(second, second, sem.at[2]).wait()
    pltpu.make_async_copy(early.at[ours], targets[2].at[ours], sem.at[3]).wait()
    if both_rows > 0:
        part = early.at[pl.ds(0, n - 2), pl.ds(0, both_rows)]
        pltpu.make_async_copy(part, part, sem.at[4]).wait()
    for copy in writes:
        copy.wait()


def place_last(early, late, before, target, sem):
    n, rows = early.shape[0], early.shape[1]
    chips = n // 2
    starts, both, extra = value_split(rows)
    me = lax.axis_index("shard")
    chip, core = me // 2, lax.rem(me, 2)

    def put(source, owner, start, stop):
        if start < stop:
            size = (starts[stop] - starts[start]) // 2
            for part in range(2):
                where = owner, pl.ds(starts[start] + part * size, size)
                pltpu.make_async_copy(source.at[where], target.at[where], sem.at[0]).start()

    count = len(starts) - 1
    for offset in range(1, chips):
        other = lax.rem(chip + offset, chips) * 2
        put(late, other + 1 - core, both, count)

        @pl.when(core == LEAD)
        def _():
            put(late, other + core, both, count)

        @pl.when(core != LEAD)
        def _():
            put(early, other + core, both, both + extra)
            put(late, other + core, both + extra, count)

    part = late.at[pl.ds(0, n - 2), pl.ds(starts[both], rows - starts[both])]
    pltpu.make_async_copy(part, part, sem.at[0]).wait()


def body(n, width, w_query, low_query, high_query, w_key, low_key, high_key, w_value, low_value, high_value, norm_train, norm_step):
    rows, columns = w_query.shape
    rank = low_query.shape[1]
    length = norm_train.shape[0]
    half = n // 4
    count = chunks_of(rows)
    raw = 1
    rounds = n.bit_length() - 1
    reach = min(rows, -(-(rows // count) * raw // 128) * 128)
    slots = len(ring_slots(half))
    starts, both, _ = value_split(rows)
    block = jax.ShapeDtypeStruct((n, rows, columns), jnp.bfloat16)

    def near(value):
        return pltpu.with_memory_space_constraint(value, pltpu.VMEM)

    def far(value):
        return pltpu.with_memory_space_constraint(value, pltpu.HBM)

    ready, early, factors, gains = pl.pallas_call(
        functools.partial(gather_kernel, n, width),
        name="merge_gather",
        out_shape=[
            pltpu.VMEM((2, n, rows, columns), jnp.bfloat16),
            pltpu.VMEM((n, rows, columns), jnp.bfloat16),
            jax.ShapeDtypeStruct((3, 1, columns), jnp.float32),
            jax.ShapeDtypeStruct((width, n, 1, length), jnp.float32),
        ],
        in_specs=[ANY] * 11,
        out_specs=[pl.BlockSpec(memory_space=pltpu.VMEM)] * 2 + [HBM] * 2,
        scratch_shapes=[
            pltpu.VMEM((3, rows, columns), jnp.bfloat16),
            pltpu.VMEM((3, rows, rank), jnp.bfloat16),
            pltpu.VMEM((3, rank, columns), jnp.bfloat16),
            pltpu.VMEM((2, 1, length), jnp.float32),
            pltpu.VMEM((3, rows, columns), jnp.float32),
            pltpu.VMEM((3, 1, columns), jnp.float32),
            pltpu.VMEM((3, rounds + 1, 1, columns), jnp.float32),
            pltpu.SemaphoreType.DMA((4, 3)),
            pltpu.SemaphoreType.DMA((4,)),
            pltpu.SemaphoreType.DMA((3,)),
            pltpu.SemaphoreType.DMA((1,)),
            pltpu.SemaphoreType.DMA((3, rounds)),
            pltpu.SemaphoreType.DMA((1,)),
            pltpu.SemaphoreType.DMA((rounds,)),
            pltpu.SemaphoreType.DMA((5, slots)),
            pltpu.SemaphoreType.DMA((3,)),
            pltpu.VMEM((3, rank, rows), jnp.bfloat16),
            pltpu.VMEM((3, 1, columns), jnp.float32),
            pltpu.VMEM((width, n, 1, length), jnp.float32),
            pltpu.SemaphoreType.DMA((2,)),
            pltpu.VMEM((n, rank, reach), jnp.bfloat16),
            pltpu.VMEM((n, reach, rank), jnp.bfloat16),
            pltpu.SemaphoreType.DMA((raw, slots)),
            pltpu.SemaphoreType.DMA((1,)),
            pltpu.SemaphoreType.DMA((2 * half,)),
            pltpu.VMEM((3, rounds, 1, columns), jnp.float32),
            pltpu.SemaphoreType.DMA((2,)),
            pltpu.SemaphoreType.DMA((2, max(width - 1, 1))),
        ],
        compiler_params=pltpu.CompilerParams(
            collective_id=0, has_side_effects=True, vmem_limit_bytes=20 * 2**20
        ),
    )(
        w_query, w_key, w_value,
        low_query.T, low_key.T, low_value.T,
        high_query, high_key, high_value,
        norm_train.reshape(1, length), norm_step.reshape(1, length),
    )
    query, key, value, *small = pl.pallas_call(
        place_first,
        name="place_first",
        out_shape=[block] * 3
        + [jax.ShapeDtypeStruct((columns,), jnp.float32)] * 3
        + [jax.ShapeDtypeStruct((n * width * length,), jnp.bfloat16)],
        in_specs=[ANY] * 2 + [HBM] * 2,
        out_specs=[HBM] * 7,
        scratch_shapes=[
            pltpu.SemaphoreType.DMA((5,)),
            pltpu.VMEM((3, 1, columns), jnp.float32),
            pltpu.VMEM((width, n, 1, length), jnp.float32),
            pltpu.SemaphoreType.DMA((6,)),
            *[pltpu.VMEM((columns,), jnp.float32)] * 3,
            pltpu.VMEM((n * width * length,), jnp.bfloat16),
        ],
        compiler_params=pltpu.CompilerParams(vmem_limit_bytes=2**20),
    )(near(ready), near(early), far(factors), far(gains))
    late = pl.pallas_call(
        functools.partial(late_kernel, n),
        name="gather_late",
        out_shape=pltpu.VMEM((n, rows, columns), jnp.bfloat16),
        in_specs=[ANY, HBM],
        out_specs=pl.BlockSpec(memory_space=pltpu.VMEM),
        scratch_shapes=[
            pltpu.SemaphoreType.DMA((1,)),
            pltpu.SemaphoreType.DMA((1,)),
            pltpu.SemaphoreType.DMA((1,)),
            pltpu.SemaphoreType.DMA((len(starts) - 1 - both, slots)),
            pltpu.SemaphoreType.REGULAR,
            pltpu.SemaphoreType.DMA((2, last_parts(rows))),
        ],
        compiler_params=pltpu.CompilerParams(
            collective_id=1, has_side_effects=True, vmem_limit_bytes=2**20
        ),
    )(near(early), far(small[0]))
    value = pl.pallas_call(
        place_last,
        name="place_last",
        out_shape=block,
        in_specs=[ANY] * 2 + [HBM],
        out_specs=HBM,
        scratch_shapes=[pltpu.SemaphoreType.DMA((1,))],
        input_output_aliases={2: 0},
        compiler_params=pltpu.CompilerParams(vmem_limit_bytes=2**20),
    )(near(early), near(late), far(value))
    return (
        *(ready.reshape(n * rows, columns) for ready in (query, key, value)),
        *small,
    )


def solution(mesh):
    n, width = mesh.shape["shard"], mesh.shape["width"]
    return jax.shard_map(
        functools.partial(body, n, width),
        mesh=mesh,
        in_specs=(
            P("shard", "width"),
            P("shard", None),
            P(None, "width"),
            P("shard", "width"),
            P("shard", None),
            P(None, "width"),
            P("shard", "width"),
            P("shard", None),
            P(None, "width"),
            P(("shard", "width")),
            P(("shard", "width")),
        ),
        out_specs=(
            P(None, "width"),
            P(None, "width"),
            P(None, "width"),
            P("width"),
            P("width"),
            P("width"),
            P(),
        ),
        check_vma=False,
    )
```
